32 devices in a mesh: row: 16 (over z, y, x), col: 2 (over core).
Axes of the slice: x: 2, y: 2, z: 4, core: 2. Of those that a mesh axis runs over, the one named last changes fastest.
Arguments:
- tokens: bfloat16 [16400, 1024], P('row', 'col'), may hold values from -6 to 6
- norm1_gain: bfloat16 [1024], P('row'), may hold values from 0.099609375 to 1.8984375
- norm1_bias: bfloat16 [1024], P('row'), may hold values from -1.75 to 1.75
- qkv_weight: bfloat16 [1024, 3, 1024], P('row', None, 'col'), may hold values from -0.1875 to 0.1875
- query_bias: bfloat16 [1024], P('col'), may hold values from -1.75 to 1.75
- value_bias: bfloat16 [1024], P('col'), may hold values from -0.3125 to 0.3125
- proj_weight: bfloat16 [1024, 1024], P('col', 'row'), may hold values from -6 to 6
- proj_bias: bfloat16 [1024], P('row'), may hold values from -1.75 to 1.75
- norm2_gain: bfloat16 [1024], P('row'), may hold values from 0.099609375 to 1.8984375
- norm2_bias: bfloat16 [1024], P('row'), may hold values from -1.75 to 1.75
- gate_weight: bfloat16 [1024, 2730], P('row', 'col'), may hold values from -0.1875 to 0.1875
- gate_bias: bfloat16 [2730], P('col'), may hold values from -1.75 to 1.75
- up_weight: bfloat16 [1024, 2730], P('row', 'col'), may hold values from -0.1875 to 0.1875
- up_bias: bfloat16 [2730], P('col'), may hold values from -1.75 to 1.75
- inner_gain: bfloat16 [2730], P('col'), may hold values from 0.099609375 to 1.8984375
- inner_bias: bfloat16 [2730], P('col'), may hold values from -1.75 to 1.75
- down_weight: bfloat16 [2730, 1024], P('col', 'row'), may hold values from -0.109375 to 0.109375
- down_bias: bfloat16 [1024], P('row'), may hold values from -1.75 to 1.75
- cotangent: bfloat16 [16400, 1024], P('row', 'col'), may hold values from -6 to 6
Outputs:
- layer_out: bfloat16 [16400, 1024], P('row', 'col')
- input_grad: bfloat16 [16400, 1024], P('row', 'col')
- norm1_gain_grad: float32 [1024], P('row')
- norm1_bias_grad: float32 [1024], P('row')
- qkv_weight_grad: float32 [1024, 3, 1024], P('row', None, 'col')
- query_bias_grad: float32 [1024], P('col')
- value_bias_grad: float32 [1024], P('col')
- proj_weight_grad: float32 [1024, 1024], P('col', 'row')
- proj_bias_grad: float32 [1024], P('row')
- norm2_gain_grad: float32 [1024], P('row')
- norm2_bias_grad: float32 [1024], P('row')
- gate_weight_grad: float32 [1024, 2730], P('row', 'col')
- gate_bias_grad: float32 [2730], P('col')
- up_weight_grad: float32 [1024, 2730], P('row', 'col')
- up_bias_grad: float32 [2730], P('col')
- inner_gain_grad: float32 [2730], P('col')
- inner_bias_grad: float32 [2730], P('col')
- down_weight_grad: float32 [2730, 1024], P('col', 'row')
- down_bias_grad: float32 [1024], P('row')
The draws below stay inside these ranges and needn't reach their ends.
All inputs are finite; a program needn't handle non-finite values.
Results may differ from the reference program's by a relative error of at most 0.023.
Values may be sent and summed in bfloat16 or wider, within the bound.
A program may use at most 192 MiB of HBM per device.

```python
import math
import jax
import jax.numpy as jnp
from jax import lax

D = 1024
HEADS = 16
HD = 64
FF = 2730
GRID = 32
SEQ = 1025
IMAGES = 16
TOKENS = 16400


def spiked(drawn, stream_key, source, target, shards_of, factor):
    def block_of(dim):
        return (jnp.arange(drawn.shape[dim]) // (drawn.shape[dim] // shards_of)).reshape((-1,) + (1,) * (drawn.ndim - 1 - dim))

    first = jax.random.permutation(stream_key, shards_of)[block_of(target)]
    second = (block_of(target) + shards_of // 2) % shards_of
    return jnp.where((block_of(source) == first) | (block_of(source) == second), factor * drawn, drawn)


def level_of(rng, extent, shards, least, high):
    def one(dim, shards_of):
        heights = jax.random.uniform(jax.random.fold_in(jax.random.fold_in(rng, 6), dim), (shards_of,), jnp.float32, least / len(shards), high / len(shards))
        return jnp.repeat(jnp.exp(heights), extent[dim] // shards_of).reshape((-1,) + (1,) * (len(extent) - dim - 1))

    factor_of = one(*shards[0])
    for cut in shards[1:]:
        factor_of = factor_of * one(*cut)
    return factor_of


def noise(stream_key, dims, scale, limit, shards=(), held_as=jnp.bfloat16):
    values = jax.random.normal(stream_key, dims, jnp.float32) * scale
    if len(shards) > 0:
        values = level_of(stream_key, dims, shards, -0.22, 0.18) * values
    return jnp.clip(values, min=-limit, max=limit).astype(held_as)


def noise_with(rng, extent, spread, most, shards, heavy, kind=jnp.bfloat16):
    drawn = spread * jax.random.normal(rng, extent, jnp.float32)
    if shards:
        drawn = drawn * level_of(rng, extent, shards, -0.22, 0.18)
    return jnp.clip(spiked(drawn, jax.random.fold_in(rng, 3), *heavy), -most, most).astype(kind)


def setup_inputs(seed: int = 0) -> dict:
    keys = jax.random.split(jax.random.key(seed), 20)
    tokens = noise(keys[0], (TOKENS, D), 1.0, 6.0, ((0, 16), (1, 2)))
    norm1_gain = jnp.clip(1.0 + 0.18 * jax.random.normal(keys[1], (D,), jnp.float32), 0.099609375, 1.8984375).astype(jnp.bfloat16)
    norm1_bias = noise(keys[2], (D,), 0.3, 1.75, ((0, 16),))
    qkv_weight = noise(keys[3], (D, 3, D), D ** -0.5, 0.1875, ((0, 16), (2, 2)))
    query_bias = noise(keys[4], (D,), 0.3, 1.75, ((0, 2),))
    value_bias = noise(keys[5], (D,), 0.05, 0.3125, ((0, 2),))
    proj_weight = noise(keys[6], (D, D), (max(2 * D // SEQ, 1)) ** -0.5, 6.0, ((0, 2), (1, 16)))
    proj_bias = noise(keys[7], (D,), 0.3, 1.75, ((0, 16),))
    norm2_gain = jnp.clip(1.0 + 0.18 * jax.random.normal(keys[8], (D,), jnp.float32), 0.099609375, 1.8984375).astype(jnp.bfloat16)
    norm2_bias = noise(keys[9], (D,), 0.3, 1.75, ((0, 16),))
    gate_weight = noise(keys[10], (D, FF), D ** -0.5, 0.1875, ((0, 16), (1, 2)))
    gate_bias = noise(keys[11], (FF,), 0.3, 1.75, ((0, 2),))
    up_weight = noise(keys[12], (D, FF), D ** -0.5, 0.1875, ((0, 16), (1, 2)))
    up_bias = noise(keys[13], (FF,), 0.3, 1.75, ((0, 2),))
    inner_gain = jnp.clip(1.0 + 0.18 * jax.random.normal(keys[14], (FF,), jnp.float32), 0.099609375, 1.8984375).astype(jnp.bfloat16)
    inner_bias = noise(keys[15], (FF,), 0.3, 1.75, ((0, 2),))
    down_weight = noise(keys[16], (FF, D), FF ** -0.5, 0.109375, ((0, 2), (1, 16)))
    down_bias = noise(keys[17], (D,), 0.3, 1.75, ((0, 16),))
    cotangent = noise_with(keys[18], (TOKENS, D), 1.0, 6.0, ((0, 16), (1, 2)), (0, 1, 16, 2.0))
    return {"tokens": tokens, "norm1_gain": norm1_gain, "norm1_bias": norm1_bias, "qkv_weight": qkv_weight, "query_bias": query_bias, "value_bias": value_bias, "proj_weight": proj_weight, "proj_bias": proj_bias, "norm2_gain": norm2_gain, "norm2_bias": norm2_bias, "gate_weight": gate_weight, "gate_bias": gate_bias, "up_weight": up_weight, "up_bias": up_bias, "inner_gain": inner_gain, "inner_bias": inner_bias, "down_weight": down_weight, "down_bias": down_bias, "cotangent": cotangent}


EPSILON = 1e-06
HIGHEST = lax.Precision.HIGHEST

@jax.custom_vjp
def low(v):
    return lax.optimization_barrier(v.astype(jnp.bfloat16)).astype(jnp.float32)

@jax.custom_vjp
def low_back(v):
    return v

def low_keep(v):
    return (low(v), None)

def low_pass(kept, grad):
    return (grad,)

def back_keep(v):
    return (v, None)

def back_low(kept, grad):
    return (low(grad),)
low.defvjp(low_keep, low_pass)
low_back.defvjp(back_keep, back_low)

def layer_norm(values, norm_gain, norm_shift):
    row_mean = lax.optimization_barrier(jnp.mean(values, axis=-1, keepdims=True))
    centred = values - row_mean
    variance = lax.optimization_barrier(jnp.mean(centred * centred, axis=-1, keepdims=True))
    return centred * lax.rsqrt(variance + EPSILON) * norm_gain + norm_shift

def rotary_tables(length, seq_len, grid_side, head_size):
    quarter = head_size // 4
    position = jnp.arange(length, dtype=jnp.int32) % seq_len
    patch_index = jnp.maximum(position - 1, 0)
    inside = (position > 0).astype(jnp.float32)
    row_pos = (patch_index // grid_side).astype(jnp.float32) * inside
    col_pos = (patch_index % grid_side).astype(jnp.float32) * inside
    frequency = jnp.exp(-math.log(10000.0) * jnp.arange(quarter, dtype=jnp.float32) / quarter)
    row_angle = row_pos[:, None] * frequency[None, :]
    col_angle = col_pos[:, None] * frequency[None, :]
    angles = jnp.concatenate([row_angle, row_angle, col_angle, col_angle], axis=1)
    return (jnp.cos(angles), jnp.sin(angles))

def rotate(values):
    pieces = jnp.split(values, 4, axis=-1)
    return jnp.concatenate([-pieces[1], pieces[0], -pieces[3], pieces[2]], axis=-1)

def apply_rotary(values, cosine_table, sine_table):
    return values * cosine_table[:, None, :] + rotate(values) * sine_table[:, None, :]

def head_attention(operands):
    query_head, key_head, value_head = operands
    scores = low_back(jnp.dot(query_head, key_head.T, precision=HIGHEST) * (1.0 / math.sqrt(HD)))
    weights = jax.nn.softmax(scores, axis=-1)
    return jnp.dot(low(weights), value_head, precision=HIGHEST)

def image_layer(params, image):
    norm1_gain, norm1_bias, qkv_weight, query_bias, value_bias, proj_weight, proj_bias, norm2_gain, norm2_bias, gate_weight, gate_bias, up_weight, up_bias, inner_gain, inner_bias, down_weight, down_bias = params
    cosine_table, sine_table = rotary_tables(SEQ, SEQ, GRID, HD)
    first_input = low(layer_norm(image, norm1_gain, norm1_bias))
    qkv_bias = jnp.stack([query_bias, jnp.zeros_like(query_bias), value_bias])
    projected = low_back(jnp.einsum('td,dpe->tpe', first_input, qkv_weight, precision=HIGHEST) + qkv_bias)
    queries = low(apply_rotary(projected[:, 0].reshape(SEQ, HEADS, HD), cosine_table, sine_table))
    keys_all = low(apply_rotary(projected[:, 1].reshape(SEQ, HEADS, HD), cosine_table, sine_table))
    values_all = low(projected[:, 2].reshape(SEQ, HEADS, HD))
    heads_out = lax.map(jax.checkpoint(head_attention), (queries.transpose(1, 0, 2), keys_all.transpose(1, 0, 2), values_all.transpose(1, 0, 2)))
    attended = low(low_back(heads_out.transpose(1, 0, 2).reshape(SEQ, D)))
    attn_branch = low_back(jnp.dot(attended, proj_weight, precision=HIGHEST) + proj_bias)
    residual = image + attn_branch
    second_input = low(layer_norm(residual, norm2_gain, norm2_bias))
    gate_value = low_back(jnp.dot(second_input, gate_weight, precision=HIGHEST) + gate_bias)
    up_value = low_back(jnp.dot(second_input, up_weight, precision=HIGHEST) + up_bias)
    hidden = jax.nn.silu(gate_value) * up_value
    down_input = low(layer_norm(hidden, inner_gain, inner_bias))
    ffn_branch = low_back(jnp.dot(down_input, down_weight, precision=HIGHEST) + down_bias)
    return residual + ffn_branch

def reference(tokens, norm1_gain, norm1_bias, qkv_weight, query_bias, value_bias, proj_weight, proj_bias, norm2_gain, norm2_bias, gate_weight, gate_bias, up_weight, up_bias, inner_gain, inner_bias, down_weight, down_bias, cotangent):
    params = tuple((item.astype(jnp.float32) for item in (norm1_gain, norm1_bias, qkv_weight, query_bias, value_bias, proj_weight, proj_bias, norm2_gain, norm2_bias, gate_weight, gate_bias, up_weight, up_bias, inner_gain, inner_bias, down_weight, down_bias)))
    images = tokens.astype(jnp.float32).reshape(IMAGES, SEQ, D)
    image_grads = cotangent.astype(jnp.float32).reshape(IMAGES, SEQ, D)

    def one_image(totals, operands):
        image, image_grad = operands
        result, backward = jax.vjp(image_layer, params, image)
        param_grads, input_part = backward(image_grad)
        totals = jax.tree.map(jnp.add, totals, param_grads)
        return (totals, (result.astype(jnp.bfloat16), input_part.astype(jnp.bfloat16)))
    zeros = tuple((jnp.zeros_like(item) for item in params))
    totals, (results, input_parts) = lax.scan(one_image, zeros, (images, image_grads))
    return (results.reshape(TOKENS, D), input_parts.reshape(TOKENS, D), totals[0], totals[1], totals[2], totals[3], totals[4], totals[5], totals[6], totals[7], totals[8], totals[9], totals[10], totals[11], totals[12], totals[13], totals[14], totals[15], totals[16])
```

```python
import functools
import math

import jax
import jax.numpy as jnp
from jax import lax
from jax.sharding import PartitionSpec as P

HD = 64
FF = 2730
GRID = 32
SEQ = 1025


EPSILON = 1e-06


def norm_forward(values, norm_gain, norm_shift):
    row_mean = jnp.mean(values, axis=-1, keepdims=True)
    centred = values - row_mean
    variance = jnp.mean(centred * centred, axis=-1, keepdims=True)
    inv_std = lax.rsqrt(variance + EPSILON)
    normed = centred * inv_std
    return (normed * norm_gain + norm_shift, normed, inv_std)


def norm_backward(upstream, normed, inv_std, norm_gain):
    scaled = upstream * norm_gain
    first_mean = jnp.mean(scaled, axis=-1, keepdims=True)
    second_mean = jnp.mean(scaled * normed, axis=-1, keepdims=True)
    delta = inv_std * (scaled - first_mean - normed * second_mean)
    return (delta, jnp.sum(upstream * normed, axis=0), jnp.sum(upstream, axis=0))


def rotary_tables(length, seq_len, grid_side, head_size):
    quarter = head_size // 4
    position = jnp.arange(length, dtype=jnp.int32) % seq_len
    patch_index = jnp.maximum(position - 1, 0)
    inside = (position > 0).astype(jnp.float32)
    row_pos = (patch_index // grid_side).astype(jnp.float32) * inside
    col_pos = (patch_index % grid_side).astype(jnp.float32) * inside
    frequency = jnp.exp(-math.log(10000.0) * jnp.arange(quarter, dtype=jnp.float32) / quarter)
    row_angle = row_pos[:, None] * frequency[None, :]
    col_angle = col_pos[:, None] * frequency[None, :]
    angles = jnp.concatenate([row_angle, row_angle, col_angle, col_angle], axis=1)
    return (jnp.cos(angles), jnp.sin(angles))


def rotate(values):
    pieces = jnp.split(values, 4, axis=-1)
    return jnp.concatenate([-pieces[1], pieces[0], -pieces[3], pieces[2]], axis=-1)


def rotate_transposed(values):
    pieces = jnp.split(values, 4, axis=-1)
    return jnp.concatenate([pieces[1], -pieces[0], pieces[3], -pieces[2]], axis=-1)


def apply_rotary(values, cosine_table, sine_table):
    return values * cosine_table[:, None, :] + rotate(values) * sine_table[:, None, :]


def rotary_back(grads, cosine_table, sine_table):
    return grads * cosine_table[:, None, :] + rotate_transposed(grads * sine_table[:, None, :])


def own_half(vector, column, half_width):
    return lax.dynamic_slice_in_dim(vector, column * half_width, half_width, axis=vector.ndim - 1)


def share_columns(partial_sums):
    return lax.psum_scatter(
        partial_sums.astype(jnp.bfloat16), "col", scatter_dimension=1, tiled=True
    ).astype(jnp.float32)


def join_columns(partial_sums):
    return lax.psum(partial_sums.astype(jnp.bfloat16), "col").astype(jnp.float32)


def hidden_totals(row_sums):
    return lax.psum(row_sums, "col")


def lane_round(width):
    return -(-width // 128) * 128


def pack(pieces):
    offsets = []
    padded = []
    position = 0
    for piece in pieces:
        width = lane_round(piece.shape[1])
        offsets.append(position)
        padded.append(jnp.pad(piece, ((0, 0), (0, width - piece.shape[1]))))
        position += width
    return jnp.concatenate(padded, axis=1), offsets


def spread(vector, rows_local, row_count):
    cols = -(-vector.shape[0] // rows_local)
    block = jnp.pad(vector, (0, rows_local * cols - vector.shape[0])).reshape(rows_local, cols)
    return jnp.tile(block, (row_count, 1))


def body(
    row_count,
    tokens,
    norm1_gain,
    norm1_bias,
    qkv_weight,
    query_bias,
    value_bias,
    proj_weight,
    proj_bias,
    norm2_gain,
    norm2_bias,
    gate_weight,
    gate_bias,
    up_weight,
    up_bias,
    inner_gain,
    inner_bias,
    down_weight,
    down_bias,
    cotangent,
):
    single = jnp.float32
    narrow = jnp.bfloat16
    local_rows = tokens.shape[0]
    half_width = tokens.shape[1]
    rows_local = norm1_gain.shape[0]
    model_width = rows_local * row_count
    ff_local = gate_weight.shape[1]
    head_local = half_width // HD
    images_local = local_rows // SEQ
    column = lax.axis_index("col")
    scaling = 1.0 / math.sqrt(HD)
    cosine_table, sine_table = rotary_tables(local_rows, SEQ, GRID, HD)

    def by_head(array):
        shaped = array.reshape(images_local, SEQ, head_local, HD).transpose(0, 2, 1, 3)
        return shaped.reshape(images_local * head_local, SEQ, HD)

    def from_head(array):
        shaped = array.reshape(images_local, head_local, SEQ, HD).transpose(0, 2, 1, 3)
        return shaped.reshape(local_rows, half_width)

    attn_pack, attn_at = pack(
        [
            qkv_weight.reshape(rows_local, 3 * half_width),
            proj_weight.T,
            jnp.stack([norm1_gain, norm1_bias, proj_bias], axis=1),
        ]
    )
    attn_full = lax.all_gather(attn_pack, "row", axis=0, tiled=True)
    qkv_full = attn_full[:, attn_at[0] : attn_at[0] + 3 * half_width].reshape(
        model_width, 3, half_width
    )
    proj_t = attn_full[:, attn_at[1] : attn_at[1] + half_width]
    attn_vectors = attn_full[:, attn_at[2] : attn_at[2] + 3].astype(single)

    whole_input = lax.all_gather(tokens, "col", axis=1, tiled=True).astype(single)
    normed_out, normed_one, inv_std_one = norm_forward(
        whole_input, attn_vectors[:, 0], attn_vectors[:, 1]
    )
    first_input = normed_out.astype(narrow)
    qkv_bias = jnp.stack(
        [query_bias.astype(single), jnp.zeros((half_width,), single), value_bias.astype(single)]
    )
    projected = (
        jnp.einsum("td,dpe->tpe", first_input, qkv_full, preferred_element_type=single) + qkv_bias
    )
    queries = apply_rotary(
        projected[:, 0].reshape(local_rows, head_local, HD), cosine_table, sine_table
    ).astype(narrow)
    keys_all = apply_rotary(
        projected[:, 1].reshape(local_rows, head_local, HD), cosine_table, sine_table
    ).astype(narrow)
    values_all = projected[:, 2].astype(narrow)

    def attend(operands):
        query_block, key_block, value_block = operands
        scores = (
            jnp.einsum("qd,kd->qk", query_block, key_block, preferred_element_type=single) * scaling
        )
        weights = jax.nn.softmax(scores, axis=-1)
        mixed = jnp.einsum(
            "qk,kd->qd", weights.astype(narrow), value_block, preferred_element_type=single
        )
        return mixed.astype(narrow)

    attended = from_head(
        lax.map(attend, (by_head(queries), by_head(keys_all), by_head(values_all)))
    )
    attn_partial = jnp.einsum("te,de->td", attended, proj_t, preferred_element_type=single)
    residual_half = (
        tokens.astype(single)
        + share_columns(attn_partial)
        + own_half(attn_vectors[:, 2], column, half_width)
    )
    residual_full = lax.all_gather(
        residual_half.astype(jnp.bfloat16), "col", axis=1, tiled=True
    ).astype(residual_half.dtype)

    ffn_pack, ffn_at = pack(
        [
            gate_weight,
            up_weight,
            down_weight.T,
            jnp.stack([norm2_gain, norm2_bias, down_bias], axis=1),
        ]
    )
    ffn_full = lax.all_gather(ffn_pack, "row", axis=0, tiled=True)
    gate_full = ffn_full[:, ffn_at[0] : ffn_at[0] + ff_local]
    up_full = ffn_full[:, ffn_at[1] : ffn_at[1] + ff_local]
    down_t = ffn_full[:, ffn_at[2] : ffn_at[2] + ff_local]
    ffn_vectors = ffn_full[:, ffn_at[3] : ffn_at[3] + 3].astype(single)

    second_out, normed_two, inv_std_two = norm_forward(
        residual_full, ffn_vectors[:, 0], ffn_vectors[:, 1]
    )
    second_input = second_out.astype(narrow)
    gate_value = jnp.dot(second_input, gate_full, preferred_element_type=single) + gate_bias.astype(
        single
    )
    up_value = jnp.dot(second_input, up_full, preferred_element_type=single) + up_bias.astype(
        single
    )
    sigmoid_gate = jax.nn.sigmoid(gate_value)
    hidden = gate_value * sigmoid_gate * up_value
    hidden_mean = hidden_totals((jnp.sum(hidden, axis=1),))[0][:, None] / FF
    hidden_centred = hidden - hidden_mean
    hidden_var = hidden_totals((jnp.sum(hidden_centred * hidden_centred, axis=1),))[0][:, None] / FF
    hidden_inv = lax.rsqrt(hidden_var + EPSILON)
    hidden_normed = hidden_centred * hidden_inv
    down_input = (hidden_normed * inner_gain.astype(single) + inner_bias.astype(single)).astype(
        narrow
    )
    ffn_partial = jnp.einsum("tf,df->td", down_input, down_t, preferred_element_type=single)
    layer_out = (
        residual_half
        + share_columns(ffn_partial)
        + own_half(ffn_vectors[:, 2], column, half_width)
    ).astype(narrow)
    out_full = lax.all_gather(cotangent, "col", axis=1, tiled=True)
    out_float = out_full.astype(single)
    down_weight_grad_t = jnp.einsum(
        "td,tf->df", out_full, down_input, preferred_element_type=single
    )
    down_bias_grad = jnp.sum(out_float, axis=0)
    normed_grad = jnp.einsum("td,df->tf", out_full, down_t, preferred_element_type=single)
    scaled_grad = normed_grad * inner_gain.astype(single)
    first_total, second_total = hidden_totals(
        (jnp.sum(scaled_grad, axis=1), jnp.sum(scaled_grad * hidden_normed, axis=1))
    )
    hidden_grad = hidden_inv * (
        scaled_grad - first_total[:, None] / FF - hidden_normed * (second_total[:, None] / FF)
    )
    inner_gain_grad = jnp.sum(normed_grad * hidden_normed, axis=0)
    inner_bias_grad = jnp.sum(normed_grad, axis=0)
    gate_grad = (
        hidden_grad * up_value * sigmoid_gate * (1.0 + gate_value * (1.0 - sigmoid_gate))
    ).astype(narrow)
    up_grad = (hidden_grad * gate_value * sigmoid_gate).astype(narrow)
    gate_bias_grad = jnp.sum(gate_grad.astype(single), axis=0)
    up_bias_grad = jnp.sum(up_grad.astype(single), axis=0)
    gate_weight_grad = jnp.einsum(
        "td,tf->df", second_input, gate_grad, preferred_element_type=single
    )
    up_weight_grad = jnp.einsum("td,tf->df", second_input, up_grad, preferred_element_type=single)
    second_back = join_columns(
        jnp.einsum("tf,df->td", gate_grad, gate_full, preferred_element_type=single)
        + jnp.einsum("tf,df->td", up_grad, up_full, preferred_element_type=single)
    )
    second_delta, gain_two_grad, shift_two_grad = norm_backward(
        second_back, normed_two, inv_std_two, ffn_vectors[:, 0]
    )
    residual_grad = out_float + second_delta
    attn_grad = residual_grad.astype(narrow)
    proj_bias_grad = jnp.sum(attn_grad.astype(single), axis=0)
    proj_weight_grad_t = jnp.einsum(
        "td,te->de", attn_grad, attended, preferred_element_type=single
    )
    mid_small = jnp.concatenate([gate_bias_grad, up_bias_grad, inner_gain_grad, inner_bias_grad])
    mid_pack, mid_at = pack(
        [
            gate_weight_grad.astype(narrow),
            up_weight_grad.astype(narrow),
            down_weight_grad_t.astype(narrow),
            proj_weight_grad_t.astype(narrow),
            jnp.stack(
                [gain_two_grad, shift_two_grad, down_bias_grad, proj_bias_grad], axis=1
            ).astype(narrow),
            spread(mid_small, rows_local, row_count).astype(narrow),
        ]
    )
    mid_sums = lax.psum_scatter(mid_pack, "row", scatter_dimension=0, tiled=True).astype(single)
    attended_grad = jnp.einsum(
        "td,de->te", attn_grad, proj_t, preferred_element_type=single
    ).astype(narrow)

    def attend_back(operands):
        query_block, key_block, value_block, grad_block = operands
        scores = (
            jnp.einsum("qd,kd->qk", query_block, key_block, preferred_element_type=single) * scaling
        )
        weights = jax.nn.softmax(scores, axis=-1)
        value_grad = jnp.einsum(
            "qk,qd->kd", weights.astype(narrow), grad_block, preferred_element_type=single
        )
        weight_grad = jnp.einsum(
            "qd,kd->qk", grad_block, value_block, preferred_element_type=single
        )
        score_grad = (
            weights * (weight_grad - jnp.sum(weight_grad * weights, axis=-1, keepdims=True))
        ).astype(narrow)
        query_grad = (
            jnp.einsum("qk,kd->qd", score_grad, key_block, preferred_element_type=single) * scaling
        )
        key_grad = (
            jnp.einsum("qk,qd->kd", score_grad, query_block, preferred_element_type=single)
            * scaling
        )
        return (query_grad, key_grad, value_grad)

    query_grads, key_grads, value_grads = lax.map(
        attend_back,
        (by_head(queries), by_head(keys_all), by_head(values_all), by_head(attended_grad)),
    )
    query_pre = rotary_back(
        from_head(query_grads).reshape(local_rows, head_local, HD), cosine_table, sine_table
    )
    key_pre = rotary_back(
        from_head(key_grads).reshape(local_rows, head_local, HD), cosine_table, sine_table
    )
    qkv_grad = jnp.stack(
        [
            query_pre.reshape(local_rows, half_width),
            key_pre.reshape(local_rows, half_width),
            from_head(value_grads),
        ],
        axis=1,
    ).astype(narrow)
    qkv_grad_float = qkv_grad.astype(single)
    query_bias_grad = jnp.sum(qkv_grad_float[:, 0], axis=0)
    value_bias_grad = jnp.sum(qkv_grad_float[:, 2], axis=0)
    qkv_weight_grad = jnp.einsum(
        "td,tpe->dpe", first_input, qkv_grad, preferred_element_type=single
    )
    first_back = join_columns(
        jnp.einsum("tpe,dpe->td", qkv_grad, qkv_full, preferred_element_type=single)
    )
    first_delta, gain_one_grad, shift_one_grad = norm_backward(
        first_back, normed_one, inv_std_one, attn_vectors[:, 0]
    )
    input_grad = own_half(residual_grad + first_delta, column, half_width).astype(narrow)
    end_pack, end_at = pack(
        [
            qkv_weight_grad.reshape(model_width, 3 * half_width).astype(narrow),
            jnp.stack([gain_one_grad, shift_one_grad], axis=1).astype(narrow),
            spread(
                jnp.concatenate([query_bias_grad, value_bias_grad]), rows_local, row_count
            ).astype(narrow),
        ]
    )
    end_sums = lax.psum_scatter(end_pack, "row", scatter_dimension=0, tiled=True).astype(single)

    def cut(sums, offset, width):
        return sums[:, offset : offset + width]

    mid_vectors = cut(mid_sums, mid_at[4], 4)
    mid_small_sum = cut(mid_sums, mid_at[5], -(-mid_small.shape[0] // rows_local)).reshape(-1)
    end_vectors = cut(end_sums, end_at[1], 2)
    end_small_sum = cut(end_sums, end_at[2], -(-2 * half_width // rows_local)).reshape(-1)
    return (
        layer_out,
        input_grad,
        end_vectors[:, 0],
        end_vectors[:, 1],
        cut(end_sums, end_at[0], 3 * half_width).reshape(rows_local, 3, half_width),
        end_small_sum[:half_width],
        end_small_sum[half_width : 2 * half_width],
        cut(mid_sums, mid_at[3], half_width).T,
        mid_vectors[:, 3],
        mid_vectors[:, 0],
        mid_vectors[:, 1],
        cut(mid_sums, mid_at[0], ff_local),
        mid_small_sum[:ff_local],
        cut(mid_sums, mid_at[1], ff_local),
        mid_small_sum[ff_local : 2 * ff_local],
        mid_small_sum[2 * ff_local : 3 * ff_local],
        mid_small_sum[3 * ff_local : 4 * ff_local],
        cut(mid_sums, mid_at[2], ff_local).T,
        mid_vectors[:, 2],
    )


def solution(mesh):
    placed = (
        P("row", "col"),
        P("row"),
        P("row"),
        P("row", None, "col"),
        P("col"),
        P("col"),
        P("col", "row"),
        P("row"),
        P("row"),
        P("row"),
        P("row", "col"),
        P("col"),
        P("row", "col"),
        P("col"),
        P("col"),
        P("col"),
        P("col", "row"),
        P("row"),
        P("row", "col"),
    )
    return jax.shard_map(
        functools.partial(body, mesh.shape["row"]),
        mesh=mesh,
        in_specs=placed,
        out_specs=(
            P("row", "col"),
            P("row", "col"),
            P("row"),
            P("row"),
            P("row", None, "col"),
            P("col"),
            P("col"),
            P("col", "row"),
            P("row"),
            P("row"),
            P("row"),
            P("row", "col"),
            P("col"),
            P("row", "col"),
            P("col"),
            P("col"),
            P("col"),
            P("col", "row"),
            P("row"),
        ),
        check_vma=False,
    )
```

```python
import functools
import math

import jax
import jax.numpy as jnp
from jax import lax
from jax.sharding import PartitionSpec as P


HD = 64
FF = 2730
GRID = 32
SEQ = 1025


EPSILON = 1e-06


def norm_forward(values, norm_gain, norm_shift):
    row_mean = jnp.mean(values, axis=-1, keepdims=True)
    centred = values - row_mean
    variance = jnp.mean(centred * centred, axis=-1, keepdims=True)
    inv_std = lax.rsqrt(variance + EPSILON)
    normed = centred * inv_std
    return (normed * norm_gain + norm_shift, normed, inv_std)


def norm_backward(upstream, normed, inv_std, norm_gain):
    scaled = upstream * norm_gain
    first_mean = jnp.mean(scaled, axis=-1, keepdims=True)
    second_mean = jnp.mean(scaled * normed, axis=-1, keepdims=True)
    delta = inv_std * (scaled - first_mean - normed * second_mean)
    return (delta, jnp.sum(upstream * normed, axis=0), jnp.sum(upstream, axis=0))


def rotary_tables(length, seq_len, grid_side, head_size):
    quarter = head_size // 4
    position = jnp.arange(length, dtype=jnp.int32) % seq_len
    patch_index = jnp.maximum(position - 1, 0)
    inside = (position > 0).astype(jnp.float32)
    row_pos = (patch_index // grid_side).astype(jnp.float32) * inside
    col_pos = (patch_index % grid_side).astype(jnp.float32) * inside
    frequency = jnp.exp(-math.log(10000.0) * jnp.arange(quarter, dtype=jnp.float32) / quarter)
    row_angle = row_pos[:, None] * frequency[None, :]
    col_angle = col_pos[:, None] * frequency[None, :]
    angles = jnp.concatenate([row_angle, row_angle, col_angle, col_angle], axis=1)
    return (jnp.cos(angles), jnp.sin(angles))


def rotate(values):
    pieces = jnp.split(values, 4, axis=-1)
    return jnp.concatenate([-pieces[1], pieces[0], -pieces[3], pieces[2]], axis=-1)


def rotate_transposed(values):
    pieces = jnp.split(values, 4, axis=-1)
    return jnp.concatenate([pieces[1], -pieces[0], pieces[3], -pieces[2]], axis=-1)


def apply_rotary(values, cosine_table, sine_table):
    return values * cosine_table[:, None, :] + rotate(values) * sine_table[:, None, :]


def rotary_back(grads, cosine_table, sine_table):
    return grads * cosine_table[:, None, :] + rotate_transposed(grads * sine_table[:, None, :])


def own_half(vector, column, half_width):
    return lax.dynamic_slice_in_dim(vector, column * half_width, half_width, axis=vector.ndim - 1)


def swap_columns(values):
    return lax.ppermute(values, "col", [(0, 1), (1, 0)])


def share_columns(partial_sums):
    half = partial_sums.shape[1] // 2
    column = lax.axis_index("col")
    own = lax.dynamic_slice_in_dim(partial_sums, column * half, half, axis=1)
    other = lax.dynamic_slice_in_dim(partial_sums, (1 - column) * half, half, axis=1)
    return own + swap_columns(other.astype(jnp.bfloat16)).astype(jnp.float32)


def join_columns(partial_sums):
    narrow = partial_sums.astype(jnp.bfloat16)
    return narrow.astype(jnp.float32) + swap_columns(narrow).astype(jnp.float32)


def gather_columns(values):
    other = swap_columns(values)
    first = lax.axis_index("col") == 0
    return jnp.concatenate(
        [jnp.where(first, values, other), jnp.where(first, other, values)], axis=1
    )


def hidden_totals(row_sums):
    return lax.psum(row_sums, "col")


def lane_round(width):
    return -(-width // 128) * 128


def pack(pieces):
    offsets = []
    padded = []
    position = 0
    for piece in pieces:
        width = lane_round(piece.shape[1])
        offsets.append(position)
        padded.append(jnp.pad(piece, ((0, 0), (0, width - piece.shape[1]))))
        position += width
    return jnp.concatenate(padded, axis=1), offsets


def spread(vector, rows_local, row_count):
    cols = -(-vector.shape[0] // rows_local)
    block = jnp.pad(vector, (0, rows_local * cols - vector.shape[0])).reshape(rows_local, cols)
    return jnp.tile(block, (row_count, 1))


def body(
    row_count,
    tokens,
    norm1_gain,
    norm1_bias,
    qkv_weight,
    query_bias,
    value_bias,
    proj_weight,
    proj_bias,
    norm2_gain,
    norm2_bias,
    gate_weight,
    gate_bias,
    up_weight,
    up_bias,
    inner_gain,
    inner_bias,
    down_weight,
    down_bias,
    cotangent,
):
    single = jnp.float32
    narrow = jnp.bfloat16
    local_rows = tokens.shape[0]
    half_width = tokens.shape[1]
    rows_local = norm1_gain.shape[0]
    model_width = rows_local * row_count
    ff_local = gate_weight.shape[1]
    head_local = half_width // HD
    images_local = local_rows // SEQ
    column = lax.axis_index("col")
    scaling = 1.0 / math.sqrt(HD)
    cosine_table, sine_table = rotary_tables(local_rows, SEQ, GRID, HD)

    def by_head(array):
        shaped = array.reshape(images_local, SEQ, head_local, HD).transpose(0, 2, 1, 3)
        return shaped.reshape(images_local * head_local, SEQ, HD)

    def from_head(array):
        shaped = array.reshape(images_local, head_local, SEQ, HD).transpose(0, 2, 1, 3)
        return shaped.reshape(local_rows, half_width)

    attn_pack, attn_at = pack(
        [
            qkv_weight.reshape(rows_local, 3 * half_width),
            proj_weight.T,
            jnp.stack([norm1_gain, norm1_bias, proj_bias], axis=1),
        ]
    )
    attn_full = lax.all_gather(attn_pack, "row", axis=0, tiled=True)
    qkv_full = attn_full[:, attn_at[0] : attn_at[0] + 3 * half_width].reshape(
        model_width, 3, half_width
    )
    proj_t = attn_full[:, attn_at[1] : attn_at[1] + half_width]
    attn_vectors = attn_full[:, attn_at[2] : attn_at[2] + 3].astype(single)

    whole_input = gather_columns(tokens).astype(single)
    normed_out, normed_one, inv_std_one = norm_forward(
        whole_input, attn_vectors[:, 0], attn_vectors[:, 1]
    )
    first_input = normed_out.astype(narrow)
    qkv_bias = jnp.stack(
        [query_bias.astype(single), jnp.zeros((half_width,), single), value_bias.astype(single)]
    )
    projected = (
        jnp.einsum("td,dpe->tpe", first_input, qkv_full, preferred_element_type=single) + qkv_bias
    )
    queries = apply_rotary(
        projected[:, 0].reshape(local_rows, head_local, HD), cosine_table, sine_table
    ).astype(narrow)
    keys_all = apply_rotary(
        projected[:, 1].reshape(local_rows, head_local, HD), cosine_table, sine_table
    ).astype(narrow)
    values_all = projected[:, 2].astype(narrow)

    def attend(operands):
        query_block, key_block, value_block = operands
        scores = (
            jnp.einsum("qd,kd->qk", query_block, key_block, preferred_element_type=single) * scaling
        )
        weights = jax.nn.softmax(scores, axis=-1)
        mixed = jnp.einsum(
            "qk,kd->qd", weights.astype(narrow), value_block, preferred_element_type=single
        )
        return mixed.astype(narrow)

    attended = from_head(
        lax.map(attend, (by_head(queries), by_head(keys_all), by_head(values_all)))
    )
    attn_partial = jnp.einsum("te,de->td", attended, proj_t, preferred_element_type=single)
    residual_half = (
        tokens.astype(single)
        + share_columns(attn_partial)
        + own_half(attn_vectors[:, 2], column, half_width)
    )
    residual_full = gather_columns(residual_half.astype(jnp.bfloat16)).astype(residual_half.dtype)

    ffn_pack, ffn_at = pack(
        [
            gate_weight,
            up_weight,
            down_weight.T,
            jnp.stack([norm2_gain, norm2_bias, down_bias], axis=1),
        ]
    )
    ffn_full = lax.all_gather(ffn_pack, "row", axis=0, tiled=True)
    gate_full = ffn_full[:, ffn_at[0] : ffn_at[0] + ff_local]
    up_full = ffn_full[:, ffn_at[1] : ffn_at[1] + ff_local]
    down_t = ffn_full[:, ffn_at[2] : ffn_at[2] + ff_local]
    ffn_vectors = ffn_full[:, ffn_at[3] : ffn_at[3] + 3].astype(single)

    second_out, normed_two, inv_std_two = norm_forward(
        residual_full, ffn_vectors[:, 0], ffn_vectors[:, 1]
    )
    second_input = second_out.astype(narrow)
    gate_value = jnp.dot(second_input, gate_full, preferred_element_type=single) + gate_bias.astype(
        single
    )
    up_value = jnp.dot(second_input, up_full, preferred_element_type=single) + up_bias.astype(
        single
    )
    sigmoid_gate = jax.nn.sigmoid(gate_value)
    hidden = gate_value * sigmoid_gate * up_value
    hidden_mean = hidden_totals((jnp.sum(hidden, axis=1),))[0][:, None] / FF
    hidden_centred = hidden - hidden_mean
    hidden_var = hidden_totals((jnp.sum(hidden_centred * hidden_centred, axis=1),))[0][:, None] / FF
    hidden_inv = lax.rsqrt(hidden_var + EPSILON)
    hidden_normed = hidden_centred * hidden_inv
    down_input = (hidden_normed * inner_gain.astype(single) + inner_bias.astype(single)).astype(
        narrow
    )
    ffn_partial = jnp.einsum("tf,df->td", down_input, down_t, preferred_element_type=single)
    layer_out = (
        residual_half
        + share_columns(ffn_partial)
        + own_half(ffn_vectors[:, 2], column, half_width)
    ).astype(narrow)
    out_full = gather_columns(cotangent)
    out_float = out_full.astype(single)
    down_weight_grad_t = jnp.einsum(
        "td,tf->df", out_full, down_input, preferred_element_type=single
    )
    down_bias_grad = jnp.sum(out_float, axis=0)
    normed_grad = jnp.einsum("td,df->tf", out_full, down_t, preferred_element_type=single)
    scaled_grad = normed_grad * inner_gain.astype(single)
    first_total, second_total = hidden_totals(
        (jnp.sum(scaled_grad, axis=1), jnp.sum(scaled_grad * hidden_normed, axis=1))
    )
    hidden_grad = hidden_inv * (
        scaled_grad - first_total[:, None] / FF - hidden_normed * (second_total[:, None] / FF)
    )
    inner_gain_grad = jnp.sum(normed_grad * hidden_normed, axis=0)
    inner_bias_grad = jnp.sum(normed_grad, axis=0)
    down_small = jnp.concatenate([inner_gain_grad, inner_bias_grad])
    down_pack, down_at = pack(
        [
            down_weight_grad_t.astype(narrow),
            down_bias_grad[:, None].astype(narrow),
            spread(down_small, rows_local, row_count).astype(narrow),
        ]
    )
    down_pack, hidden_grad = lax.optimization_barrier((down_pack, hidden_grad))
    down_sums = lax.psum_scatter(down_pack, "row", scatter_dimension=0, tiled=True)
    gate_grad = (
        hidden_grad * up_value * sigmoid_gate * (1.0 + gate_value * (1.0 - sigmoid_gate))
    ).astype(narrow)
    up_grad = (hidden_grad * gate_value * sigmoid_gate).astype(narrow)
    gate_bias_grad = jnp.sum(gate_grad.astype(single), axis=0)
    up_bias_grad = jnp.sum(up_grad.astype(single), axis=0)
    gate_weight_grad = jnp.einsum(
        "td,tf->df", second_input, gate_grad, preferred_element_type=single
    )
    up_weight_grad = jnp.einsum("td,tf->df", second_input, up_grad, preferred_element_type=single)
    second_back = join_columns(
        jnp.einsum("tf,df->td", gate_grad, gate_full, preferred_element_type=single)
        + jnp.einsum("tf,df->td", up_grad, up_full, preferred_element_type=single)
    )
    second_delta, gain_two_grad, shift_two_grad = norm_backward(
        second_back, normed_two, inv_std_two, ffn_vectors[:, 0]
    )
    residual_grad = out_float + second_delta
    attn_grad = residual_grad.astype(narrow)
    proj_bias_grad = jnp.sum(attn_grad.astype(single), axis=0)
    proj_weight_grad_t = jnp.einsum(
        "td,te->de", attn_grad, attended, preferred_element_type=single
    )
    mid_small = jnp.concatenate([gate_bias_grad, up_bias_grad])
    mid_pack, mid_at = pack(
        [
            gate_weight_grad.astype(narrow),
            up_weight_grad.astype(narrow),
            proj_weight_grad_t.astype(narrow),
            jnp.stack([gain_two_grad, shift_two_grad, proj_bias_grad], axis=1).astype(narrow),
            spread(mid_small, rows_local, row_count).astype(narrow),
        ]
    )
    mid_pack, attn_grad_held = lax.optimization_barrier((mid_pack, attn_grad))
    mid_sums = lax.psum_scatter(mid_pack, "row", scatter_dimension=0, tiled=True).astype(single)
    attended_grad = jnp.einsum(
        "td,de->te", attn_grad_held, proj_t, preferred_element_type=single
    ).astype(narrow)

    def attend_back(operands):
        query_block, key_block, value_block, grad_block = operands
        scores = (
            jnp.einsum("qd,kd->qk", query_block, key_block, preferred_element_type=single) * scaling
        )
        weights = jax.nn.softmax(scores, axis=-1)
        value_grad = jnp.einsum(
            "qk,qd->kd", weights.astype(narrow), grad_block, preferred_element_type=single
        )
        weight_grad = jnp.einsum(
            "qd,kd->qk", grad_block, value_block, preferred_element_type=single
        )
        score_grad = (
            weights * (weight_grad - jnp.sum(weight_grad * weights, axis=-1, keepdims=True))
        ).astype(narrow)
        query_grad = (
            jnp.einsum("qk,kd->qd", score_grad, key_block, preferred_element_type=single) * scaling
        )
        key_grad = (
            jnp.einsum("qk,qd->kd", score_grad, query_block, preferred_element_type=single)
            * scaling
        )
        return (query_grad, key_grad, value_grad)

    query_grads, key_grads, value_grads = lax.map(
        attend_back,
        (by_head(queries), by_head(keys_all), by_head(values_all), by_head(attended_grad)),
    )
    query_grads, down_sums = lax.optimization_barrier((query_grads, down_sums))
    query_pre = rotary_back(
        from_head(query_grads).reshape(local_rows, head_local, HD), cosine_table, sine_table
    )
    key_pre = rotary_back(
        from_head(key_grads).reshape(local_rows, head_local, HD), cosine_table, sine_table
    )
    qkv_grad = jnp.stack(
        [
            query_pre.reshape(local_rows, half_width),
            key_pre.reshape(local_rows, half_width),
            from_head(value_grads),
        ],
        axis=1,
    ).astype(narrow)
    qkv_grad_float = qkv_grad.astype(single)
    query_bias_grad = jnp.sum(qkv_grad_float[:, 0], axis=0)
    value_bias_grad = jnp.sum(qkv_grad_float[:, 2], axis=0)
    qkv_weight_grad = jnp.einsum(
        "td,tpe->dpe", first_input, qkv_grad, preferred_element_type=single
    )
    first_back = join_columns(
        jnp.einsum("tpe,dpe->td", qkv_grad, qkv_full, preferred_element_type=single)
    )
    first_delta, gain_one_grad, shift_one_grad = norm_backward(
        first_back, normed_one, inv_std_one, attn_vectors[:, 0]
    )
    input_grad = own_half(residual_grad + first_delta, column, half_width).astype(narrow)
    end_pack, end_at = pack(
        [
            qkv_weight_grad.reshape(model_width, 3 * half_width).astype(narrow),
            jnp.stack([gain_one_grad, shift_one_grad], axis=1).astype(narrow),
            spread(
                jnp.concatenate([query_bias_grad, value_bias_grad]), rows_local, row_count
            ).astype(narrow),
        ]
    )
    end_pack, mid_sums = lax.optimization_barrier((end_pack, mid_sums))
    end_sums = lax.psum_scatter(end_pack, "row", scatter_dimension=0, tiled=True).astype(single)

    def cut(sums, offset, width):
        return sums[:, offset : offset + width]

    down_sums = down_sums.astype(single)
    mid_vectors = cut(mid_sums, mid_at[3], 3)
    mid_small_sum = cut(mid_sums, mid_at[4], -(-mid_small.shape[0] // rows_local)).reshape(-1)
    down_small_sum = cut(down_sums, down_at[2], -(-down_small.shape[0] // rows_local)).reshape(-1)
    end_vectors = cut(end_sums, end_at[1], 2)
    end_small_sum = cut(end_sums, end_at[2], -(-2 * half_width // rows_local)).reshape(-1)
    return (
        layer_out,
        input_grad,
        end_vectors[:, 0],
        end_vectors[:, 1],
        cut(end_sums, end_at[0], 3 * half_width).reshape(rows_local, 3, half_width),
        end_small_sum[:half_width],
        end_small_sum[half_width : 2 * half_width],
        cut(mid_sums, mid_at[2], half_width).T,
        mid_vectors[:, 2],
        mid_vectors[:, 0],
        mid_vectors[:, 1],
        cut(mid_sums, mid_at[0], ff_local),
        mid_small_sum[:ff_local],
        cut(mid_sums, mid_at[1], ff_local),
        mid_small_sum[ff_local : 2 * ff_local],
        down_small_sum[:ff_local],
        down_small_sum[ff_local : 2 * ff_local],
        cut(down_sums, down_at[0], ff_local).T,
        down_sums[:, down_at[1]],
    )


def solution(mesh):
    placed = (
        P("row", "col"),
        P("row"),
        P("row"),
        P("row", None, "col"),
        P("col"),
        P("col"),
        P("col", "row"),
        P("row"),
        P("row"),
        P("row"),
        P("row", "col"),
        P("col"),
        P("row", "col"),
        P("col"),
        P("col"),
        P("col"),
        P("col", "row"),
        P("row"),
        P("row", "col"),
    )
    return jax.shard_map(
        functools.partial(body, mesh.shape["row"]),
        mesh=mesh,
        in_specs=placed,
        out_specs=(
            P("row", "col"),
            P("row", "col"),
            P("row"),
            P("row"),
            P("row", None, "col"),
            P("col"),
            P("col"),
            P("col", "row"),
            P("row"),
            P("row"),
            P("row"),
            P("row", "col"),
            P("col"),
            P("row", "col"),
            P("col"),
            P("col"),
            P("col"),
            P("col", "row"),
            P("row"),
        ),
        check_vma=False,
    )
```

```python
import functools
import math

import jax
import jax.numpy as jnp
from jax import lax
from jax.sharding import PartitionSpec as P


HD = 64
FF = 2730
GRID = 32
SEQ = 1025


EPSILON = 1e-06


def norm_forward(values, norm_gain, norm_shift):
    row_mean = jnp.mean(values, axis=-1, keepdims=True)
    centred = values - row_mean
    variance = jnp.mean(centred * centred, axis=-1, keepdims=True)
    inv_std = lax.rsqrt(variance + EPSILON)
    normed = centred * inv_std
    return (normed * norm_gain + norm_shift, normed, inv_std)


def norm_backward(upstream, normed, inv_std, norm_gain):
    scaled = upstream * norm_gain
    first_mean = jnp.mean(scaled, axis=-1, keepdims=True)
    second_mean = jnp.mean(scaled * normed, axis=-1, keepdims=True)
    delta = inv_std * (scaled - first_mean - normed * second_mean)
    return (delta, jnp.sum(upstream * normed, axis=0), jnp.sum(upstream, axis=0))


def rotary_tables(length, seq_len, grid_side, head_size):
    quarter = head_size // 4
    position = jnp.arange(length, dtype=jnp.int32) % seq_len
    patch_index = jnp.maximum(position - 1, 0)
    inside = (position > 0).astype(jnp.float32)
    row_pos = (patch_index // grid_side).astype(jnp.float32) * inside
    col_pos = (patch_index % grid_side).astype(jnp.float32) * inside
    frequency = jnp.exp(-math.log(10000.0) * jnp.arange(quarter, dtype=jnp.float32) / quarter)
    row_angle = row_pos[:, None] * frequency[None, :]
    col_angle = col_pos[:, None] * frequency[None, :]
    angles = jnp.concatenate([row_angle, row_angle, col_angle, col_angle], axis=1)
    return (jnp.cos(angles), jnp.sin(angles))


def rotate(values):
    pieces = jnp.split(values, 4, axis=-1)
    return jnp.concatenate([-pieces[1], pieces[0], -pieces[3], pieces[2]], axis=-1)


def rotate_transposed(values):
    pieces = jnp.split(values, 4, axis=-1)
    return jnp.concatenate([pieces[1], -pieces[0], pieces[3], -pieces[2]], axis=-1)


def apply_rotary(values, cosine_table, sine_table):
    return values * cosine_table[:, None, :] + rotate(values) * sine_table[:, None, :]


def rotary_back(grads, cosine_table, sine_table):
    return grads * cosine_table[:, None, :] + rotate_transposed(grads * sine_table[:, None, :])


def own_half(vector, column, half_width):
    return lax.dynamic_slice_in_dim(vector, column * half_width, half_width, axis=vector.ndim - 1)


def swap_columns(values):
    return lax.ppermute(values, "col", [(0, 1), (1, 0)])


def share_columns(partial_sums):
    half = partial_sums.shape[1] // 2
    column = lax.axis_index("col")
    own = lax.dynamic_slice_in_dim(partial_sums, column * half, half, axis=1)
    other = lax.dynamic_slice_in_dim(partial_sums, (1 - column) * half, half, axis=1)
    return own + swap_columns(other.astype(jnp.bfloat16)).astype(jnp.float32)


def join_columns(partial_sums):
    narrow = partial_sums.astype(jnp.bfloat16)
    return narrow.astype(jnp.float32) + swap_columns(narrow).astype(jnp.float32)


def gather_columns(values):
    other = swap_columns(values)
    first = lax.axis_index("col") == 0
    return jnp.concatenate(
        [jnp.where(first, values, other), jnp.where(first, other, values)], axis=1
    )


def hidden_totals(row_sums):
    return tuple(part + swap_columns(part) for part in row_sums)


def lane_round(width):
    return -(-width // 128) * 128


def pack(pieces):
    offsets = []
    padded = []
    position = 0
    for piece in pieces:
        width = lane_round(piece.shape[1])
        offsets.append(position)
        padded.append(jnp.pad(piece, ((0, 0), (0, width - piece.shape[1]))))
        position += width
    return jnp.concatenate(padded, axis=1), offsets


def spread(vector, rows_local, row_count):
    cols = -(-vector.shape[0] // rows_local)
    block = jnp.pad(vector, (0, rows_local * cols - vector.shape[0])).reshape(rows_local, cols)
    return jnp.tile(block, (row_count, 1))


def body(
    row_count,
    tokens,
    norm1_gain,
    norm1_bias,
    qkv_weight,
    query_bias,
    value_bias,
    proj_weight,
    proj_bias,
    norm2_gain,
    norm2_bias,
    gate_weight,
    gate_bias,
    up_weight,
    up_bias,
    inner_gain,
    inner_bias,
    down_weight,
    down_bias,
    cotangent,
):
    single = jnp.float32
    narrow = jnp.bfloat16
    local_rows = tokens.shape[0]
    half_width = tokens.shape[1]
    rows_local = norm1_gain.shape[0]
    model_width = rows_local * row_count
    ff_local = gate_weight.shape[1]
    head_local = half_width // HD
    images_local = local_rows // SEQ
    column = lax.axis_index("col")
    scaling = 1.0 / math.sqrt(HD)
    cosine_table, sine_table = rotary_tables(local_rows, SEQ, GRID, HD)

    def by_head(array):
        shaped = array.reshape(images_local, SEQ, head_local, HD).transpose(0, 2, 1, 3)
        return shaped.reshape(images_local * head_local, SEQ, HD)

    def from_head(array):
        shaped = array.reshape(images_local, head_local, SEQ, HD).transpose(0, 2, 1, 3)
        return shaped.reshape(local_rows, half_width)

    attn_pack, attn_at = pack(
        [
            qkv_weight.reshape(rows_local, 3 * half_width),
            proj_weight.T,
            jnp.stack([norm1_gain, norm1_bias, proj_bias], axis=1),
        ]
    )
    attn_full = lax.all_gather(attn_pack, "row", axis=0, tiled=True)
    qkv_full = attn_full[:, attn_at[0] : attn_at[0] + 3 * half_width].reshape(
        model_width, 3, half_width
    )
    proj_t = attn_full[:, attn_at[1] : attn_at[1] + half_width]
    attn_vectors = attn_full[:, attn_at[2] : attn_at[2] + 3].astype(single)

    whole_input = gather_columns(tokens).astype(single)
    normed_out, normed_one, inv_std_one = norm_forward(
        whole_input, attn_vectors[:, 0], attn_vectors[:, 1]
    )
    first_input = normed_out.astype(narrow)
    qkv_bias = jnp.stack(
        [query_bias.astype(single), jnp.zeros((half_width,), single), value_bias.astype(single)]
    )
    projected = (
        jnp.einsum("td,dpe->tpe", first_input, qkv_full, preferred_element_type=single) + qkv_bias
    )
    queries = apply_rotary(
        projected[:, 0].reshape(local_rows, head_local, HD), cosine_table, sine_table
    ).astype(narrow)
    keys_all = apply_rotary(
        projected[:, 1].reshape(local_rows, head_local, HD), cosine_table, sine_table
    ).astype(narrow)
    values_all = projected[:, 2].astype(narrow)

    def attend(operands):
        query_block, key_block, value_block = operands
        scores = (
            jnp.einsum("qd,kd->qk", query_block, key_block, preferred_element_type=single) * scaling
        )
        weights = jax.nn.softmax(scores, axis=-1)
        mixed = jnp.einsum(
            "qk,kd->qd", weights.astype(narrow), value_block, preferred_element_type=single
        )
        return mixed.astype(narrow)

    attended = from_head(
        lax.map(attend, (by_head(queries), by_head(keys_all), by_head(values_all)))
    )
    attn_partial = jnp.einsum("te,de->td", attended, proj_t, preferred_element_type=single)
    residual_half = (
        tokens.astype(single)
        + share_columns(attn_partial)
        + own_half(attn_vectors[:, 2], column, half_width)
    )
    residual_full = gather_columns(residual_half.astype(jnp.bfloat16)).astype(residual_half.dtype)

    ffn_pack, ffn_at = pack(
        [
            gate_weight,
            up_weight,
            down_weight.T,
            jnp.stack([norm2_gain, norm2_bias, down_bias], axis=1),
        ]
    )
    ffn_full = lax.all_gather(ffn_pack, "row", axis=0, tiled=True)
    gate_full = ffn_full[:, ffn_at[0] : ffn_at[0] + ff_local]
    up_full = ffn_full[:, ffn_at[1] : ffn_at[1] + ff_local]
    down_t = ffn_full[:, ffn_at[2] : ffn_at[2] + ff_local]
    ffn_vectors = ffn_full[:, ffn_at[3] : ffn_at[3] + 3].astype(single)

    second_out, normed_two, inv_std_two = norm_forward(
        residual_full, ffn_vectors[:, 0], ffn_vectors[:, 1]
    )
    second_input = second_out.astype(narrow)
    gate_value = jnp.dot(second_input, gate_full, preferred_element_type=single) + gate_bias.astype(
        single
    )
    up_value = jnp.dot(second_input, up_full, preferred_element_type=single) + up_bias.astype(
        single
    )
    sigmoid_gate = jax.nn.sigmoid(gate_value)
    hidden = gate_value * sigmoid_gate * up_value
    hidden_mean = hidden_totals((jnp.sum(hidden, axis=1),))[0][:, None] / FF
    hidden_centred = hidden - hidden_mean
    hidden_var = hidden_totals((jnp.sum(hidden_centred * hidden_centred, axis=1),))[0][:, None] / FF
    hidden_inv = lax.rsqrt(hidden_var + EPSILON)
    hidden_normed = hidden_centred * hidden_inv
    down_input = (hidden_normed * inner_gain.astype(single) + inner_bias.astype(single)).astype(
        narrow
    )
    ffn_partial = jnp.einsum("tf,df->td", down_input, down_t, preferred_element_type=single)
    layer_out = (
        residual_half
        + share_columns(ffn_partial)
        + own_half(ffn_vectors[:, 2], column, half_width)
    ).astype(narrow)
    out_full = gather_columns(cotangent)
    out_float = out_full.astype(single)
    down_weight_grad_t = jnp.einsum(
        "td,tf->df", out_full, down_input, preferred_element_type=single
    )
    down_bias_grad = jnp.sum(out_float, axis=0)
    normed_grad = jnp.einsum("td,df->tf", out_full, down_t, preferred_element_type=single)
    scaled_grad = normed_grad * inner_gain.astype(single)
    first_total, second_total = hidden_totals(
        (jnp.sum(scaled_grad, axis=1), jnp.sum(scaled_grad * hidden_normed, axis=1))
    )
    hidden_grad = hidden_inv * (
        scaled_grad - first_total[:, None] / FF - hidden_normed * (second_total[:, None] / FF)
    )
    inner_gain_grad = jnp.sum(normed_grad * hidden_normed, axis=0)
    inner_bias_grad = jnp.sum(normed_grad, axis=0)
    gate_grad = (
        hidden_grad * up_value * sigmoid_gate * (1.0 + gate_value * (1.0 - sigmoid_gate))
    ).astype(narrow)
    up_grad = (hidden_grad * gate_value * sigmoid_gate).astype(narrow)
    gate_bias_grad = jnp.sum(gate_grad.astype(single), axis=0)
    up_bias_grad = jnp.sum(up_grad.astype(single), axis=0)
    gate_weight_grad = jnp.einsum(
        "td,tf->df", second_input, gate_grad, preferred_element_type=single
    )
    up_weight_grad = jnp.einsum("td,tf->df", second_input, up_grad, preferred_element_type=single)
    second_back = join_columns(
        jnp.einsum("tf,df->td", gate_grad, gate_full, preferred_element_type=single)
        + jnp.einsum("tf,df->td", up_grad, up_full, preferred_element_type=single)
    )
    second_delta, gain_two_grad, shift_two_grad = norm_backward(
        second_back, normed_two, inv_std_two, ffn_vectors[:, 0]
    )
    residual_grad = out_float + second_delta
    attn_grad = residual_grad.astype(narrow)
    proj_bias_grad = jnp.sum(attn_grad.astype(single), axis=0)
    proj_weight_grad_t = jnp.einsum(
        "td,te->de", attn_grad, attended, preferred_element_type=single
    )
    mid_small = jnp.concatenate([gate_bias_grad, up_bias_grad, inner_gain_grad, inner_bias_grad])
    mid_pack, mid_at = pack(
        [
            gate_weight_grad.astype(narrow),
            up_weight_grad.astype(narrow),
            down_weight_grad_t.astype(narrow),
            proj_weight_grad_t.astype(narrow),
            jnp.stack(
                [gain_two_grad, shift_two_grad, down_bias_grad, proj_bias_grad], axis=1
            ).astype(narrow),
            spread(mid_small, rows_local, row_count).astype(narrow),
        ]
    )
    mid_pack, attn_grad_held = lax.optimization_barrier((mid_pack, attn_grad))
    mid_sums = lax.psum_scatter(mid_pack, "row", scatter_dimension=0, tiled=True).astype(single)
    attended_grad = jnp.einsum(
        "td,de->te", attn_grad_held, proj_t, preferred_element_type=single
    ).astype(narrow)

    def attend_back(operands):
        query_block, key_block, value_block, grad_block = operands
        scores = (
            jnp.einsum("qd,kd->qk", query_block, key_block, preferred_element_type=single) * scaling
        )
        weights = jax.nn.softmax(scores, axis=-1)
        value_grad = jnp.einsum(
            "qk,qd->kd", weights.astype(narrow), grad_block, preferred_element_type=single
        )
        weight_grad = jnp.einsum(
            "qd,kd->qk", grad_block, value_block, preferred_element_type=single
        )
        score_grad = (
            weights * (weight_grad - jnp.sum(weight_grad * weights, axis=-1, keepdims=True))
        ).astype(narrow)
        query_grad = (
            jnp.einsum("qk,kd->qd", score_grad, key_block, preferred_element_type=single) * scaling
        )
        key_grad = (
            jnp.einsum("qk,qd->kd", score_grad, query_block, preferred_element_type=single)
            * scaling
        )
        return (query_grad, key_grad, value_grad)

    query_grads, key_grads, value_grads = lax.map(
        attend_back,
        (by_head(queries), by_head(keys_all), by_head(values_all), by_head(attended_grad)),
    )
    query_pre = rotary_back(
        from_head(query_grads).reshape(local_rows, head_local, HD), cosine_table, sine_table
    )
    key_pre = rotary_back(
        from_head(key_grads).reshape(local_rows, head_local, HD), cosine_table, sine_table
    )
    qkv_grad = jnp.stack(
        [
            query_pre.reshape(local_rows, half_width),
            key_pre.reshape(local_rows, half_width),
            from_head(value_grads),
        ],
        axis=1,
    ).astype(narrow)
    qkv_grad_float = qkv_grad.astype(single)
    query_bias_grad = jnp.sum(qkv_grad_float[:, 0], axis=0)
    value_bias_grad = jnp.sum(qkv_grad_float[:, 2], axis=0)
    qkv_weight_grad = jnp.einsum(
        "td,tpe->dpe", first_input, qkv_grad, preferred_element_type=single
    )
    first_back = join_columns(
        jnp.einsum("tpe,dpe->td", qkv_grad, qkv_full, preferred_element_type=single)
    )
    first_delta, gain_one_grad, shift_one_grad = norm_backward(
        first_back, normed_one, inv_std_one, attn_vectors[:, 0]
    )
    input_grad = own_half(residual_grad + first_delta, column, half_width).astype(narrow)
    end_pack, end_at = pack(
        [
            qkv_weight_grad.reshape(model_width, 3 * half_width).astype(narrow),
            jnp.stack([gain_one_grad, shift_one_grad], axis=1).astype(narrow),
            spread(
                jnp.concatenate([query_bias_grad, value_bias_grad]), rows_local, row_count
            ).astype(narrow),
        ]
    )
    end_pack, mid_sums = lax.optimization_barrier((end_pack, mid_sums))
    end_sums = lax.psum_scatter(end_pack, "row", scatter_dimension=0, tiled=True).astype(single)

    def cut(sums, offset, width):
        return sums[:, offset : offset + width]

    mid_vectors = cut(mid_sums, mid_at[4], 4)
    mid_small_sum = cut(mid_sums, mid_at[5], -(-mid_small.shape[0] // rows_local)).reshape(-1)
    end_vectors = cut(end_sums, end_at[1], 2)
    end_small_sum = cut(end_sums, end_at[2], -(-2 * half_width // rows_local)).reshape(-1)
    return (
        layer_out,
        input_grad,
        end_vectors[:, 0],
        end_vectors[:, 1],
        cut(end_sums, end_at[0], 3 * half_width).reshape(rows_local, 3, half_width),
        end_small_sum[:half_width],
        end_small_sum[half_width : 2 * half_width],
        cut(mid_sums, mid_at[3], half_width).T,
        mid_vectors[:, 3],
        mid_vectors[:, 0],
        mid_vectors[:, 1],
        cut(mid_sums, mid_at[0], ff_local),
        mid_small_sum[:ff_local],
        cut(mid_sums, mid_at[1], ff_local),
        mid_small_sum[ff_local : 2 * ff_local],
        mid_small_sum[2 * ff_local : 3 * ff_local],
        mid_small_sum[3 * ff_local : 4 * ff_local],
        cut(mid_sums, mid_at[2], ff_local).T,
        mid_vectors[:, 2],
    )


def solution(mesh):
    placed = (
        P("row", "col"),
        P("row"),
        P("row"),
        P("row", None, "col"),
        P("col"),
        P("col"),
        P("col", "row"),
        P("row"),
        P("row"),
        P("row"),
        P("row", "col"),
        P("col"),
        P("row", "col"),
        P("col"),
        P("col"),
        P("col"),
        P("col", "row"),
        P("row"),
        P("row", "col"),
    )
    return jax.shard_map(
        functools.partial(body, mesh.shape["row"]),
        mesh=mesh,
        in_specs=placed,
        out_specs=(
            P("row", "col"),
            P("row", "col"),
            P("row"),
            P("row"),
            P("row", None, "col"),
            P("col"),
            P("col"),
            P("col", "row"),
            P("row"),
            P("row"),
            P("row"),
            P("row", "col"),
            P("col"),
            P("row", "col"),
            P("col"),
            P("col"),
            P("col"),
            P("col", "row"),
            P("row"),
        ),
        check_vma=False,
    )
```

```python
import functools
import math

import jax
import jax.numpy as jnp
from jax import lax
from jax.sharding import PartitionSpec as P


HD = 64
FF = 2730
GRID = 32
SEQ = 1025


EPSILON = 1e-06


def norm_forward(values, norm_gain, norm_shift):
    row_mean = jnp.mean(values, axis=-1, keepdims=True)
    centred = values - row_mean
    variance = jnp.mean(centred * centred, axis=-1, keepdims=True)
    inv_std = lax.rsqrt(variance + EPSILON)
    normed = centred * inv_std
    return (normed * norm_gain + norm_shift, normed, inv_std)


def norm_backward(upstream, normed, inv_std, norm_gain):
    scaled = upstream * norm_gain
    first_mean = jnp.mean(scaled, axis=-1, keepdims=True)
    second_mean = jnp.mean(scaled * normed, axis=-1, keepdims=True)
    delta = inv_std * (scaled - first_mean - normed * second_mean)
    return (delta, jnp.sum(upstream * normed, axis=0), jnp.sum(upstream, axis=0))


def rotary_tables(length, seq_len, grid_side, head_size):
    quarter = head_size // 4
    position = jnp.arange(length, dtype=jnp.int32) % seq_len
    patch_index = jnp.maximum(position - 1, 0)
    inside = (position > 0).astype(jnp.float32)
    row_pos = (patch_index // grid_side).astype(jnp.float32) * inside
    col_pos = (patch_index % grid_side).astype(jnp.float32) * inside
    frequency = jnp.exp(-math.log(10000.0) * jnp.arange(quarter, dtype=jnp.float32) / quarter)
    row_angle = row_pos[:, None] * frequency[None, :]
    col_angle = col_pos[:, None] * frequency[None, :]
    angles = jnp.concatenate([row_angle, row_angle, col_angle, col_angle], axis=1)
    return (jnp.cos(angles), jnp.sin(angles))


def rotate(values):
    pieces = jnp.split(values, 4, axis=-1)
    return jnp.concatenate([-pieces[1], pieces[0], -pieces[3], pieces[2]], axis=-1)


def rotate_transposed(values):
    pieces = jnp.split(values, 4, axis=-1)
    return jnp.concatenate([pieces[1], -pieces[0], pieces[3], -pieces[2]], axis=-1)


def apply_rotary(values, cosine_table, sine_table):
    return values * cosine_table[:, None, :] + rotate(values) * sine_table[:, None, :]


def rotary_back(grads, cosine_table, sine_table):
    return grads * cosine_table[:, None, :] + rotate_transposed(grads * sine_table[:, None, :])


def own_half(vector, column, half_width):
    return lax.dynamic_slice_in_dim(vector, column * half_width, half_width, axis=vector.ndim - 1)


def swap_columns(values):
    return lax.ppermute(values, "col", [(0, 1), (1, 0)])


def share_columns(partial_sums):
    half = partial_sums.shape[1] // 2
    column = lax.axis_index("col")
    own = lax.dynamic_slice_in_dim(partial_sums, column * half, half, axis=1)
    other = lax.dynamic_slice_in_dim(partial_sums, (1 - column) * half, half, axis=1)
    return own + swap_columns(other.astype(jnp.bfloat16)).astype(jnp.float32)


def join_columns(partial_sums):
    narrow = partial_sums.astype(jnp.bfloat16)
    return narrow.astype(jnp.float32) + swap_columns(narrow).astype(jnp.float32)


def gather_columns(values):
    other = swap_columns(values)
    first = lax.axis_index("col") == 0
    return jnp.concatenate(
        [jnp.where(first, values, other), jnp.where(first, other, values)], axis=1
    )


def hidden_totals(row_sums):
    return tuple(part + swap_columns(part) for part in row_sums)


def lane_round(width):
    return -(-width // 128) * 128


def pack(pieces):
    offsets = []
    padded = []
    position = 0
    for piece in pieces:
        width = lane_round(piece.shape[1])
        offsets.append(position)
        padded.append(jnp.pad(piece, ((0, 0), (0, width - piece.shape[1]))))
        position += width
    return jnp.concatenate(padded, axis=1), offsets


def spread(vector, rows_local, row_count):
    cols = -(-vector.shape[0] // rows_local)
    block = jnp.pad(vector, (0, rows_local * cols - vector.shape[0])).reshape(rows_local, cols)
    return jnp.tile(block, (row_count, 1))


def body(
    row_count,
    tokens,
    norm1_gain,
    norm1_bias,
    qkv_weight,
    query_bias,
    value_bias,
    proj_weight,
    proj_bias,
    norm2_gain,
    norm2_bias,
    gate_weight,
    gate_bias,
    up_weight,
    up_bias,
    inner_gain,
    inner_bias,
    down_weight,
    down_bias,
    cotangent,
):
    single = jnp.float32
    narrow = jnp.bfloat16
    local_rows = tokens.shape[0]
    half_width = tokens.shape[1]
    rows_local = norm1_gain.shape[0]
    model_width = rows_local * row_count
    ff_local = gate_weight.shape[1]
    head_local = half_width // HD
    images_local = local_rows // SEQ
    column = lax.axis_index("col")
    scaling = 1.0 / math.sqrt(HD)
    cosine_table, sine_table = rotary_tables(local_rows, SEQ, GRID, HD)

    def by_head(array):
        shaped = array.reshape(images_local, SEQ, head_local, HD).transpose(0, 2, 1, 3)
        return shaped.reshape(images_local * head_local, SEQ, HD)

    def from_head(array):
        shaped = array.reshape(images_local, head_local, SEQ, HD).transpose(0, 2, 1, 3)
        return shaped.reshape(local_rows, half_width)

    attn_pack, attn_at = pack(
        [
            qkv_weight.reshape(rows_local, 3 * half_width),
            proj_weight.T,
            jnp.stack([norm1_gain, norm1_bias, proj_bias], axis=1),
        ]
    )
    attn_full = lax.all_gather(attn_pack, "row", axis=0, tiled=True)
    qkv_full = attn_full[:, attn_at[0] : attn_at[0] + 3 * half_width].reshape(
        model_width, 3, half_width
    )
    proj_t = attn_full[:, attn_at[1] : attn_at[1] + half_width]
    attn_vectors = attn_full[:, attn_at[2] : attn_at[2] + 3].astype(single)

    whole_input = gather_columns(tokens).astype(single)
    normed_out, normed_one, inv_std_one = norm_forward(
        whole_input, attn_vectors[:, 0], attn_vectors[:, 1]
    )
    first_input = normed_out.astype(narrow)
    qkv_bias = jnp.stack(
        [query_bias.astype(single), jnp.zeros((half_width,), single), value_bias.astype(single)]
    )
    projected = (
        jnp.einsum("td,dpe->tpe", first_input, qkv_full, preferred_element_type=single) + qkv_bias
    )
    queries = apply_rotary(
        projected[:, 0].reshape(local_rows, head_local, HD), cosine_table, sine_table
    ).astype(narrow)
    keys_all = apply_rotary(
        projected[:, 1].reshape(local_rows, head_local, HD), cosine_table, sine_table
    ).astype(narrow)
    values_all = projected[:, 2].astype(narrow)

    def attend(operands):
        query_block, key_block, value_block = operands
        scores = (
            jnp.einsum("qd,kd->qk", query_block, key_block, preferred_element_type=single) * scaling
        )
        weights = jax.nn.softmax(scores, axis=-1)
        mixed = jnp.einsum(
            "qk,kd->qd", weights.astype(narrow), value_block, preferred_element_type=single
        )
        return mixed.astype(narrow)

    attended = from_head(
        lax.map(attend, (by_head(queries), by_head(keys_all), by_head(values_all)))
    )
    attn_partial = jnp.einsum("te,de->td", attended, proj_t, preferred_element_type=single)
    residual_half = (
        tokens.astype(single)
        + share_columns(attn_partial)
        + own_half(attn_vectors[:, 2], column, half_width)
    )
    residual_full = gather_columns(residual_half.astype(jnp.bfloat16)).astype(residual_half.dtype)

    ffn_pack, ffn_at = pack(
        [
            gate_weight,
            up_weight,
            down_weight.T,
            jnp.stack([norm2_gain, norm2_bias, down_bias], axis=1),
        ]
    )
    ffn_full = lax.all_gather(ffn_pack, "row", axis=0, tiled=True)
    gate_full = ffn_full[:, ffn_at[0] : ffn_at[0] + ff_local]
    up_full = ffn_full[:, ffn_at[1] : ffn_at[1] + ff_local]
    down_t = ffn_full[:, ffn_at[2] : ffn_at[2] + ff_local]
    ffn_vectors = ffn_full[:, ffn_at[3] : ffn_at[3] + 3].astype(single)

    second_out, normed_two, inv_std_two = norm_forward(
        residual_full, ffn_vectors[:, 0], ffn_vectors[:, 1]
    )
    second_input = second_out.astype(narrow)
    gate_value = jnp.dot(second_input, gate_full, preferred_element_type=single) + gate_bias.astype(
        single
    )
    up_value = jnp.dot(second_input, up_full, preferred_element_type=single) + up_bias.astype(
        single
    )
    sigmoid_gate = jax.nn.sigmoid(gate_value)
    hidden = gate_value * sigmoid_gate * up_value
    hidden_mean = hidden_totals((jnp.sum(hidden, axis=1),))[0][:, None] / FF
    hidden_centred = hidden - hidden_mean
    hidden_var = hidden_totals((jnp.sum(hidden_centred * hidden_centred, axis=1),))[0][:, None] / FF
    hidden_inv = lax.rsqrt(hidden_var + EPSILON)
    hidden_normed = hidden_centred * hidden_inv
    down_input = (hidden_normed * inner_gain.astype(single) + inner_bias.astype(single)).astype(
        narrow
    )
    ffn_partial = jnp.einsum("tf,df->td", down_input, down_t, preferred_element_type=single)
    layer_out = (
        residual_half
        + share_columns(ffn_partial)
        + own_half(ffn_vectors[:, 2], column, half_width)
    ).astype(narrow)
    out_full = gather_columns(cotangent)
    out_float = out_full.astype(single)
    down_weight_grad_t = jnp.einsum(
        "td,tf->df", out_full, down_input, preferred_element_type=single
    )
    down_bias_grad = jnp.sum(out_float, axis=0)
    normed_grad = jnp.einsum("td,df->tf", out_full, down_t, preferred_element_type=single)
    scaled_grad = normed_grad * inner_gain.astype(single)
    first_total, second_total = hidden_totals(
        (jnp.sum(scaled_grad, axis=1), jnp.sum(scaled_grad * hidden_normed, axis=1))
    )
    hidden_grad = hidden_inv * (
        scaled_grad - first_total[:, None] / FF - hidden_normed * (second_total[:, None] / FF)
    )
    inner_gain_grad = jnp.sum(normed_grad * hidden_normed, axis=0)
    inner_bias_grad = jnp.sum(normed_grad, axis=0)
    gate_grad = (
        hidden_grad * up_value * sigmoid_gate * (1.0 + gate_value * (1.0 - sigmoid_gate))
    ).astype(narrow)
    up_grad = (hidden_grad * gate_value * sigmoid_gate).astype(narrow)
    gate_bias_grad = jnp.sum(gate_grad.astype(single), axis=0)
    up_bias_grad = jnp.sum(up_grad.astype(single), axis=0)
    gate_weight_grad = jnp.einsum(
        "td,tf->df", second_input, gate_grad, preferred_element_type=single
    )
    up_weight_grad = jnp.einsum("td,tf->df", second_input, up_grad, preferred_element_type=single)
    mid_small = jnp.concatenate([gate_bias_grad, up_bias_grad, inner_gain_grad, inner_bias_grad])
    mid_pack, mid_at = pack(
        [
            gate_weight_grad.astype(narrow),
            up_weight_grad.astype(narrow),
            down_weight_grad_t.astype(narrow),
            jnp.concatenate(
                [down_bias_grad[:, None], spread(mid_small, rows_local, row_count)], axis=1
            ).astype(narrow),
        ]
    )
    mid_pack, gate_grad, up_grad = lax.optimization_barrier((mid_pack, gate_grad, up_grad))
    mid_sums = lax.psum_scatter(mid_pack, "row", scatter_dimension=0, tiled=True).astype(single)
    second_back = join_columns(
        jnp.einsum("tf,df->td", gate_grad, gate_full, preferred_element_type=single)
        + jnp.einsum("tf,df->td", up_grad, up_full, preferred_element_type=single)
    )
    second_delta, gain_two_grad, shift_two_grad = norm_backward(
        second_back, normed_two, inv_std_two, ffn_vectors[:, 0]
    )
    residual_grad = out_float + second_delta
    attn_grad = residual_grad.astype(narrow)
    proj_bias_grad = jnp.sum(attn_grad.astype(single), axis=0)
    proj_weight_grad_t = jnp.einsum(
        "td,te->de", attn_grad, attended, preferred_element_type=single
    )
    attended_grad = jnp.einsum(
        "td,de->te", attn_grad, proj_t, preferred_element_type=single
    ).astype(narrow)

    def attend_back(operands):
        query_block, key_block, value_block, grad_block = operands
        scores = (
            jnp.einsum("qd,kd->qk", query_block, key_block, preferred_element_type=single) * scaling
        )
        weights = jax.nn.softmax(scores, axis=-1)
        value_grad = jnp.einsum(
            "qk,qd->kd", weights.astype(narrow), grad_block, preferred_element_type=single
        )
        weight_grad = jnp.einsum(
            "qd,kd->qk", grad_block, value_block, preferred_element_type=single
        )
        score_grad = (
            weights * (weight_grad - jnp.sum(weight_grad * weights, axis=-1, keepdims=True))
        ).astype(narrow)
        query_grad = (
            jnp.einsum("qk,kd->qd", score_grad, key_block, preferred_element_type=single) * scaling
        )
        key_grad = (
            jnp.einsum("qk,qd->kd", score_grad, query_block, preferred_element_type=single)
            * scaling
        )
        return (query_grad, key_grad, value_grad)

    query_grads, key_grads, value_grads = lax.map(
        attend_back,
        (by_head(queries), by_head(keys_all), by_head(values_all), by_head(attended_grad)),
    )
    query_pre = rotary_back(
        from_head(query_grads).reshape(local_rows, head_local, HD), cosine_table, sine_table
    )
    key_pre = rotary_back(
        from_head(key_grads).reshape(local_rows, head_local, HD), cosine_table, sine_table
    )
    qkv_grad = jnp.stack(
        [
            query_pre.reshape(local_rows, half_width),
            key_pre.reshape(local_rows, half_width),
            from_head(value_grads),
        ],
        axis=1,
    ).astype(narrow)
    qkv_grad_float = qkv_grad.astype(single)
    query_bias_grad = jnp.sum(qkv_grad_float[:, 0], axis=0)
    value_bias_grad = jnp.sum(qkv_grad_float[:, 2], axis=0)
    qkv_weight_grad = jnp.einsum(
        "td,tpe->dpe", first_input, qkv_grad, preferred_element_type=single
    )
    first_back = join_columns(
        jnp.einsum("tpe,dpe->td", qkv_grad, qkv_full, preferred_element_type=single)
    )
    first_delta, gain_one_grad, shift_one_grad = norm_backward(
        first_back, normed_one, inv_std_one, attn_vectors[:, 0]
    )
    input_grad = own_half(residual_grad + first_delta, column, half_width).astype(narrow)
    end_pack, end_at = pack(
        [
            qkv_weight_grad.reshape(model_width, 3 * half_width).astype(narrow),
            proj_weight_grad_t.astype(narrow),
            jnp.concatenate(
                [
                    jnp.stack(
                        [gain_one_grad, shift_one_grad, proj_bias_grad, gain_two_grad, shift_two_grad],
                        axis=1,
                    ),
                    spread(
                        jnp.concatenate([query_bias_grad, value_bias_grad]), rows_local, row_count
                    ),
                ],
                axis=1,
            ).astype(narrow),
        ]
    )
    end_pack, mid_sums = lax.optimization_barrier((end_pack, mid_sums))
    end_sums = lax.psum_scatter(end_pack, "row", scatter_dimension=0, tiled=True).astype(single)

    def cut(sums, offset, width):
        return sums[:, offset : offset + width]

    mid_tail = cut(mid_sums, mid_at[3], 1 + -(-mid_small.shape[0] // rows_local))
    mid_small_sum = mid_tail[:, 1:].reshape(-1)
    end_tail = cut(end_sums, end_at[2], 5 + -(-2 * half_width // rows_local))
    end_small_sum = end_tail[:, 5:].reshape(-1)
    return (
        layer_out,
        input_grad,
        end_tail[:, 0],
        end_tail[:, 1],
        cut(end_sums, end_at[0], 3 * half_width).reshape(rows_local, 3, half_width),
        end_small_sum[:half_width],
        end_small_sum[half_width : 2 * half_width],
        cut(end_sums, end_at[1], half_width).T,
        end_tail[:, 2],
        end_tail[:, 3],
        end_tail[:, 4],
        cut(mid_sums, mid_at[0], ff_local),
        mid_small_sum[:ff_local],
        cut(mid_sums, mid_at[1], ff_local),
        mid_small_sum[ff_local : 2 * ff_local],
        mid_small_sum[2 * ff_local : 3 * ff_local],
        mid_small_sum[3 * ff_local : 4 * ff_local],
        cut(mid_sums, mid_at[2], ff_local).T,
        mid_tail[:, 0],
    )


def solution(mesh):
    placed = (
        P("row", "col"),
        P("row"),
        P("row"),
        P("row", None, "col"),
        P("col"),
        P("col"),
        P("col", "row"),
        P("row"),
        P("row"),
        P("row"),
        P("row", "col"),
        P("col"),
        P("row", "col"),
        P("col"),
        P("col"),
        P("col"),
        P("col", "row"),
        P("row"),
        P("row", "col"),
    )
    return jax.shard_map(
        functools.partial(body, mesh.shape["row"]),
        mesh=mesh,
        in_specs=placed,
        out_specs=(
            P("row", "col"),
            P("row", "col"),
            P("row"),
            P("row"),
            P("row", None, "col"),
            P("col"),
            P("col"),
            P("col", "row"),
            P("row"),
            P("row"),
            P("row"),
            P("row", "col"),
            P("col"),
            P("row", "col"),
            P("col"),
            P("col"),
            P("col"),
            P("col", "row"),
            P("row"),
        ),
        check_vma=False,
    )
```

```python
import functools
import math

import jax
import jax.numpy as jnp
from jax import lax
from jax.experimental.layout import Layout, with_layout_constraint
from jax.sharding import PartitionSpec as P


HD = 64
FF = 2730
GRID = 32
SEQ = 1025


EPSILON = 1e-06


def norm_forward(values, norm_gain, norm_shift):
    row_mean = jnp.mean(values, axis=-1, keepdims=True)
    centred = values - row_mean
    variance = jnp.mean(centred * centred, axis=-1, keepdims=True)
    inv_std = lax.rsqrt(variance + EPSILON)
    normed = centred * inv_std
    return (normed * norm_gain + norm_shift, normed, inv_std)


def norm_backward(upstream, normed, inv_std, norm_gain):
    scaled = upstream * norm_gain
    first_mean = jnp.mean(scaled, axis=-1, keepdims=True)
    second_mean = jnp.mean(scaled * normed, axis=-1, keepdims=True)
    delta = inv_std * (scaled - first_mean - normed * second_mean)
    return (delta, jnp.sum(upstream * normed, axis=0), jnp.sum(upstream, axis=0))


def rotary_tables(length, seq_len, grid_side, head_size):
    quarter = head_size // 4
    position = jnp.arange(length, dtype=jnp.int32) % seq_len
    patch_index = jnp.maximum(position - 1, 0)
    inside = (position > 0).astype(jnp.float32)
    row_pos = (patch_index // grid_side).astype(jnp.float32) * inside
    col_pos = (patch_index % grid_side).astype(jnp.float32) * inside
    frequency = jnp.exp(-math.log(10000.0) * jnp.arange(quarter, dtype=jnp.float32) / quarter)
    row_angle = row_pos[:, None] * frequency[None, :]
    col_angle = col_pos[:, None] * frequency[None, :]
    angles = jnp.concatenate([row_angle, row_angle, col_angle, col_angle], axis=1)
    return (jnp.cos(angles), jnp.sin(angles))


def rotate(values):
    pieces = jnp.split(values, 4, axis=-1)
    return jnp.concatenate([-pieces[1], pieces[0], -pieces[3], pieces[2]], axis=-1)


def rotate_transposed(values):
    pieces = jnp.split(values, 4, axis=-1)
    return jnp.concatenate([pieces[1], -pieces[0], pieces[3], -pieces[2]], axis=-1)


def apply_rotary(values, cosine_table, sine_table):
    return values * cosine_table[:, None, :] + rotate(values) * sine_table[:, None, :]


def rotary_back(grads, cosine_table, sine_table):
    return grads * cosine_table[:, None, :] + rotate_transposed(grads * sine_table[:, None, :])


def own_half(vector, column, half_width):
    return lax.dynamic_slice_in_dim(vector, column * half_width, half_width, axis=vector.ndim - 1)


def swap_columns(values):
    return lax.ppermute(values, "col", [(0, 1), (1, 0)])


def share_columns(partial_sums):
    half = partial_sums.shape[1] // 2
    column = lax.axis_index("col")
    own = lax.dynamic_slice_in_dim(partial_sums, column * half, half, axis=1)
    other = lax.dynamic_slice_in_dim(partial_sums, (1 - column) * half, half, axis=1)
    return own + swap_columns(other.astype(jnp.bfloat16)).astype(jnp.float32)


def join_columns(partial_sums):
    narrow = partial_sums.astype(jnp.bfloat16)
    return narrow.astype(jnp.float32) + swap_columns(narrow).astype(jnp.float32)


def gather_columns(values):
    other = swap_columns(values)
    first = lax.axis_index("col") == 0
    return jnp.concatenate(
        [jnp.where(first, values, other), jnp.where(first, other, values)], axis=1
    )


def hidden_totals(row_sums):
    return tuple(part + swap_columns(part) for part in row_sums)


def row_major(values):
    return with_layout_constraint(values, Layout((0, 1)))


def lane_round(width):
    return -(-width // 128) * 128


def pack(pieces):
    offsets = []
    padded = []
    position = 0
    for piece in pieces:
        width = lane_round(piece.shape[1])
        offsets.append(position)
        padded.append(jnp.pad(piece, ((0, 0), (0, width - piece.shape[1]))))
        position += width
    return jnp.concatenate(padded, axis=1), offsets


def spread(vector, rows_local, row_count):
    cols = -(-vector.shape[0] // rows_local)
    block = jnp.pad(vector, (0, rows_local * cols - vector.shape[0])).reshape(rows_local, cols)
    return jnp.tile(block, (row_count, 1))


def body(
    row_count,
    tokens,
    norm1_gain,
    norm1_bias,
    qkv_weight,
    query_bias,
    value_bias,
    proj_weight,
    proj_bias,
    norm2_gain,
    norm2_bias,
    gate_weight,
    gate_bias,
    up_weight,
    up_bias,
    inner_gain,
    inner_bias,
    down_weight,
    down_bias,
    cotangent,
):
    single = jnp.float32
    narrow = jnp.bfloat16
    local_rows = tokens.shape[0]
    half_width = tokens.shape[1]
    rows_local = norm1_gain.shape[0]
    model_width = rows_local * row_count
    ff_local = gate_weight.shape[1]
    head_local = half_width // HD
    images_local = local_rows // SEQ
    column = lax.axis_index("col")
    scaling = 1.0 / math.sqrt(HD)
    cosine_table, sine_table = rotary_tables(local_rows, SEQ, GRID, HD)

    def by_head(array):
        shaped = array.reshape(images_local, SEQ, head_local, HD).transpose(0, 2, 1, 3)
        return shaped.reshape(images_local * head_local, SEQ, HD)

    def from_head(array):
        shaped = array.reshape(images_local, head_local, SEQ, HD).transpose(0, 2, 1, 3)
        return shaped.reshape(local_rows, half_width)

    attn_pack, attn_at = pack(
        [
            qkv_weight.reshape(rows_local, 3 * half_width),
            proj_weight.T,
            jnp.stack([norm1_gain, norm1_bias, proj_bias], axis=1),
        ]
    )
    attn_full = lax.all_gather(attn_pack, "row", axis=0, tiled=True)
    qkv_full = attn_full[:, attn_at[0] : attn_at[0] + 3 * half_width].reshape(
        model_width, 3, half_width
    )
    proj_t = attn_full[:, attn_at[1] : attn_at[1] + half_width]
    attn_vectors = attn_full[:, attn_at[2] : attn_at[2] + 3].astype(single)

    whole_input = gather_columns(tokens).astype(single)
    normed_out, normed_one, inv_std_one = norm_forward(
        whole_input, attn_vectors[:, 0], attn_vectors[:, 1]
    )
    first_input = normed_out.astype(narrow)
    qkv_bias = jnp.stack(
        [query_bias.astype(single), jnp.zeros((half_width,), single), value_bias.astype(single)]
    )
    projected = (
        jnp.einsum("td,dpe->tpe", first_input, qkv_full, preferred_element_type=single) + qkv_bias
    )
    queries = apply_rotary(
        projected[:, 0].reshape(local_rows, head_local, HD), cosine_table, sine_table
    ).astype(narrow)
    keys_all = apply_rotary(
        projected[:, 1].reshape(local_rows, head_local, HD), cosine_table, sine_table
    ).astype(narrow)
    values_all = projected[:, 2].astype(narrow)

    def attend(operands):
        query_block, key_block, value_block = operands
        scores = (
            jnp.einsum("qd,kd->qk", query_block, key_block, preferred_element_type=single) * scaling
        )
        weights = jax.nn.softmax(scores, axis=-1)
        mixed = jnp.einsum(
            "qk,kd->qd", weights.astype(narrow), value_block, preferred_element_type=single
        )
        return mixed.astype(narrow)

    attended = from_head(
        lax.map(attend, (by_head(queries), by_head(keys_all), by_head(values_all)))
    )
    attn_partial = jnp.einsum("te,de->td", attended, proj_t, preferred_element_type=single)
    residual_half = (
        tokens.astype(single)
        + share_columns(attn_partial)
        + own_half(attn_vectors[:, 2], column, half_width)
    )
    residual_full = gather_columns(residual_half.astype(jnp.bfloat16)).astype(residual_half.dtype)

    ffn_pack, ffn_at = pack(
        [
            gate_weight,
            up_weight,
            down_weight.T,
            jnp.stack([norm2_gain, norm2_bias, down_bias], axis=1),
        ]
    )
    ffn_full = lax.all_gather(ffn_pack, "row", axis=0, tiled=True)
    gate_full = ffn_full[:, ffn_at[0] : ffn_at[0] + ff_local]
    up_full = ffn_full[:, ffn_at[1] : ffn_at[1] + ff_local]
    down_t = ffn_full[:, ffn_at[2] : ffn_at[2] + ff_local]
    ffn_vectors = ffn_full[:, ffn_at[3] : ffn_at[3] + 3].astype(single)

    second_out, normed_two, inv_std_two = norm_forward(
        residual_full, ffn_vectors[:, 0], ffn_vectors[:, 1]
    )
    second_input = second_out.astype(narrow)
    gate_value = jnp.dot(second_input, gate_full, preferred_element_type=single) + gate_bias.astype(
        single
    )
    up_value = jnp.dot(second_input, up_full, preferred_element_type=single) + up_bias.astype(
        single
    )
    sigmoid_gate = jax.nn.sigmoid(gate_value)
    hidden = gate_value * sigmoid_gate * up_value
    hidden_mean = hidden_totals((jnp.sum(hidden, axis=1),))[0][:, None] / FF
    hidden_centred = hidden - hidden_mean
    hidden_var = hidden_totals((jnp.sum(hidden_centred * hidden_centred, axis=1),))[0][:, None] / FF
    hidden_inv = lax.rsqrt(hidden_var + EPSILON)
    hidden_normed = hidden_centred * hidden_inv
    down_input = (hidden_normed * inner_gain.astype(single) + inner_bias.astype(single)).astype(
        narrow
    )
    ffn_partial = jnp.einsum("tf,df->td", down_input, down_t, preferred_element_type=single)
    layer_out = (
        residual_half
        + share_columns(ffn_partial)
        + own_half(ffn_vectors[:, 2], column, half_width)
    ).astype(narrow)
    out_full = gather_columns(cotangent)
    out_float = out_full.astype(single)
    down_weight_grad_t = jnp.einsum(
        "td,tf->df", out_full, down_input, preferred_element_type=single
    )
    down_bias_grad = jnp.sum(out_float, axis=0)
    normed_grad = jnp.einsum("td,df->tf", out_full, down_t, preferred_element_type=single)
    scaled_grad = normed_grad * inner_gain.astype(single)
    first_total, second_total = hidden_totals(
        (jnp.sum(scaled_grad, axis=1), jnp.sum(scaled_grad * hidden_normed, axis=1))
    )
    hidden_grad = hidden_inv * (
        scaled_grad - first_total[:, None] / FF - hidden_normed * (second_total[:, None] / FF)
    )
    inner_gain_grad = jnp.sum(normed_grad * hidden_normed, axis=0)
    inner_bias_grad = jnp.sum(normed_grad, axis=0)
    gate_grad = (
        hidden_grad * up_value * sigmoid_gate * (1.0 + gate_value * (1.0 - sigmoid_gate))
    ).astype(narrow)
    up_grad = (hidden_grad * gate_value * sigmoid_gate).astype(narrow)
    gate_bias_grad = jnp.sum(gate_grad.astype(single), axis=0)
    up_bias_grad = jnp.sum(up_grad.astype(single), axis=0)
    gate_weight_grad = jnp.einsum(
        "td,tf->df", second_input, gate_grad, preferred_element_type=single
    )
    up_weight_grad = jnp.einsum("td,tf->df", second_input, up_grad, preferred_element_type=single)
    second_back = join_columns(
        jnp.einsum("tf,df->td", gate_grad, gate_full, preferred_element_type=single)
        + jnp.einsum("tf,df->td", up_grad, up_full, preferred_element_type=single)
    )
    second_delta, gain_two_grad, shift_two_grad = norm_backward(
        second_back, normed_two, inv_std_two, ffn_vectors[:, 0]
    )
    residual_grad = out_float + second_delta
    attn_grad = residual_grad.astype(narrow)
    proj_bias_grad = jnp.sum(attn_grad.astype(single), axis=0)
    proj_weight_grad_t = jnp.einsum(
        "td,te->de", attn_grad, attended, preferred_element_type=single
    )
    mid_small = jnp.concatenate([gate_bias_grad, up_bias_grad, inner_gain_grad, inner_bias_grad])
    mid_pack, mid_at = pack(
        [
            row_major(gate_weight_grad.astype(narrow)),
            row_major(up_weight_grad.astype(narrow)),
            row_major(down_weight_grad_t.astype(narrow)),
            row_major(proj_weight_grad_t.astype(narrow)),
            jnp.stack(
                [gain_two_grad, shift_two_grad, down_bias_grad, proj_bias_grad], axis=1
            ).astype(narrow),
            spread(mid_small, rows_local, row_count).astype(narrow),
        ]
    )
    mid_pack, attn_grad_held = lax.optimization_barrier((mid_pack, attn_grad))
    mid_sums = lax.psum_scatter(mid_pack, "row", scatter_dimension=0, tiled=True).astype(single)
    attended_grad = jnp.einsum(
        "td,de->te", attn_grad_held, proj_t, preferred_element_type=single
    ).astype(narrow)

    def attend_back(operands):
        query_block, key_block, value_block, grad_block = operands
        scores = (
            jnp.einsum("qd,kd->qk", query_block, key_block, preferred_element_type=single) * scaling
        )
        weights = jax.nn.softmax(scores, axis=-1)
        value_grad = jnp.einsum(
            "qk,qd->kd", weights.astype(narrow), grad_block, preferred_element_type=single
        )
        weight_grad = jnp.einsum(
            "qd,kd->qk", grad_block, value_block, preferred_element_type=single
        )
        score_grad = (
            weights * (weight_grad - jnp.sum(weight_grad * weights, axis=-1, keepdims=True))
        ).astype(narrow)
        query_grad = (
            jnp.einsum("qk,kd->qd", score_grad, key_block, preferred_element_type=single) * scaling
        )
        key_grad = (
            jnp.einsum("qk,qd->kd", score_grad, query_block, preferred_element_type=single)
            * scaling
        )
        return (query_grad, key_grad, value_grad)

    query_grads, key_grads, value_grads = lax.map(
        attend_back,
        (by_head(queries), by_head(keys_all), by_head(values_all), by_head(attended_grad)),
    )
    query_pre = rotary_back(
        from_head(query_grads).reshape(local_rows, head_local, HD), cosine_table, sine_table
    )
    key_pre = rotary_back(
        from_head(key_grads).reshape(local_rows, head_local, HD), cosine_table, sine_table
    )
    qkv_grad = jnp.stack(
        [
            query_pre.reshape(local_rows, half_width),
            key_pre.reshape(local_rows, half_width),
            from_head(value_grads),
        ],
        axis=1,
    ).astype(narrow)
    qkv_grad_float = qkv_grad.astype(single)
    query_bias_grad = jnp.sum(qkv_grad_float[:, 0], axis=0)
    value_bias_grad = jnp.sum(qkv_grad_float[:, 2], axis=0)
    qkv_weight_grad = jnp.einsum(
        "td,tpe->dpe", first_input, qkv_grad, preferred_element_type=single
    )
    first_back = join_columns(
        jnp.einsum("tpe,dpe->td", qkv_grad, qkv_full, preferred_element_type=single)
    )
    first_delta, gain_one_grad, shift_one_grad = norm_backward(
        first_back, normed_one, inv_std_one, attn_vectors[:, 0]
    )
    input_grad = own_half(residual_grad + first_delta, column, half_width).astype(narrow)
    end_pack, end_at = pack(
        [
            qkv_weight_grad.reshape(model_width, 3 * half_width).astype(narrow),
            jnp.stack([gain_one_grad, shift_one_grad], axis=1).astype(narrow),
            spread(
                jnp.concatenate([query_bias_grad, value_bias_grad]), rows_local, row_count
            ).astype(narrow),
        ]
    )
    end_pack, mid_sums = lax.optimization_barrier((end_pack, mid_sums))
    end_sums = lax.psum_scatter(end_pack, "row", scatter_dimension=0, tiled=True).astype(single)

    def cut(sums, offset, width):
        return sums[:, offset : offset + width]

    mid_vectors = cut(mid_sums, mid_at[4], 4)
    mid_small_sum = cut(mid_sums, mid_at[5], -(-mid_small.shape[0] // rows_local)).reshape(-1)
    end_vectors = cut(end_sums, end_at[1], 2)
    end_small_sum = cut(end_sums, end_at[2], -(-2 * half_width // rows_local)).reshape(-1)
    return (
        layer_out,
        input_grad,
        end_vectors[:, 0],
        end_vectors[:, 1],
        cut(end_sums, end_at[0], 3 * half_width).reshape(rows_local, 3, half_width),
        end_small_sum[:half_width],
        end_small_sum[half_width : 2 * half_width],
        cut(mid_sums, mid_at[3], half_width).T,
        mid_vectors[:, 3],
        mid_vectors[:, 0],
        mid_vectors[:, 1],
        cut(mid_sums, mid_at[0], ff_local),
        mid_small_sum[:ff_local],
        cut(mid_sums, mid_at[1], ff_local),
        mid_small_sum[ff_local : 2 * ff_local],
        mid_small_sum[2 * ff_local : 3 * ff_local],
        mid_small_sum[3 * ff_local : 4 * ff_local],
        cut(mid_sums, mid_at[2], ff_local).T,
        mid_vectors[:, 2],
    )


def solution(mesh):
    placed = (
        P("row", "col"),
        P("row"),
        P("row"),
        P("row", None, "col"),
        P("col"),
        P("col"),
        P("col", "row"),
        P("row"),
        P("row"),
        P("row"),
        P("row", "col"),
        P("col"),
        P("row", "col"),
        P("col"),
        P("col"),
        P("col"),
        P("col", "row"),
        P("row"),
        P("row", "col"),
    )
    return jax.shard_map(
        functools.partial(body, mesh.shape["row"]),
        mesh=mesh,
        in_specs=placed,
        out_specs=(
            P("row", "col"),
            P("row", "col"),
            P("row"),
            P("row"),
            P("row", None, "col"),
            P("col"),
            P("col"),
            P("col", "row"),
            P("row"),
            P("row"),
            P("row"),
            P("row", "col"),
            P("col"),
            P("row", "col"),
            P("col"),
            P("col"),
            P("col"),
            P("col", "row"),
            P("row"),
        ),
        check_vma=False,
    )
```

```python
import functools
import math

import jax
import jax.numpy as jnp
from jax import lax
from jax.experimental.layout import Layout, with_layout_constraint
from jax.sharding import PartitionSpec as P


HD = 64
FF = 2730
GRID = 32
SEQ = 1025


EPSILON = 1e-06


def norm_forward(values, norm_gain, norm_shift):
    row_mean = jnp.mean(values, axis=-1, keepdims=True)
    centred = values - row_mean
    variance = jnp.mean(centred * centred, axis=-1, keepdims=True)
    inv_std = lax.rsqrt(variance + EPSILON)
    normed = centred * inv_std
    return (normed * norm_gain + norm_shift, normed, inv_std)


def norm_backward(upstream, normed, inv_std, norm_gain):
    scaled = upstream * norm_gain
    first_mean = jnp.mean(scaled, axis=-1, keepdims=True)
    second_mean = jnp.mean(scaled * normed, axis=-1, keepdims=True)
    delta = inv_std * (scaled - first_mean - normed * second_mean)
    return (delta, jnp.sum(upstream * normed, axis=0), jnp.sum(upstream, axis=0))


def rotary_tables(length, seq_len, grid_side, head_size):
    quarter = head_size // 4
    position = jnp.arange(length, dtype=jnp.int32) % seq_len
    patch_index = jnp.maximum(position - 1, 0)
    inside = (position > 0).astype(jnp.float32)
    row_pos = (patch_index // grid_side).astype(jnp.float32) * inside
    col_pos = (patch_index % grid_side).astype(jnp.float32) * inside
    frequency = jnp.exp(-math.log(10000.0) * jnp.arange(quarter, dtype=jnp.float32) / quarter)
    row_angle = row_pos[:, None] * frequency[None, :]
    col_angle = col_pos[:, None] * frequency[None, :]
    angles = jnp.concatenate([row_angle, row_angle, col_angle, col_angle], axis=1)
    return (jnp.cos(angles), jnp.sin(angles))


def rotate(values):
    pieces = jnp.split(values, 4, axis=-1)
    return jnp.concatenate([-pieces[1], pieces[0], -pieces[3], pieces[2]], axis=-1)


def rotate_transposed(values):
    pieces = jnp.split(values, 4, axis=-1)
    return jnp.concatenate([pieces[1], -pieces[0], pieces[3], -pieces[2]], axis=-1)


def apply_rotary(values, cosine_table, sine_table):
    return values * cosine_table[:, None, :] + rotate(values) * sine_table[:, None, :]


def rotary_back(grads, cosine_table, sine_table):
    return grads * cosine_table[:, None, :] + rotate_transposed(grads * sine_table[:, None, :])


def own_half(vector, column, half_width):
    return lax.dynamic_slice_in_dim(vector, column * half_width, half_width, axis=vector.ndim - 1)


def swap_columns(values):
    return lax.ppermute(values, "col", [(0, 1), (1, 0)])


def share_columns(partial_sums):
    half = partial_sums.shape[1] // 2
    column = lax.axis_index("col")
    own = lax.dynamic_slice_in_dim(partial_sums, column * half, half, axis=1)
    other = lax.dynamic_slice_in_dim(partial_sums, (1 - column) * half, half, axis=1)
    return own + swap_columns(other.astype(jnp.bfloat16)).astype(jnp.float32)


def join_columns(partial_sums):
    narrow = partial_sums.astype(jnp.bfloat16)
    return narrow.astype(jnp.float32) + swap_columns(narrow).astype(jnp.float32)


def gather_columns(values):
    other = swap_columns(values)
    first = lax.axis_index("col") == 0
    return jnp.concatenate(
        [jnp.where(first, values, other), jnp.where(first, other, values)], axis=1
    )


def hidden_totals(row_sums):
    return tuple(part + swap_columns(part) for part in row_sums)


def row_major(values):
    return with_layout_constraint(values, Layout((0, 1)))


def lane_round(width):
    return -(-width // 128) * 128


def pack(pieces):
    offsets = []
    padded = []
    position = 0
    for piece in pieces:
        width = lane_round(piece.shape[1])
        offsets.append(position)
        padded.append(jnp.pad(piece, ((0, 0), (0, width - piece.shape[1]))))
        position += width
    return jnp.concatenate(padded, axis=1), offsets


def spread(vector, rows_local, row_count):
    cols = -(-vector.shape[0] // rows_local)
    block = jnp.pad(vector, (0, rows_local * cols - vector.shape[0])).reshape(rows_local, cols)
    return jnp.tile(block, (row_count, 1))


def body(
    row_count,
    tokens,
    norm1_gain,
    norm1_bias,
    qkv_weight,
    query_bias,
    value_bias,
    proj_weight,
    proj_bias,
    norm2_gain,
    norm2_bias,
    gate_weight,
    gate_bias,
    up_weight,
    up_bias,
    inner_gain,
    inner_bias,
    down_weight,
    down_bias,
    cotangent,
):
    single = jnp.float32
    narrow = jnp.bfloat16
    local_rows = tokens.shape[0]
    half_width = tokens.shape[1]
    rows_local = norm1_gain.shape[0]
    model_width = rows_local * row_count
    ff_local = gate_weight.shape[1]
    head_local = half_width // HD
    images_local = local_rows // SEQ
    column = lax.axis_index("col")
    scaling = 1.0 / math.sqrt(HD)
    cosine_table, sine_table = rotary_tables(local_rows, SEQ, GRID, HD)

    def by_head(array):
        shaped = array.reshape(images_local, SEQ, head_local, HD).transpose(0, 2, 1, 3)
        return shaped.reshape(images_local * head_local, SEQ, HD)

    def from_head(array):
        shaped = array.reshape(images_local, head_local, SEQ, HD).transpose(0, 2, 1, 3)
        return shaped.reshape(local_rows, half_width)

    attn_pack, attn_at = pack(
        [
            qkv_weight.reshape(rows_local, 3 * half_width),
            proj_weight.T,
            jnp.stack([norm1_gain, norm1_bias, proj_bias], axis=1),
        ]
    )
    attn_full = lax.all_gather(attn_pack, "row", axis=0, tiled=True)
    qkv_full = attn_full[:, attn_at[0] : attn_at[0] + 3 * half_width].reshape(
        model_width, 3, half_width
    )
    proj_t = attn_full[:, attn_at[1] : attn_at[1] + half_width]
    attn_vectors = attn_full[:, attn_at[2] : attn_at[2] + 3].astype(single)

    whole_input = gather_columns(tokens).astype(single)
    normed_out, normed_one, inv_std_one = norm_forward(
        whole_input, attn_vectors[:, 0], attn_vectors[:, 1]
    )
    first_input = normed_out.astype(narrow)
    qkv_bias = jnp.stack(
        [query_bias.astype(single), jnp.zeros((half_width,), single), value_bias.astype(single)]
    )
    projected = (
        jnp.einsum("td,dpe->tpe", first_input, qkv_full, preferred_element_type=single) + qkv_bias
    )
    queries = apply_rotary(
        projected[:, 0].reshape(local_rows, head_local, HD), cosine_table, sine_table
    ).astype(narrow)
    keys_all = apply_rotary(
        projected[:, 1].reshape(local_rows, head_local, HD), cosine_table, sine_table
    ).astype(narrow)
    values_all = projected[:, 2].astype(narrow)

    def attend(operands):
        query_block, key_block, value_block = operands
        scores = (
            jnp.einsum("qd,kd->qk", query_block, key_block, preferred_element_type=single) * scaling
        )
        weights = jax.nn.softmax(scores, axis=-1)
        mixed = jnp.einsum(
            "qk,kd->qd", weights.astype(narrow), value_block, preferred_element_type=single
        )
        return mixed.astype(narrow)

    attended = from_head(
        lax.map(attend, (by_head(queries), by_head(keys_all), by_head(values_all)))
    )
    attn_partial = jnp.einsum("te,de->td", attended, proj_t, preferred_element_type=single)
    residual_half = (
        tokens.astype(single)
        + share_columns(attn_partial)
        + own_half(attn_vectors[:, 2], column, half_width)
    )
    residual_full = gather_columns(residual_half.astype(jnp.bfloat16)).astype(residual_half.dtype)

    ffn_pack, ffn_at = pack(
        [
            gate_weight,
            up_weight,
            down_weight.T,
            jnp.stack([norm2_gain, norm2_bias, down_bias], axis=1),
        ]
    )
    ffn_full = lax.all_gather(ffn_pack, "row", axis=0, tiled=True)
    gate_full = ffn_full[:, ffn_at[0] : ffn_at[0] + ff_local]
    up_full = ffn_full[:, ffn_at[1] : ffn_at[1] + ff_local]
    down_t = ffn_full[:, ffn_at[2] : ffn_at[2] + ff_local]
    ffn_vectors = ffn_full[:, ffn_at[3] : ffn_at[3] + 3].astype(single)

    second_out, normed_two, inv_std_two = norm_forward(
        residual_full, ffn_vectors[:, 0], ffn_vectors[:, 1]
    )
    second_input = second_out.astype(narrow)
    gate_value = jnp.dot(second_input, gate_full, preferred_element_type=single) + gate_bias.astype(
        single
    )
    up_value = jnp.dot(second_input, up_full, preferred_element_type=single) + up_bias.astype(
        single
    )
    sigmoid_gate = jax.nn.sigmoid(gate_value)
    hidden = gate_value * sigmoid_gate * up_value
    hidden_mean = hidden_totals((jnp.sum(hidden, axis=1),))[0][:, None] / FF
    hidden_centred = hidden - hidden_mean
    hidden_var = hidden_totals((jnp.sum(hidden_centred * hidden_centred, axis=1),))[0][:, None] / FF
    hidden_inv = lax.rsqrt(hidden_var + EPSILON)
    hidden_normed = hidden_centred * hidden_inv
    down_input = (hidden_normed * inner_gain.astype(single) + inner_bias.astype(single)).astype(
        narrow
    )
    out_full = gather_columns(cotangent)
    out_float = out_full.astype(single)
    down_weight_grad_t = jnp.einsum(
        "td,tf->df", out_full, down_input, preferred_element_type=single
    )
    down_bias_grad = jnp.sum(out_float, axis=0)
    normed_grad = jnp.einsum("td,df->tf", out_full, down_t, preferred_element_type=single)
    scaled_grad = normed_grad * inner_gain.astype(single)
    first_total, second_total = hidden_totals(
        (jnp.sum(scaled_grad, axis=1), jnp.sum(scaled_grad * hidden_normed, axis=1))
    )
    hidden_grad = hidden_inv * (
        scaled_grad - first_total[:, None] / FF - hidden_normed * (second_total[:, None] / FF)
    )
    inner_gain_grad = jnp.sum(normed_grad * hidden_normed, axis=0)
    inner_bias_grad = jnp.sum(normed_grad, axis=0)
    gate_grad = (
        hidden_grad * up_value * sigmoid_gate * (1.0 + gate_value * (1.0 - sigmoid_gate))
    ).astype(narrow)
    up_grad = (hidden_grad * gate_value * sigmoid_gate).astype(narrow)
    gate_bias_grad = jnp.sum(gate_grad.astype(single), axis=0)
    up_bias_grad = jnp.sum(up_grad.astype(single), axis=0)
    gate_weight_grad = jnp.einsum(
        "td,tf->df", second_input, gate_grad, preferred_element_type=single
    )
    up_weight_grad = jnp.einsum("td,tf->df", second_input, up_grad, preferred_element_type=single)
    second_back = join_columns(
        jnp.einsum("tf,df->td", gate_grad, gate_full, preferred_element_type=single)
        + jnp.einsum("tf,df->td", up_grad, up_full, preferred_element_type=single)
    )
    second_delta, gain_two_grad, shift_two_grad = norm_backward(
        second_back, normed_two, inv_std_two, ffn_vectors[:, 0]
    )
    residual_grad = out_float + second_delta
    attn_grad = residual_grad.astype(narrow)
    proj_bias_grad = jnp.sum(attn_grad.astype(single), axis=0)
    proj_weight_grad_t = jnp.einsum(
        "td,te->de", attn_grad, attended, preferred_element_type=single
    )
    mid_small = jnp.concatenate([gate_bias_grad, up_bias_grad, inner_gain_grad, inner_bias_grad])
    mid_pack, mid_at = pack(
        [
            row_major(gate_weight_grad.astype(narrow)),
            row_major(up_weight_grad.astype(narrow)),
            row_major(down_weight_grad_t.astype(narrow)),
            row_major(proj_weight_grad_t.astype(narrow)),
            jnp.stack(
                [gain_two_grad, shift_two_grad, down_bias_grad, proj_bias_grad], axis=1
            ).astype(narrow),
            spread(mid_small, rows_local, row_count).astype(narrow),
        ]
    )
    mid_pack, attn_grad_held, down_input_held = lax.optimization_barrier(
        (mid_pack, attn_grad, down_input)
    )
    ffn_partial = jnp.einsum(
        "tf,df->td", down_input_held, down_t, preferred_element_type=single
    )
    layer_out = (
        residual_half
        + share_columns(ffn_partial)
        + own_half(ffn_vectors[:, 2], column, half_width)
    ).astype(narrow)
    mid_sums = lax.psum_scatter(mid_pack, "row", scatter_dimension=0, tiled=True).astype(single)
    attended_grad = jnp.einsum(
        "td,de->te", attn_grad_held, proj_t, preferred_element_type=single
    ).astype(narrow)

    def attend_back(operands):
        query_block, key_block, value_block, grad_block = operands
        scores = (
            jnp.einsum("qd,kd->qk", query_block, key_block, preferred_element_type=single) * scaling
        )
        weights = jax.nn.softmax(scores, axis=-1)
        value_grad = jnp.einsum(
            "qk,qd->kd", weights.astype(narrow), grad_block, preferred_element_type=single
        )
        weight_grad = jnp.einsum(
            "qd,kd->qk", grad_block, value_block, preferred_element_type=single
        )
        score_grad = (
            weights * (weight_grad - jnp.sum(weight_grad * weights, axis=-1, keepdims=True))
        ).astype(narrow)
        query_grad = (
            jnp.einsum("qk,kd->qd", score_grad, key_block, preferred_element_type=single) * scaling
        )
        key_grad = (
            jnp.einsum("qk,qd->kd", score_grad, query_block, preferred_element_type=single)
            * scaling
        )
        return (query_grad, key_grad, value_grad)

    query_grads, key_grads, value_grads = lax.map(
        attend_back,
        (by_head(queries), by_head(keys_all), by_head(values_all), by_head(attended_grad)),
    )
    query_pre = rotary_back(
        from_head(query_grads).reshape(local_rows, head_local, HD), cosine_table, sine_table
    )
    key_pre = rotary_back(
        from_head(key_grads).reshape(local_rows, head_local, HD), cosine_table, sine_table
    )
    qkv_grad = jnp.stack(
        [
            query_pre.reshape(local_rows, half_width),
            key_pre.reshape(local_rows, half_width),
            from_head(value_grads),
        ],
        axis=1,
    ).astype(narrow)
    qkv_grad_float = qkv_grad.astype(single)
    query_bias_grad = jnp.sum(qkv_grad_float[:, 0], axis=0)
    value_bias_grad = jnp.sum(qkv_grad_float[:, 2], axis=0)
    qkv_weight_grad = jnp.einsum(
        "td,tpe->dpe", first_input, qkv_grad, preferred_element_type=single
    )
    first_back = join_columns(
        jnp.einsum("tpe,dpe->td", qkv_grad, qkv_full, preferred_element_type=single)
    )
    first_delta, gain_one_grad, shift_one_grad = norm_backward(
        first_back, normed_one, inv_std_one, attn_vectors[:, 0]
    )
    input_grad = own_half(residual_grad + first_delta, column, half_width).astype(narrow)
    end_pack, end_at = pack(
        [
            qkv_weight_grad.reshape(model_width, 3 * half_width).astype(narrow),
            jnp.stack([gain_one_grad, shift_one_grad], axis=1).astype(narrow),
            spread(
                jnp.concatenate([query_bias_grad, value_bias_grad]), rows_local, row_count
            ).astype(narrow),
        ]
    )
    end_pack, mid_sums = lax.optimization_barrier((end_pack, mid_sums))
    end_sums = lax.psum_scatter(end_pack, "row", scatter_dimension=0, tiled=True).astype(single)

    def cut(sums, offset, width):
        return sums[:, offset : offset + width]

    mid_vectors = cut(mid_sums, mid_at[4], 4)
    mid_small_sum = cut(mid_sums, mid_at[5], -(-mid_small.shape[0] // rows_local)).reshape(-1)
    end_vectors = cut(end_sums, end_at[1], 2)
    end_small_sum = cut(end_sums, end_at[2], -(-2 * half_width // rows_local)).reshape(-1)
    return (
        layer_out,
        input_grad,
        end_vectors[:, 0],
        end_vectors[:, 1],
        cut(end_sums, end_at[0], 3 * half_width).reshape(rows_local, 3, half_width),
        end_small_sum[:half_width],
        end_small_sum[half_width : 2 * half_width],
        cut(mid_sums, mid_at[3], half_width).T,
        mid_vectors[:, 3],
        mid_vectors[:, 0],
        mid_vectors[:, 1],
        cut(mid_sums, mid_at[0], ff_local),
        mid_small_sum[:ff_local],
        cut(mid_sums, mid_at[1], ff_local),
        mid_small_sum[ff_local : 2 * ff_local],
        mid_small_sum[2 * ff_local : 3 * ff_local],
        mid_small_sum[3 * ff_local : 4 * ff_local],
        cut(mid_sums, mid_at[2], ff_local).T,
        mid_vectors[:, 2],
    )


def solution(mesh):
    placed = (
        P("row", "col"),
        P("row"),
        P("row"),
        P("row", None, "col"),
        P("col"),
        P("col"),
        P("col", "row"),
        P("row"),
        P("row"),
        P("row"),
        P("row", "col"),
        P("col"),
        P("row", "col"),
        P("col"),
        P("col"),
        P("col"),
        P("col", "row"),
        P("row"),
        P("row", "col"),
    )
    return jax.shard_map(
        functools.partial(body, mesh.shape["row"]),
        mesh=mesh,
        in_specs=placed,
        out_specs=(
            P("row", "col"),
            P("row", "col"),
            P("row"),
            P("row"),
            P("row", None, "col"),
            P("col"),
            P("col"),
            P("col", "row"),
            P("row"),
            P("row"),
            P("row"),
            P("row", "col"),
            P("col"),
            P("row", "col"),
            P("col"),
            P("col"),
            P("col"),
            P("col", "row"),
            P("row"),
        ),
        check_vma=False,
    )
```

```python
import functools
import math

import jax
import jax.numpy as jnp
from jax import lax
from jax.experimental.layout import Layout, with_layout_constraint
from jax.sharding import PartitionSpec as P


HD = 64
FF = 2730
GRID = 32
SEQ = 1025


EPSILON = 1e-06


def norm_forward(values, norm_gain, norm_shift):
    row_mean = jnp.mean(values, axis=-1, keepdims=True)
    centred = values - row_mean
    variance = jnp.mean(centred * centred, axis=-1, keepdims=True)
    inv_std = lax.rsqrt(variance + EPSILON)
    normed = centred * inv_std
    return (normed * norm_gain + norm_shift, normed, inv_std)


def norm_backward(upstream, normed, inv_std, norm_gain):
    scaled = upstream * norm_gain
    first_mean = jnp.mean(scaled, axis=-1, keepdims=True)
    second_mean = jnp.mean(scaled * normed, axis=-1, keepdims=True)
    delta = inv_std * (scaled - first_mean - normed * second_mean)
    return (delta, jnp.sum(upstream * normed, axis=0), jnp.sum(upstream, axis=0))


def rotary_tables(length, seq_len, grid_side, head_size):
    quarter = head_size // 4
    position = jnp.arange(length, dtype=jnp.int32) % seq_len
    patch_index = jnp.maximum(position - 1, 0)
    inside = (position > 0).astype(jnp.float32)
    row_pos = (patch_index // grid_side).astype(jnp.float32) * inside
    col_pos = (patch_index % grid_side).astype(jnp.float32) * inside
    frequency = jnp.exp(-math.log(10000.0) * jnp.arange(quarter, dtype=jnp.float32) / quarter)
    row_angle = row_pos[:, None] * frequency[None, :]
    col_angle = col_pos[:, None] * frequency[None, :]
    angles = jnp.concatenate([row_angle, row_angle, col_angle, col_angle], axis=1)
    return (jnp.cos(angles), jnp.sin(angles))


def rotate(values):
    pieces = jnp.split(values, 4, axis=-1)
    return jnp.concatenate([-pieces[1], pieces[0], -pieces[3], pieces[2]], axis=-1)


def rotate_transposed(values):
    pieces = jnp.split(values, 4, axis=-1)
    return jnp.concatenate([pieces[1], -pieces[0], pieces[3], -pieces[2]], axis=-1)


def apply_rotary(values, cosine_table, sine_table):
    return values * cosine_table[:, None, :] + rotate(values) * sine_table[:, None, :]


def rotary_back(grads, cosine_table, sine_table):
    return grads * cosine_table[:, None, :] + rotate_transposed(grads * sine_table[:, None, :])


def own_half(vector, column, half_width):
    return lax.dynamic_slice_in_dim(vector, column * half_width, half_width, axis=vector.ndim - 1)


def swap_columns(values):
    return lax.ppermute(values, "col", [(0, 1), (1, 0)])


def share_columns(partial_sums):
    half = partial_sums.shape[1] // 2
    column = lax.axis_index("col")
    own = lax.dynamic_slice_in_dim(partial_sums, column * half, half, axis=1)
    other = lax.dynamic_slice_in_dim(partial_sums, (1 - column) * half, half, axis=1)
    return own + swap_columns(other.astype(jnp.bfloat16)).astype(jnp.float32)


def join_columns(partial_sums):
    narrow = partial_sums.astype(jnp.bfloat16)
    return narrow.astype(jnp.float32) + swap_columns(narrow).astype(jnp.float32)


def gather_columns(values):
    other = swap_columns(values)
    first = lax.axis_index("col") == 0
    return jnp.concatenate(
        [jnp.where(first, values, other), jnp.where(first, other, values)], axis=1
    )


def hidden_totals(row_sums):
    return tuple(part + swap_columns(part) for part in row_sums)


def row_major(values):
    return with_layout_constraint(values, Layout((0, 1)))


def lane_round(width):
    return -(-width // 128) * 128


def pack(pieces):
    offsets = []
    padded = []
    position = 0
    for piece in pieces:
        width = lane_round(piece.shape[1])
        offsets.append(position)
        padded.append(jnp.pad(piece, ((0, 0), (0, width - piece.shape[1]))))
        position += width
    return jnp.concatenate(padded, axis=1), offsets


def spread(vector, rows_local, row_count):
    cols = -(-vector.shape[0] // rows_local)
    block = jnp.pad(vector, (0, rows_local * cols - vector.shape[0])).reshape(rows_local, cols)
    return jnp.tile(block, (row_count, 1))


def body(
    row_count,
    tokens,
    norm1_gain,
    norm1_bias,
    qkv_weight,
    query_bias,
    value_bias,
    proj_weight,
    proj_bias,
    norm2_gain,
    norm2_bias,
    gate_weight,
    gate_bias,
    up_weight,
    up_bias,
    inner_gain,
    inner_bias,
    down_weight,
    down_bias,
    cotangent,
):
    single = jnp.float32
    narrow = jnp.bfloat16
    local_rows = tokens.shape[0]
    half_width = tokens.shape[1]
    rows_local = norm1_gain.shape[0]
    model_width = rows_local * row_count
    ff_local = gate_weight.shape[1]
    head_local = half_width // HD
    images_local = local_rows // SEQ
    column = lax.axis_index("col")
    scaling = 1.0 / math.sqrt(HD)
    cosine_table, sine_table = rotary_tables(local_rows, SEQ, GRID, HD)

    def by_head(array):
        shaped = array.reshape(images_local, SEQ, head_local, HD).transpose(0, 2, 1, 3)
        return shaped.reshape(images_local * head_local, SEQ, HD)

    def from_head(array):
        shaped = array.reshape(images_local, head_local, SEQ, HD).transpose(0, 2, 1, 3)
        return shaped.reshape(local_rows, half_width)

    attn_pack, attn_at = pack(
        [
            qkv_weight.reshape(rows_local, 3 * half_width),
            proj_weight.T,
            jnp.stack(
                [norm1_gain, norm1_bias, proj_bias, norm2_gain, norm2_bias, down_bias], axis=1
            ),
        ]
    )
    attn_full = lax.all_gather(attn_pack, "row", axis=0, tiled=True)
    qkv_full = attn_full[:, attn_at[0] : attn_at[0] + 3 * half_width].reshape(
        model_width, 3, half_width
    )
    proj_t = attn_full[:, attn_at[1] : attn_at[1] + half_width]
    attn_vectors = attn_full[:, attn_at[2] : attn_at[2] + 6].astype(single)
    ffn_vectors = attn_vectors[:, 3:]

    whole_input = gather_columns(tokens).astype(single)
    normed_out, normed_one, inv_std_one = norm_forward(
        whole_input, attn_vectors[:, 0], attn_vectors[:, 1]
    )
    first_input = normed_out.astype(narrow)
    qkv_bias = jnp.stack(
        [query_bias.astype(single), jnp.zeros((half_width,), single), value_bias.astype(single)]
    )
    projected = (
        jnp.einsum("td,dpe->tpe", first_input, qkv_full, preferred_element_type=single) + qkv_bias
    )
    queries = apply_rotary(
        projected[:, 0].reshape(local_rows, head_local, HD), cosine_table, sine_table
    ).astype(narrow)
    keys_all = apply_rotary(
        projected[:, 1].reshape(local_rows, head_local, HD), cosine_table, sine_table
    ).astype(narrow)
    values_all = projected[:, 2].astype(narrow)

    def attend(operands):
        query_block, key_block, value_block = operands
        scores = (
            jnp.einsum("qd,kd->qk", query_block, key_block, preferred_element_type=single) * scaling
        )
        weights = jax.nn.softmax(scores, axis=-1)
        mixed = jnp.einsum(
            "qk,kd->qd", weights.astype(narrow), value_block, preferred_element_type=single
        )
        return mixed.astype(narrow)

    attended = from_head(
        lax.map(attend, (by_head(queries), by_head(keys_all), by_head(values_all)))
    )
    attn_partial = jnp.einsum("te,de->td", attended, proj_t, preferred_element_type=single)
    residual_half = (
        tokens.astype(single)
        + share_columns(attn_partial)
        + own_half(attn_vectors[:, 2], column, half_width)
    )
    residual_full = gather_columns(residual_half.astype(jnp.bfloat16)).astype(residual_half.dtype)

    ffn_pack, ffn_at = pack(
        [
            gate_weight,
            up_weight,
            down_weight.T,
        ]
    )
    ffn_full = lax.all_gather(ffn_pack, "row", axis=0, tiled=True)
    gate_full = ffn_full[:, ffn_at[0] : ffn_at[0] + ff_local]
    up_full = ffn_full[:, ffn_at[1] : ffn_at[1] + ff_local]
    down_t = ffn_full[:, ffn_at[2] : ffn_at[2] + ff_local]

    second_out, normed_two, inv_std_two = norm_forward(
        residual_full, ffn_vectors[:, 0], ffn_vectors[:, 1]
    )
    second_input = second_out.astype(narrow)
    gate_value = jnp.dot(second_input, gate_full, preferred_element_type=single) + gate_bias.astype(
        single
    )
    up_value = jnp.dot(second_input, up_full, preferred_element_type=single) + up_bias.astype(
        single
    )
    sigmoid_gate = jax.nn.sigmoid(gate_value)
    hidden = gate_value * sigmoid_gate * up_value
    hidden_mean = hidden_totals((jnp.sum(hidden, axis=1),))[0][:, None] / FF
    hidden_centred = hidden - hidden_mean
    hidden_var = hidden_totals((jnp.sum(hidden_centred * hidden_centred, axis=1),))[0][:, None] / FF
    hidden_inv = lax.rsqrt(hidden_var + EPSILON)
    hidden_normed = hidden_centred * hidden_inv
    down_input = (hidden_normed * inner_gain.astype(single) + inner_bias.astype(single)).astype(
        narrow
    )
    out_full = gather_columns(cotangent)
    out_float = out_full.astype(single)
    down_weight_grad_t = jnp.einsum(
        "td,tf->df", out_full, down_input, preferred_element_type=single
    )
    down_bias_grad = jnp.sum(out_float, axis=0)
    normed_grad = jnp.einsum("td,df->tf", out_full, down_t, preferred_element_type=single)
    scaled_grad = normed_grad * inner_gain.astype(single)
    first_total, second_total = hidden_totals(
        (jnp.sum(scaled_grad, axis=1), jnp.sum(scaled_grad * hidden_normed, axis=1))
    )
    hidden_grad = hidden_inv * (
        scaled_grad - first_total[:, None] / FF - hidden_normed * (second_total[:, None] / FF)
    )
    inner_gain_grad = jnp.sum(normed_grad * hidden_normed, axis=0)
    inner_bias_grad = jnp.sum(normed_grad, axis=0)
    gate_grad = (
        hidden_grad * up_value * sigmoid_gate * (1.0 + gate_value * (1.0 - sigmoid_gate))
    ).astype(narrow)
    up_grad = (hidden_grad * gate_value * sigmoid_gate).astype(narrow)
    gate_bias_grad = jnp.sum(gate_grad.astype(single), axis=0)
    up_bias_grad = jnp.sum(up_grad.astype(single), axis=0)
    gate_weight_grad = jnp.einsum(
        "td,tf->df", second_input, gate_grad, preferred_element_type=single
    )
    up_weight_grad = jnp.einsum("td,tf->df", second_input, up_grad, preferred_element_type=single)
    second_back = join_columns(
        jnp.einsum("tf,df->td", gate_grad, gate_full, preferred_element_type=single)
        + jnp.einsum("tf,df->td", up_grad, up_full, preferred_element_type=single)
    )
    second_delta, gain_two_grad, shift_two_grad = norm_backward(
        second_back, normed_two, inv_std_two, ffn_vectors[:, 0]
    )
    residual_grad = out_float + second_delta
    attn_grad = residual_grad.astype(narrow)
    proj_bias_grad = jnp.sum(attn_grad.astype(single), axis=0)
    proj_weight_grad_t = jnp.einsum(
        "td,te->de", attn_grad, attended, preferred_element_type=single
    )
    mid_small = jnp.concatenate([gate_bias_grad, up_bias_grad, inner_gain_grad, inner_bias_grad])
    mid_pack, mid_at = pack(
        [
            row_major(gate_weight_grad.astype(narrow)),
            row_major(up_weight_grad.astype(narrow)),
            row_major(down_weight_grad_t.astype(narrow)),
            row_major(proj_weight_grad_t.astype(narrow)),
            jnp.stack(
                [gain_two_grad, shift_two_grad, down_bias_grad, proj_bias_grad], axis=1
            ).astype(narrow),
            spread(mid_small, rows_local, row_count).astype(narrow),
        ]
    )
    mid_pack, attn_grad_held, down_input_held = lax.optimization_barrier(
        (mid_pack, attn_grad, down_input)
    )
    ffn_partial = jnp.einsum(
        "tf,df->td", down_input_held, down_t, preferred_element_type=single
    )
    layer_out = (
        residual_half
        + share_columns(ffn_partial)
        + own_half(ffn_vectors[:, 2], column, half_width)
    ).astype(narrow)
    mid_sums = lax.psum_scatter(mid_pack, "row", scatter_dimension=0, tiled=True).astype(single)
    attended_grad = jnp.einsum(
        "td,de->te", attn_grad_held, proj_t, preferred_element_type=single
    ).astype(narrow)

    def attend_back(operands):
        query_block, key_block, value_block, grad_block = operands
        scores = (
            jnp.einsum("qd,kd->qk", query_block, key_block, preferred_element_type=single) * scaling
        )
        weights = jax.nn.softmax(scores, axis=-1)
        value_grad = jnp.einsum(
            "qk,qd->kd", weights.astype(narrow), grad_block, preferred_element_type=single
        )
        weight_grad = jnp.einsum(
            "qd,kd->qk", grad_block, value_block, preferred_element_type=single
        )
        score_grad = (
            weights * (weight_grad - jnp.sum(weight_grad * weights, axis=-1, keepdims=True))
        ).astype(narrow)
        query_grad = (
            jnp.einsum("qk,kd->qd", score_grad, key_block, preferred_element_type=single) * scaling
        )
        key_grad = (
            jnp.einsum("qk,qd->kd", score_grad, query_block, preferred_element_type=single)
            * scaling
        )
        return (query_grad, key_grad, value_grad)

    query_grads, key_grads, value_grads = lax.map(
        attend_back,
        (by_head(queries), by_head(keys_all), by_head(values_all), by_head(attended_grad)),
    )
    query_pre = rotary_back(
        from_head(query_grads).reshape(local_rows, head_local, HD), cosine_table, sine_table
    )
    key_pre = rotary_back(
        from_head(key_grads).reshape(local_rows, head_local, HD), cosine_table, sine_table
    )
    qkv_grad = jnp.stack(
        [
            query_pre.reshape(local_rows, half_width),
            key_pre.reshape(local_rows, half_width),
            from_head(value_grads),
        ],
        axis=1,
    ).astype(narrow)
    qkv_grad_float = qkv_grad.astype(single)
    query_bias_grad = jnp.sum(qkv_grad_float[:, 0], axis=0)
    value_bias_grad = jnp.sum(qkv_grad_float[:, 2], axis=0)
    qkv_weight_grad = jnp.einsum(
        "td,tpe->dpe", first_input, qkv_grad, preferred_element_type=single
    )
    first_back = join_columns(
        jnp.einsum("tpe,dpe->td", qkv_grad, qkv_full, preferred_element_type=single)
    )
    first_delta, gain_one_grad, shift_one_grad = norm_backward(
        first_back, normed_one, inv_std_one, attn_vectors[:, 0]
    )
    input_grad = own_half(residual_grad + first_delta, column, half_width).astype(narrow)
    end_pack, end_at = pack(
        [
            qkv_weight_grad.reshape(model_width, 3 * half_width).astype(narrow),
            jnp.stack([gain_one_grad, shift_one_grad], axis=1).astype(narrow),
            spread(
                jnp.concatenate([query_bias_grad, value_bias_grad]), rows_local, row_count
            ).astype(narrow),
        ]
    )
    end_pack, mid_sums = lax.optimization_barrier((end_pack, mid_sums))
    end_sums = lax.psum_scatter(end_pack, "row", scatter_dimension=0, tiled=True).astype(single)

    def cut(sums, offset, width):
        return sums[:, offset : offset + width]

    mid_vectors = cut(mid_sums, mid_at[4], 4)
    mid_small_sum = cut(mid_sums, mid_at[5], -(-mid_small.shape[0] // rows_local)).reshape(-1)
    end_vectors = cut(end_sums, end_at[1], 2)
    end_small_sum = cut(end_sums, end_at[2], -(-2 * half_width // rows_local)).reshape(-1)
    return (
        layer_out,
        input_grad,
        end_vectors[:, 0],
        end_vectors[:, 1],
        cut(end_sums, end_at[0], 3 * half_width).reshape(rows_local, 3, half_width),
        end_small_sum[:half_width],
        end_small_sum[half_width : 2 * half_width],
        cut(mid_sums, mid_at[3], half_width).T,
        mid_vectors[:, 3],
        mid_vectors[:, 0],
        mid_vectors[:, 1],
        cut(mid_sums, mid_at[0], ff_local),
        mid_small_sum[:ff_local],
        cut(mid_sums, mid_at[1], ff_local),
        mid_small_sum[ff_local : 2 * ff_local],
        mid_small_sum[2 * ff_local : 3 * ff_local],
        mid_small_sum[3 * ff_local : 4 * ff_local],
        cut(mid_sums, mid_at[2], ff_local).T,
        mid_vectors[:, 2],
    )


def solution(mesh):
    placed = (
        P("row", "col"),
        P("row"),
        P("row"),
        P("row", None, "col"),
        P("col"),
        P("col"),
        P("col", "row"),
        P("row"),
        P("row"),
        P("row"),
        P("row", "col"),
        P("col"),
        P("row", "col"),
        P("col"),
        P("col"),
        P("col"),
        P("col", "row"),
        P("row"),
        P("row", "col"),
    )
    return jax.shard_map(
        functools.partial(body, mesh.shape["row"]),
        mesh=mesh,
        in_specs=placed,
        out_specs=(
            P("row", "col"),
            P("row", "col"),
            P("row"),
            P("row"),
            P("row", None, "col"),
            P("col"),
            P("col"),
            P("col", "row"),
            P("row"),
            P("row"),
            P("row"),
            P("row", "col"),
            P("col"),
            P("row", "col"),
            P("col"),
            P("col"),
            P("col"),
            P("col", "row"),
            P("row"),
        ),
        check_vma=False,
    )
```

```python
import functools
import math

import jax
import jax.numpy as jnp
from jax import lax
from jax.experimental.layout import Layout, with_layout_constraint
from jax.sharding import PartitionSpec as P


HD = 64
FF = 2730
GRID = 32
SEQ = 1025


EPSILON = 1e-06


def norm_forward(values, norm_gain, norm_shift):
    row_mean = jnp.mean(values, axis=-1, keepdims=True)
    centred = values - row_mean
    variance = jnp.mean(centred * centred, axis=-1, keepdims=True)
    inv_std = lax.rsqrt(variance + EPSILON)
    normed = centred * inv_std
    return (normed * norm_gain + norm_shift, normed, inv_std)


def norm_backward(upstream, normed, inv_std, norm_gain):
    scaled = upstream * norm_gain
    first_mean = jnp.mean(scaled, axis=-1, keepdims=True)
    second_mean = jnp.mean(scaled * normed, axis=-1, keepdims=True)
    delta = inv_std * (scaled - first_mean - normed * second_mean)
    return (delta, jnp.sum(upstream * normed, axis=0), jnp.sum(upstream, axis=0))


def rotary_tables(length, seq_len, grid_side, head_size):
    quarter = head_size // 4
    position = jnp.arange(length, dtype=jnp.int32) % seq_len
    patch_index = jnp.maximum(position - 1, 0)
    inside = (position > 0).astype(jnp.float32)
    row_pos = (patch_index // grid_side).astype(jnp.float32) * inside
    col_pos = (patch_index % grid_side).astype(jnp.float32) * inside
    frequency = jnp.exp(-math.log(10000.0) * jnp.arange(quarter, dtype=jnp.float32) / quarter)
    row_angle = row_pos[:, None] * frequency[None, :]
    col_angle = col_pos[:, None] * frequency[None, :]
    angles = jnp.concatenate([row_angle, row_angle, col_angle, col_angle], axis=1)
    return (jnp.cos(angles), jnp.sin(angles))


def rotate(values):
    pieces = jnp.split(values, 4, axis=-1)
    return jnp.concatenate([-pieces[1], pieces[0], -pieces[3], pieces[2]], axis=-1)


def rotate_transposed(values):
    pieces = jnp.split(values, 4, axis=-1)
    return jnp.concatenate([pieces[1], -pieces[0], pieces[3], -pieces[2]], axis=-1)


def apply_rotary(values, cosine_table, sine_table):
    return values * cosine_table[:, None, :] + rotate(values) * sine_table[:, None, :]


def rotary_back(grads, cosine_table, sine_table):
    return grads * cosine_table[:, None, :] + rotate_transposed(grads * sine_table[:, None, :])


def own_half(vector, column, half_width):
    return lax.dynamic_slice_in_dim(vector, column * half_width, half_width, axis=vector.ndim - 1)


def swap_columns(values):
    return lax.ppermute(values, "col", [(0, 1), (1, 0)])


def share_columns(partial_sums):
    half = partial_sums.shape[1] // 2
    column = lax.axis_index("col")
    own = lax.dynamic_slice_in_dim(partial_sums, column * half, half, axis=1)
    other = lax.dynamic_slice_in_dim(partial_sums, (1 - column) * half, half, axis=1)
    return own + swap_columns(other.astype(jnp.bfloat16)).astype(jnp.float32)


def join_columns(partial_sums):
    narrow = partial_sums.astype(jnp.bfloat16)
    return narrow.astype(jnp.float32) + swap_columns(narrow).astype(jnp.float32)


def gather_columns(values):
    other = swap_columns(values)
    first = lax.axis_index("col") == 0
    return jnp.concatenate(
        [jnp.where(first, values, other), jnp.where(first, other, values)], axis=1
    )


def hidden_totals(row_sums):
    return tuple(part + swap_columns(part) for part in row_sums)


def row_major(values):
    return with_layout_constraint(values, Layout((0, 1)))


def lane_round(width):
    return -(-width // 128) * 128


def pack(pieces):
    offsets = []
    padded = []
    position = 0
    for piece in pieces:
        width = lane_round(piece.shape[1])
        offsets.append(position)
        padded.append(jnp.pad(piece, ((0, 0), (0, width - piece.shape[1]))))
        position += width
    return jnp.concatenate(padded, axis=1), offsets


def spread(vector, rows_local, row_count):
    cols = -(-vector.shape[0] // rows_local)
    block = jnp.pad(vector, (0, rows_local * cols - vector.shape[0])).reshape(rows_local, cols)
    return jnp.tile(block, (row_count, 1))


def body(
    row_count,
    tokens,
    norm1_gain,
    norm1_bias,
    qkv_weight,
    query_bias,
    value_bias,
    proj_weight,
    proj_bias,
    norm2_gain,
    norm2_bias,
    gate_weight,
    gate_bias,
    up_weight,
    up_bias,
    inner_gain,
    inner_bias,
    down_weight,
    down_bias,
    cotangent,
):
    single = jnp.float32
    narrow = jnp.bfloat16
    local_rows = tokens.shape[0]
    half_width = tokens.shape[1]
    rows_local = norm1_gain.shape[0]
    model_width = rows_local * row_count
    ff_local = gate_weight.shape[1]
    head_local = half_width // HD
    images_local = local_rows // SEQ
    column = lax.axis_index("col")
    scaling = 1.0 / math.sqrt(HD)
    cosine_table, sine_table = rotary_tables(local_rows, SEQ, GRID, HD)

    def by_head(array):
        shaped = array.reshape(images_local, SEQ, head_local, HD).transpose(0, 2, 1, 3)
        return shaped.reshape(images_local * head_local, SEQ, HD)

    def from_head(array):
        shaped = array.reshape(images_local, head_local, SEQ, HD).transpose(0, 2, 1, 3)
        return shaped.reshape(local_rows, half_width)

    attn_pack, attn_at = pack(
        [
            qkv_weight.reshape(rows_local, 3 * half_width),
            proj_weight.T,
            jnp.stack(
                [norm1_gain, norm1_bias, proj_bias, norm2_gain, norm2_bias, down_bias], axis=1
            ),
        ]
    )
    attn_full = lax.all_gather(attn_pack, "row", axis=0, tiled=True)
    qkv_full = attn_full[:, attn_at[0] : attn_at[0] + 3 * half_width].reshape(
        model_width, 3, half_width
    )
    proj_t = attn_full[:, attn_at[1] : attn_at[1] + half_width]
    attn_vectors = attn_full[:, attn_at[2] : attn_at[2] + 6].astype(single)
    ffn_vectors = attn_vectors[:, 3:]

    whole_input = gather_columns(tokens).astype(single)
    normed_out, normed_one, inv_std_one = norm_forward(
        whole_input, attn_vectors[:, 0], attn_vectors[:, 1]
    )
    first_input = normed_out.astype(narrow)
    qkv_bias = jnp.stack(
        [query_bias.astype(single), jnp.zeros((half_width,), single), value_bias.astype(single)]
    )
    projected = (
        jnp.einsum("td,dpe->tpe", first_input, qkv_full, preferred_element_type=single) + qkv_bias
    )
    queries = apply_rotary(
        projected[:, 0].reshape(local_rows, head_local, HD), cosine_table, sine_table
    ).astype(narrow)
    keys_all = apply_rotary(
        projected[:, 1].reshape(local_rows, head_local, HD), cosine_table, sine_table
    ).astype(narrow)
    values_all = projected[:, 2].astype(narrow)

    def attend(operands):
        query_block, key_block, value_block = operands
        scores = (
            jnp.einsum("qd,kd->qk", query_block, key_block, preferred_element_type=single) * scaling
        )
        weights = jax.nn.softmax(scores, axis=-1)
        mixed = jnp.einsum(
            "qk,kd->qd", weights.astype(narrow), value_block, preferred_element_type=single
        )
        return mixed.astype(narrow)

    attended = from_head(
        lax.map(attend, (by_head(queries), by_head(keys_all), by_head(values_all)))
    )
    attn_partial = jnp.einsum("te,de->td", attended, proj_t, preferred_element_type=single)
    residual_half = (
        tokens.astype(single)
        + share_columns(attn_partial)
        + own_half(attn_vectors[:, 2], column, half_width)
    )
    residual_full = gather_columns(residual_half.astype(jnp.bfloat16)).astype(residual_half.dtype)

    ffn_pack, ffn_at = pack(
        [
            gate_weight,
            up_weight,
            down_weight.T,
        ]
    )
    ffn_full = lax.all_gather(ffn_pack, "row", axis=0, tiled=True)
    gate_full = ffn_full[:, ffn_at[0] : ffn_at[0] + ff_local]
    up_full = ffn_full[:, ffn_at[1] : ffn_at[1] + ff_local]
    down_t = ffn_full[:, ffn_at[2] : ffn_at[2] + ff_local]

    second_out, normed_two, inv_std_two = norm_forward(
        residual_full, ffn_vectors[:, 0], ffn_vectors[:, 1]
    )
    second_input = second_out.astype(narrow)
    gate_value = jnp.dot(second_input, gate_full, preferred_element_type=single) + gate_bias.astype(
        single
    )
    up_value = jnp.dot(second_input, up_full, preferred_element_type=single) + up_bias.astype(
        single
    )
    sigmoid_gate = jax.nn.sigmoid(gate_value)
    hidden = gate_value * sigmoid_gate * up_value
    hidden_mean = hidden_totals((jnp.sum(hidden, axis=1),))[0][:, None] / FF
    hidden_centred = hidden - hidden_mean
    hidden_var = hidden_totals((jnp.sum(hidden_centred * hidden_centred, axis=1),))[0][:, None] / FF
    hidden_inv = lax.rsqrt(hidden_var + EPSILON)
    hidden_normed = hidden_centred * hidden_inv
    down_input = (hidden_normed * inner_gain.astype(single) + inner_bias.astype(single)).astype(
        narrow
    )
    out_full = gather_columns(cotangent)
    out_float = out_full.astype(single)
    down_weight_grad_t = jnp.einsum(
        "td,tf->df", out_full, down_input, preferred_element_type=single
    )
    down_bias_grad = jnp.sum(out_float, axis=0)
    normed_grad = jnp.einsum("td,df->tf", out_full, down_t, preferred_element_type=single)
    scaled_grad = normed_grad * inner_gain.astype(single)
    first_total, second_total = hidden_totals(
        (jnp.sum(scaled_grad, axis=1), jnp.sum(scaled_grad * hidden_normed, axis=1))
    )
    hidden_grad = hidden_inv * (
        scaled_grad - first_total[:, None] / FF - hidden_normed * (second_total[:, None] / FF)
    )
    inner_gain_grad = jnp.sum(normed_grad * hidden_normed, axis=0)
    inner_bias_grad = jnp.sum(normed_grad, axis=0)
    gate_grad = (
        hidden_grad * up_value * sigmoid_gate * (1.0 + gate_value * (1.0 - sigmoid_gate))
    ).astype(narrow)
    up_grad = (hidden_grad * gate_value * sigmoid_gate).astype(narrow)
    gate_bias_grad = jnp.sum(gate_grad.astype(single), axis=0)
    up_bias_grad = jnp.sum(up_grad.astype(single), axis=0)
    gate_weight_grad = jnp.einsum(
        "td,tf->df", second_input, gate_grad, preferred_element_type=single
    )
    up_weight_grad = jnp.einsum("td,tf->df", second_input, up_grad, preferred_element_type=single)
    second_back = join_columns(
        jnp.einsum("tf,df->td", gate_grad, gate_full, preferred_element_type=single)
        + jnp.einsum("tf,df->td", up_grad, up_full, preferred_element_type=single)
    )
    second_delta, gain_two_grad, shift_two_grad = norm_backward(
        second_back, normed_two, inv_std_two, ffn_vectors[:, 0]
    )
    residual_grad = out_float + second_delta
    attn_grad = residual_grad.astype(narrow)
    proj_bias_grad = jnp.sum(attn_grad.astype(single), axis=0)
    proj_weight_grad_t = jnp.einsum(
        "td,te->de", attn_grad, attended, preferred_element_type=single
    )
    mid_small = jnp.concatenate([gate_bias_grad, up_bias_grad, inner_gain_grad, inner_bias_grad])
    mid_pack, mid_at = pack(
        [
            row_major(gate_weight_grad.astype(narrow)),
            row_major(up_weight_grad.astype(narrow)),
            row_major(down_weight_grad_t.astype(narrow)),
            row_major(proj_weight_grad_t.astype(narrow)),
            jnp.concatenate(
                [
                    jnp.stack(
                        [gain_two_grad, shift_two_grad, down_bias_grad, proj_bias_grad], axis=1
                    ),
                    spread(mid_small, rows_local, row_count),
                ],
                axis=1,
            ).astype(narrow),
        ]
    )
    mid_pack, attn_grad_held, down_input_held = lax.optimization_barrier(
        (mid_pack, attn_grad, down_input)
    )
    ffn_partial = jnp.einsum(
        "tf,df->td", down_input_held, down_t, preferred_element_type=single
    )
    layer_out = (
        residual_half
        + share_columns(ffn_partial)
        + own_half(ffn_vectors[:, 2], column, half_width)
    ).astype(narrow)
    mid_sums = lax.psum_scatter(mid_pack, "row", scatter_dimension=0, tiled=True).astype(single)
    attended_grad = jnp.einsum(
        "td,de->te", attn_grad_held, proj_t, preferred_element_type=single
    ).astype(narrow)

    def attend_back(operands):
        query_block, key_block, value_block, grad_block = operands
        scores = (
            jnp.einsum("qd,kd->qk", query_block, key_block, preferred_element_type=single) * scaling
        )
        weights = jax.nn.softmax(scores, axis=-1)
        value_grad = jnp.einsum(
            "qk,qd->kd", weights.astype(narrow), grad_block, preferred_element_type=single
        )
        weight_grad = jnp.einsum(
            "qd,kd->qk", grad_block, value_block, preferred_element_type=single
        )
        score_grad = (
            weights * (weight_grad - jnp.sum(weight_grad * weights, axis=-1, keepdims=True))
        ).astype(narrow)
        query_grad = (
            jnp.einsum("qk,kd->qd", score_grad, key_block, preferred_element_type=single) * scaling
        )
        key_grad = (
            jnp.einsum("qk,qd->kd", score_grad, query_block, preferred_element_type=single)
            * scaling
        )
        return (query_grad, key_grad, value_grad)

    query_grads, key_grads, value_grads = lax.map(
        attend_back,
        (by_head(queries), by_head(keys_all), by_head(values_all), by_head(attended_grad)),
    )
    query_pre = rotary_back(
        from_head(query_grads).reshape(local_rows, head_local, HD), cosine_table, sine_table
    )
    key_pre = rotary_back(
        from_head(key_grads).reshape(local_rows, head_local, HD), cosine_table, sine_table
    )
    qkv_grad = jnp.stack(
        [
            query_pre.reshape(local_rows, half_width),
            key_pre.reshape(local_rows, half_width),
            from_head(value_grads),
        ],
        axis=1,
    ).astype(narrow)
    qkv_grad_float = qkv_grad.astype(single)
    query_bias_grad = jnp.sum(qkv_grad_float[:, 0], axis=0)
    value_bias_grad = jnp.sum(qkv_grad_float[:, 2], axis=0)
    qkv_weight_grad = jnp.einsum(
        "td,tpe->dpe", first_input, qkv_grad, preferred_element_type=single
    )
    first_back = join_columns(
        jnp.einsum("tpe,dpe->td", qkv_grad, qkv_full, preferred_element_type=single)
    )
    first_delta, gain_one_grad, shift_one_grad = norm_backward(
        first_back, normed_one, inv_std_one, attn_vectors[:, 0]
    )
    input_grad = own_half(residual_grad + first_delta, column, half_width).astype(narrow)
    end_pack, end_at = pack(
        [
            qkv_weight_grad.reshape(model_width, 3 * half_width).astype(narrow),
            jnp.concatenate(
                [
                    jnp.stack([gain_one_grad, shift_one_grad], axis=1),
                    spread(
                        jnp.concatenate([query_bias_grad, value_bias_grad]), rows_local, row_count
                    ),
                ],
                axis=1,
            ).astype(narrow),
        ]
    )
    end_pack, mid_sums = lax.optimization_barrier((end_pack, mid_sums))
    end_sums = lax.psum_scatter(end_pack, "row", scatter_dimension=0, tiled=True).astype(single)

    def cut(sums, offset, width):
        return sums[:, offset : offset + width]

    mid_vectors = cut(mid_sums, mid_at[4], 4)
    mid_small_sum = cut(
        mid_sums, mid_at[4] + 4, -(-mid_small.shape[0] // rows_local)
    ).reshape(-1)
    end_vectors = cut(end_sums, end_at[1], 2)
    end_small_sum = cut(end_sums, end_at[1] + 2, -(-2 * half_width // rows_local)).reshape(-1)
    return (
        layer_out,
        input_grad,
        end_vectors[:, 0],
        end_vectors[:, 1],
        cut(end_sums, end_at[0], 3 * half_width).reshape(rows_local, 3, half_width),
        end_small_sum[:half_width],
        end_small_sum[half_width : 2 * half_width],
        cut(mid_sums, mid_at[3], half_width).T,
        mid_vectors[:, 3],
        mid_vectors[:, 0],
        mid_vectors[:, 1],
        cut(mid_sums, mid_at[0], ff_local),
        mid_small_sum[:ff_local],
        cut(mid_sums, mid_at[1], ff_local),
        mid_small_sum[ff_local : 2 * ff_local],
        mid_small_sum[2 * ff_local : 3 * ff_local],
        mid_small_sum[3 * ff_local : 4 * ff_local],
        cut(mid_sums, mid_at[2], ff_local).T,
        mid_vectors[:, 2],
    )


def solution(mesh):
    placed = (
        P("row", "col"),
        P("row"),
        P("row"),
        P("row", None, "col"),
        P("col"),
        P("col"),
        P("col", "row"),
        P("row"),
        P("row"),
        P("row"),
        P("row", "col"),
        P("col"),
        P("row", "col"),
        P("col"),
        P("col"),
        P("col"),
        P("col", "row"),
        P("row"),
        P("row", "col"),
    )
    return jax.shard_map(
        functools.partial(body, mesh.shape["row"]),
        mesh=mesh,
        in_specs=placed,
        out_specs=(
            P("row", "col"),
            P("row", "col"),
            P("row"),
            P("row"),
            P("row", None, "col"),
            P("col"),
            P("col"),
            P("col", "row"),
            P("row"),
            P("row"),
            P("row"),
            P("row", "col"),
            P("col"),
            P("row", "col"),
            P("col"),
            P("col"),
            P("col"),
            P("col", "row"),
            P("row"),
        ),
        check_vma=False,
    )
```

```python
import functools
import math

import jax
import jax.numpy as jnp
from jax import lax
from jax.experimental.layout import Layout, with_layout_constraint
from jax.sharding import PartitionSpec as P


HD = 64
FF = 2730
GRID = 32
SEQ = 1025


EPSILON = 1e-06


def norm_forward(values, norm_gain, norm_shift):
    row_mean = jnp.mean(values, axis=-1, keepdims=True)
    centred = values - row_mean
    variance = jnp.mean(centred * centred, axis=-1, keepdims=True)
    inv_std = lax.rsqrt(variance + EPSILON)
    normed = centred * inv_std
    return (normed * norm_gain + norm_shift, normed, inv_std)


def norm_backward(upstream, normed, inv_std, norm_gain):
    scaled = upstream * norm_gain
    first_mean = jnp.mean(scaled, axis=-1, keepdims=True)
    second_mean = jnp.mean(scaled * normed, axis=-1, keepdims=True)
    delta = inv_std * (scaled - first_mean - normed * second_mean)
    return (delta, jnp.sum(upstream * normed, axis=0), jnp.sum(upstream, axis=0))


def rotary_tables(length, seq_len, grid_side, head_size):
    quarter = head_size // 4
    position = jnp.arange(length, dtype=jnp.int32) % seq_len
    patch_index = jnp.maximum(position - 1, 0)
    inside = (position > 0).astype(jnp.float32)
    row_pos = (patch_index // grid_side).astype(jnp.float32) * inside
    col_pos = (patch_index % grid_side).astype(jnp.float32) * inside
    frequency = jnp.exp(-math.log(10000.0) * jnp.arange(quarter, dtype=jnp.float32) / quarter)
    row_angle = row_pos[:, None] * frequency[None, :]
    col_angle = col_pos[:, None] * frequency[None, :]
    angles = jnp.concatenate([row_angle, row_angle, col_angle, col_angle], axis=1)
    return (jnp.cos(angles), jnp.sin(angles))


def rotate(values):
    pieces = jnp.split(values, 4, axis=-1)
    return jnp.concatenate([-pieces[1], pieces[0], -pieces[3], pieces[2]], axis=-1)


def rotate_transposed(values):
    pieces = jnp.split(values, 4, axis=-1)
    return jnp.concatenate([pieces[1], -pieces[0], pieces[3], -pieces[2]], axis=-1)


def apply_rotary(values, cosine_table, sine_table):
    return values * cosine_table[:, None, :] + rotate(values) * sine_table[:, None, :]


def rotary_back(grads, cosine_table, sine_table):
    return grads * cosine_table[:, None, :] + rotate_transposed(grads * sine_table[:, None, :])


def own_half(vector, column, half_width):
    return lax.dynamic_slice_in_dim(vector, column * half_width, half_width, axis=vector.ndim - 1)


def swap_columns(values):
    return lax.ppermute(values, "col", [(0, 1), (1, 0)])


def share_columns(partial_sums):
    half = partial_sums.shape[1] // 2
    column = lax.axis_index("col")
    own = lax.dynamic_slice_in_dim(partial_sums, column * half, half, axis=1)
    other = lax.dynamic_slice_in_dim(partial_sums, (1 - column) * half, half, axis=1)
    return own + swap_columns(other.astype(jnp.bfloat16)).astype(jnp.float32)


def join_columns(partial_sums):
    narrow = partial_sums.astype(jnp.bfloat16)
    return narrow.astype(jnp.float32) + swap_columns(narrow).astype(jnp.float32)


def gather_columns(values):
    other = swap_columns(values)
    first = lax.axis_index("col") == 0
    return jnp.concatenate(
        [jnp.where(first, values, other), jnp.where(first, other, values)], axis=1
    )


def hidden_totals(row_sums):
    return tuple(part + swap_columns(part) for part in row_sums)


def row_major(values):
    return with_layout_constraint(values, Layout((0, 1)))


def lane_round(width):
    return -(-width // 128) * 128


def pack(pieces):
    offsets = []
    padded = []
    position = 0
    for piece in pieces:
        width = lane_round(piece.shape[1])
        offsets.append(position)
        padded.append(jnp.pad(piece, ((0, 0), (0, width - piece.shape[1]))))
        position += width
    return jnp.concatenate(padded, axis=1), offsets


def spread(vector, rows_local, row_count):
    cols = -(-vector.shape[0] // rows_local)
    block = jnp.pad(vector, (0, rows_local * cols - vector.shape[0])).reshape(rows_local, cols)
    return jnp.tile(block, (row_count, 1))


def body(
    row_count,
    tokens,
    norm1_gain,
    norm1_bias,
    qkv_weight,
    query_bias,
    value_bias,
    proj_weight,
    proj_bias,
    norm2_gain,
    norm2_bias,
    gate_weight,
    gate_bias,
    up_weight,
    up_bias,
    inner_gain,
    inner_bias,
    down_weight,
    down_bias,
    cotangent,
):
    single = jnp.float32
    narrow = jnp.bfloat16
    local_rows = tokens.shape[0]
    half_width = tokens.shape[1]
    rows_local = norm1_gain.shape[0]
    model_width = rows_local * row_count
    ff_local = gate_weight.shape[1]
    head_local = half_width // HD
    images_local = local_rows // SEQ
    column = lax.axis_index("col")
    scaling = 1.0 / math.sqrt(HD)
    cosine_table, sine_table = rotary_tables(local_rows, SEQ, GRID, HD)

    def by_head(array):
        shaped = array.reshape(images_local, SEQ, head_local, HD).transpose(0, 2, 1, 3)
        return shaped.reshape(images_local * head_local, SEQ, HD)

    def from_head(array):
        shaped = array.reshape(images_local, head_local, SEQ, HD).transpose(0, 2, 1, 3)
        return shaped.reshape(local_rows, half_width)

    attn_pack, attn_at = pack(
        [
            qkv_weight.reshape(rows_local, 3 * half_width),
            proj_weight.T,
            jnp.stack(
                [norm1_gain, norm1_bias, proj_bias, norm2_gain, norm2_bias, down_bias], axis=1
            ),
        ]
    )
    attn_full = lax.all_gather(attn_pack, "row", axis=0, tiled=True)
    qkv_full = attn_full[:, attn_at[0] : attn_at[0] + 3 * half_width].reshape(
        model_width, 3, half_width
    )
    proj_t = attn_full[:, attn_at[1] : attn_at[1] + half_width]
    attn_vectors = attn_full[:, attn_at[2] : attn_at[2] + 6].astype(single)
    ffn_vectors = attn_vectors[:, 3:]

    whole_input = gather_columns(tokens).astype(single)
    normed_out, normed_one, inv_std_one = norm_forward(
        whole_input, attn_vectors[:, 0], attn_vectors[:, 1]
    )
    first_input = normed_out.astype(narrow)
    qkv_bias = jnp.stack(
        [query_bias.astype(single), jnp.zeros((half_width,), single), value_bias.astype(single)]
    )
    projected = (
        jnp.einsum("td,dpe->tpe", first_input, qkv_full, preferred_element_type=single) + qkv_bias
    )
    queries = apply_rotary(
        projected[:, 0].reshape(local_rows, head_local, HD), cosine_table, sine_table
    ).astype(narrow)
    keys_all = apply_rotary(
        projected[:, 1].reshape(local_rows, head_local, HD), cosine_table, sine_table
    ).astype(narrow)
    values_all = projected[:, 2].astype(narrow)

    def attend(operands):
        query_block, key_block, value_block = operands
        scores = (
            jnp.einsum("qd,kd->qk", query_block, key_block, preferred_element_type=single) * scaling
        )
        weights = jax.nn.softmax(scores, axis=-1)
        mixed = jnp.einsum(
            "qk,kd->qd", weights.astype(narrow), value_block, preferred_element_type=single
        )
        return mixed.astype(narrow)

    attended = from_head(
        lax.map(attend, (by_head(queries), by_head(keys_all), by_head(values_all)))
    )
    attn_partial = jnp.einsum("te,de->td", attended, proj_t, preferred_element_type=single)
    residual_half = (
        tokens.astype(single)
        + share_columns(attn_partial)
        + own_half(attn_vectors[:, 2], column, half_width)
    )
    residual_full = gather_columns(residual_half.astype(jnp.bfloat16)).astype(residual_half.dtype)

    ffn_pack, ffn_at = pack(
        [
            gate_weight,
            up_weight,
            down_weight.T,
        ]
    )
    ffn_full = lax.all_gather(ffn_pack, "row", axis=0, tiled=True)
    gate_up_full = ffn_full[:, : ffn_at[2]]
    down_t = ffn_full[:, ffn_at[2] : ffn_at[2] + ff_local]

    second_out, normed_two, inv_std_two = norm_forward(
        residual_full, ffn_vectors[:, 0], ffn_vectors[:, 1]
    )
    second_input = second_out.astype(narrow)
    gate_up_value = jnp.dot(second_input, gate_up_full, preferred_element_type=single)
    gate_value = gate_up_value[:, :ff_local] + gate_bias.astype(single)
    up_value = gate_up_value[:, ffn_at[1] : ffn_at[1] + ff_local] + up_bias.astype(single)
    sigmoid_gate = jax.nn.sigmoid(gate_value)
    hidden = gate_value * sigmoid_gate * up_value
    hidden_mean = hidden_totals((jnp.sum(hidden, axis=1),))[0][:, None] / FF
    hidden_centred = hidden - hidden_mean
    hidden_var = hidden_totals((jnp.sum(hidden_centred * hidden_centred, axis=1),))[0][:, None] / FF
    hidden_inv = lax.rsqrt(hidden_var + EPSILON)
    hidden_normed = hidden_centred * hidden_inv
    down_input = (hidden_normed * inner_gain.astype(single) + inner_bias.astype(single)).astype(
        narrow
    )
    out_full = gather_columns(cotangent)
    out_float = out_full.astype(single)
    down_weight_grad_t = jnp.einsum(
        "td,tf->df", out_full, down_input, preferred_element_type=single
    )
    down_bias_grad = jnp.sum(out_float, axis=0)
    normed_grad = jnp.einsum("td,df->tf", out_full, down_t, preferred_element_type=single)
    scaled_grad = normed_grad * inner_gain.astype(single)
    first_total, second_total = hidden_totals(
        (jnp.sum(scaled_grad, axis=1), jnp.sum(scaled_grad * hidden_normed, axis=1))
    )
    hidden_grad = hidden_inv * (
        scaled_grad - first_total[:, None] / FF - hidden_normed * (second_total[:, None] / FF)
    )
    inner_gain_grad = jnp.sum(normed_grad * hidden_normed, axis=0)
    inner_bias_grad = jnp.sum(normed_grad, axis=0)
    gate_grad = (
        hidden_grad * up_value * sigmoid_gate * (1.0 + gate_value * (1.0 - sigmoid_gate))
    ).astype(narrow)
    up_grad = (hidden_grad * gate_value * sigmoid_gate).astype(narrow)
    gate_bias_grad = jnp.sum(gate_grad.astype(single), axis=0)
    up_bias_grad = jnp.sum(up_grad.astype(single), axis=0)
    gate_up_grad, _ = pack([gate_grad, up_grad, jnp.zeros((local_rows, 0), narrow)])
    gate_up_weight_grad = jnp.einsum(
        "td,tf->df", second_input, gate_up_grad, preferred_element_type=single
    )
    second_back = join_columns(
        jnp.einsum("tf,df->td", gate_up_grad, gate_up_full, preferred_element_type=single)
    )
    second_delta, gain_two_grad, shift_two_grad = norm_backward(
        second_back, normed_two, inv_std_two, ffn_vectors[:, 0]
    )
    residual_grad = out_float + second_delta
    attn_grad = residual_grad.astype(narrow)
    proj_bias_grad = jnp.sum(attn_grad.astype(single), axis=0)
    proj_weight_grad_t = jnp.einsum(
        "td,te->de", attn_grad, attended, preferred_element_type=single
    )
    mid_small = jnp.concatenate([gate_bias_grad, up_bias_grad, inner_gain_grad, inner_bias_grad])
    mid_pack, mid_at = pack(
        [
            row_major(gate_up_weight_grad.astype(narrow)),
            row_major(down_weight_grad_t.astype(narrow)),
            row_major(proj_weight_grad_t.astype(narrow)),
            jnp.stack(
                [gain_two_grad, shift_two_grad, down_bias_grad, proj_bias_grad], axis=1
            ).astype(narrow),
            spread(mid_small, rows_local, row_count).astype(narrow),
        ]
    )
    mid_pack, attn_grad_held, down_input_held = lax.optimization_barrier(
        (mid_pack, attn_grad, down_input)
    )
    ffn_partial = jnp.einsum(
        "tf,df->td", down_input_held, down_t, preferred_element_type=single
    )
    layer_out = (
        residual_half
        + share_columns(ffn_partial)
        + own_half(ffn_vectors[:, 2], column, half_width)
    ).astype(narrow)
    mid_sums = lax.psum_scatter(mid_pack, "row", scatter_dimension=0, tiled=True).astype(single)
    attended_grad = jnp.einsum(
        "td,de->te", attn_grad_held, proj_t, preferred_element_type=single
    ).astype(narrow)

    def attend_back(operands):
        query_block, key_block, value_block, grad_block = operands
        scores = (
            jnp.einsum("qd,kd->qk", query_block, key_block, preferred_element_type=single) * scaling
        )
        weights = jax.nn.softmax(scores, axis=-1)
        value_grad = jnp.einsum(
            "qk,qd->kd", weights.astype(narrow), grad_block, preferred_element_type=single
        )
        weight_grad = jnp.einsum(
            "qd,kd->qk", grad_block, value_block, preferred_element_type=single
        )
        score_grad = (
            weights * (weight_grad - jnp.sum(weight_grad * weights, axis=-1, keepdims=True))
        ).astype(narrow)
        query_grad = (
            jnp.einsum("qk,kd->qd", score_grad, key_block, preferred_element_type=single) * scaling
        )
        key_grad = (
            jnp.einsum("qk,qd->kd", score_grad, query_block, preferred_element_type=single)
            * scaling
        )
        return (query_grad, key_grad, value_grad)

    query_grads, key_grads, value_grads = lax.map(
        attend_back,
        (by_head(queries), by_head(keys_all), by_head(values_all), by_head(attended_grad)),
    )
    query_pre = rotary_back(
        from_head(query_grads).reshape(local_rows, head_local, HD), cosine_table, sine_table
    )
    key_pre = rotary_back(
        from_head(key_grads).reshape(local_rows, head_local, HD), cosine_table, sine_table
    )
    qkv_grad = jnp.stack(
        [
            query_pre.reshape(local_rows, half_width),
            key_pre.reshape(local_rows, half_width),
            from_head(value_grads),
        ],
        axis=1,
    ).astype(narrow)
    qkv_grad_float = qkv_grad.astype(single)
    query_bias_grad = jnp.sum(qkv_grad_float[:, 0], axis=0)
    value_bias_grad = jnp.sum(qkv_grad_float[:, 2], axis=0)
    qkv_weight_grad = jnp.einsum(
        "td,tpe->dpe", first_input, qkv_grad, preferred_element_type=single
    )
    first_back = join_columns(
        jnp.einsum("tpe,dpe->td", qkv_grad, qkv_full, preferred_element_type=single)
    )
    first_delta, gain_one_grad, shift_one_grad = norm_backward(
        first_back, normed_one, inv_std_one, attn_vectors[:, 0]
    )
    input_grad = own_half(residual_grad + first_delta, column, half_width).astype(narrow)
    end_pack, end_at = pack(
        [
            qkv_weight_grad.reshape(model_width, 3 * half_width).astype(narrow),
            jnp.stack([gain_one_grad, shift_one_grad], axis=1).astype(narrow),
            spread(
                jnp.concatenate([query_bias_grad, value_bias_grad]), rows_local, row_count
            ).astype(narrow),
        ]
    )
    end_pack, mid_sums = lax.optimization_barrier((end_pack, mid_sums))
    end_sums = lax.psum_scatter(end_pack, "row", scatter_dimension=0, tiled=True).astype(single)

    def cut(sums, offset, width):
        return sums[:, offset : offset + width]

    mid_vectors = cut(mid_sums, mid_at[3], 4)
    mid_small_sum = cut(mid_sums, mid_at[4], -(-mid_small.shape[0] // rows_local)).reshape(-1)
    end_vectors = cut(end_sums, end_at[1], 2)
    end_small_sum = cut(end_sums, end_at[2], -(-2 * half_width // rows_local)).reshape(-1)
    return (
        layer_out,
        input_grad,
        end_vectors[:, 0],
        end_vectors[:, 1],
        cut(end_sums, end_at[0], 3 * half_width).reshape(rows_local, 3, half_width),
        end_small_sum[:half_width],
        end_small_sum[half_width : 2 * half_width],
        cut(mid_sums, mid_at[2], half_width).T,
        mid_vectors[:, 3],
        mid_vectors[:, 0],
        mid_vectors[:, 1],
        cut(mid_sums, mid_at[0], ff_local),
        mid_small_sum[:ff_local],
        cut(mid_sums, mid_at[0] + ffn_at[1], ff_local),
        mid_small_sum[ff_local : 2 * ff_local],
        mid_small_sum[2 * ff_local : 3 * ff_local],
        mid_small_sum[3 * ff_local : 4 * ff_local],
        cut(mid_sums, mid_at[1], ff_local).T,
        mid_vectors[:, 2],
    )


def solution(mesh):
    placed = (
        P("row", "col"),
        P("row"),
        P("row"),
        P("row", None, "col"),
        P("col"),
        P("col"),
        P("col", "row"),
        P("row"),
        P("row"),
        P("row"),
        P("row", "col"),
        P("col"),
        P("row", "col"),
        P("col"),
        P("col"),
        P("col"),
        P("col", "row"),
        P("row"),
        P("row", "col"),
    )
    return jax.shard_map(
        functools.partial(body, mesh.shape["row"]),
        mesh=mesh,
        in_specs=placed,
        out_specs=(
            P("row", "col"),
            P("row", "col"),
            P("row"),
            P("row"),
            P("row", None, "col"),
            P("col"),
            P("col"),
            P("col", "row"),
            P("row"),
            P("row"),
            P("row"),
            P("row", "col"),
            P("col"),
            P("row", "col"),
            P("col"),
            P("col"),
            P("col"),
            P("col", "row"),
            P("row"),
        ),
        check_vma=False,
    )
```

```python
import functools
import math

import jax
import jax.numpy as jnp
from jax import lax
from jax.experimental.layout import Layout, with_layout_constraint
from jax.sharding import PartitionSpec as P


HD = 64
FF = 2730
GRID = 32
SEQ = 1025


EPSILON = 1e-06


def norm_forward(values, norm_gain, norm_shift):
    row_mean = jnp.mean(values, axis=-1, keepdims=True)
    centred = values - row_mean
    variance = jnp.mean(centred * centred, axis=-1, keepdims=True)
    inv_std = lax.rsqrt(variance + EPSILON)
    normed = centred * inv_std
    return (normed * norm_gain + norm_shift, normed, inv_std)


def norm_backward(upstream, normed, inv_std, norm_gain):
    scaled = upstream * norm_gain
    first_mean = jnp.mean(scaled, axis=-1, keepdims=True)
    second_mean = jnp.mean(scaled * normed, axis=-1, keepdims=True)
    delta = inv_std * (scaled - first_mean - normed * second_mean)
    return (delta, jnp.sum(upstream * normed, axis=0), jnp.sum(upstream, axis=0))


def rotary_tables(length, seq_len, grid_side, head_size):
    quarter = head_size // 4
    position = jnp.arange(length, dtype=jnp.int32) % seq_len
    patch_index = jnp.maximum(position - 1, 0)
    inside = (position > 0).astype(jnp.float32)
    row_pos = (patch_index // grid_side).astype(jnp.float32) * inside
    col_pos = (patch_index % grid_side).astype(jnp.float32) * inside
    frequency = jnp.exp(-math.log(10000.0) * jnp.arange(quarter, dtype=jnp.float32) / quarter)
    row_angle = row_pos[:, None] * frequency[None, :]
    col_angle = col_pos[:, None] * frequency[None, :]
    angles = jnp.concatenate([row_angle, row_angle, col_angle, col_angle], axis=1)
    return (jnp.cos(angles), jnp.sin(angles))


def rotate(values):
    pieces = jnp.split(values, 4, axis=-1)
    return jnp.concatenate([-pieces[1], pieces[0], -pieces[3], pieces[2]], axis=-1)


def rotate_transposed(values):
    pieces = jnp.split(values, 4, axis=-1)
    return jnp.concatenate([pieces[1], -pieces[0], pieces[3], -pieces[2]], axis=-1)


def apply_rotary(values, cosine_table, sine_table):
    return values * cosine_table[:, None, :] + rotate(values) * sine_table[:, None, :]


def rotary_back(grads, cosine_table, sine_table):
    return grads * cosine_table[:, None, :] + rotate_transposed(grads * sine_table[:, None, :])


def own_half(vector, column, half_width):
    return lax.dynamic_slice_in_dim(vector, column * half_width, half_width, axis=vector.ndim - 1)


def swap_columns(values):
    return lax.ppermute(values, "col", [(0, 1), (1, 0)])


def share_columns(partial_sums):
    half = partial_sums.shape[1] // 2
    column = lax.axis_index("col")
    own = lax.dynamic_slice_in_dim(partial_sums, column * half, half, axis=1)
    other = lax.dynamic_slice_in_dim(partial_sums, (1 - column) * half, half, axis=1)
    return own + swap_columns(other.astype(jnp.bfloat16)).astype(jnp.float32)


def join_columns(partial_sums):
    narrow = partial_sums.astype(jnp.bfloat16)
    return narrow.astype(jnp.float32) + swap_columns(narrow).astype(jnp.float32)


def gather_columns(values):
    other = swap_columns(values)
    first = lax.axis_index("col") == 0
    return jnp.concatenate(
        [jnp.where(first, values, other), jnp.where(first, other, values)], axis=1
    )


def hidden_totals(row_sums):
    return tuple(part + swap_columns(part) for part in row_sums)


def row_major(values):
    return with_layout_constraint(values, Layout((0, 1)))


def lane_round(width):
    return -(-width // 128) * 128


def pack(pieces):
    offsets = []
    padded = []
    position = 0
    for piece in pieces:
        width = lane_round(piece.shape[1])
        offsets.append(position)
        padded.append(jnp.pad(piece, ((0, 0), (0, width - piece.shape[1]))))
        position += width
    return jnp.concatenate(padded, axis=1), offsets


def spread(vector, rows_local, row_count):
    cols = -(-vector.shape[0] // rows_local)
    block = jnp.pad(vector, (0, rows_local * cols - vector.shape[0])).reshape(rows_local, cols)
    return jnp.tile(block, (row_count, 1))


def body(
    row_count,
    tokens,
    norm1_gain,
    norm1_bias,
    qkv_weight,
    query_bias,
    value_bias,
    proj_weight,
    proj_bias,
    norm2_gain,
    norm2_bias,
    gate_weight,
    gate_bias,
    up_weight,
    up_bias,
    inner_gain,
    inner_bias,
    down_weight,
    down_bias,
    cotangent,
):
    single = jnp.float32
    narrow = jnp.bfloat16
    local_rows = tokens.shape[0]
    half_width = tokens.shape[1]
    rows_local = norm1_gain.shape[0]
    model_width = rows_local * row_count
    ff_local = gate_weight.shape[1]
    head_local = half_width // HD
    images_local = local_rows // SEQ
    column = lax.axis_index("col")
    scaling = 1.0 / math.sqrt(HD)
    cosine_table, sine_table = rotary_tables(local_rows, SEQ, GRID, HD)

    def by_head(array):
        shaped = array.reshape(images_local, SEQ, head_local, HD).transpose(0, 2, 1, 3)
        return shaped.reshape(images_local * head_local, SEQ, HD)

    def from_head(array):
        shaped = array.reshape(images_local, head_local, SEQ, HD).transpose(0, 2, 1, 3)
        return shaped.reshape(local_rows, half_width)

    attn_pack, attn_at = pack(
        [
            qkv_weight.reshape(rows_local, 3 * half_width),
            proj_weight.T,
            jnp.stack(
                [norm1_gain, norm1_bias, proj_bias, norm2_gain, norm2_bias, down_bias], axis=1
            ),
        ]
    )
    attn_full = lax.all_gather(attn_pack, "row", axis=0, tiled=True)
    qkv_full = attn_full[:, attn_at[0] : attn_at[0] + 3 * half_width].reshape(
        model_width, 3, half_width
    )
    proj_t = attn_full[:, attn_at[1] : attn_at[1] + half_width]
    attn_vectors = attn_full[:, attn_at[2] : attn_at[2] + 6].astype(single)
    ffn_vectors = attn_vectors[:, 3:]

    whole_input = gather_columns(tokens).astype(single)
    normed_out, normed_one, inv_std_one = norm_forward(
        whole_input, attn_vectors[:, 0], attn_vectors[:, 1]
    )
    first_input = normed_out.astype(narrow)
    qkv_bias = jnp.stack(
        [query_bias.astype(single), jnp.zeros((half_width,), single), value_bias.astype(single)]
    )
    projected = (
        jnp.einsum("td,dpe->tpe", first_input, qkv_full, preferred_element_type=single) + qkv_bias
    )
    queries = apply_rotary(
        projected[:, 0].reshape(local_rows, head_local, HD), cosine_table, sine_table
    ).astype(narrow)
    keys_all = apply_rotary(
        projected[:, 1].reshape(local_rows, head_local, HD), cosine_table, sine_table
    ).astype(narrow)
    values_all = projected[:, 2].astype(narrow)

    def attend(operands):
        query_block, key_block, value_block = operands
        scores = (
            jnp.einsum("qd,kd->qk", query_block, key_block, preferred_element_type=single) * scaling
        )
        weights = jax.nn.softmax(scores, axis=-1)
        mixed = jnp.einsum(
            "qk,kd->qd", weights.astype(narrow), value_block, preferred_element_type=single
        )
        return mixed.astype(narrow)

    attended = from_head(
        lax.map(attend, (by_head(queries), by_head(keys_all), by_head(values_all)))
    )
    attn_partial = jnp.einsum("te,de->td", attended, proj_t, preferred_element_type=single)
    residual_half = (
        tokens.astype(single)
        + share_columns(attn_partial)
        + own_half(attn_vectors[:, 2], column, half_width)
    )
    residual_full = gather_columns(residual_half.astype(jnp.bfloat16)).astype(residual_half.dtype)

    ffn_pack, ffn_at = pack(
        [
            gate_weight,
            up_weight,
            down_weight.T,
        ]
    )
    ffn_full = lax.all_gather(ffn_pack, "row", axis=0, tiled=True)
    gate_up_full = ffn_full[:, : ffn_at[2]]
    down_t = ffn_full[:, ffn_at[2] : ffn_at[2] + ff_local]

    second_out, normed_two, inv_std_two = norm_forward(
        residual_full, ffn_vectors[:, 0], ffn_vectors[:, 1]
    )
    second_input = second_out.astype(narrow)
    gate_up_value = jnp.dot(second_input, gate_up_full, preferred_element_type=single)
    gate_value = gate_up_value[:, :ff_local] + gate_bias.astype(single)
    up_value = gate_up_value[:, ffn_at[1] : ffn_at[1] + ff_local] + up_bias.astype(single)
    sigmoid_gate = jax.nn.sigmoid(gate_value)
    hidden = gate_value * sigmoid_gate * up_value
    hidden_mean = hidden_totals((jnp.sum(hidden, axis=1),))[0][:, None] / FF
    hidden_centred = hidden - hidden_mean
    hidden_var = hidden_totals((jnp.sum(hidden_centred * hidden_centred, axis=1),))[0][:, None] / FF
    hidden_inv = lax.rsqrt(hidden_var + EPSILON)
    hidden_normed = hidden_centred * hidden_inv
    down_input = (hidden_normed * inner_gain.astype(single) + inner_bias.astype(single)).astype(
        narrow
    )
    out_full = gather_columns(cotangent)
    out_float = out_full.astype(single)
    down_weight_grad_t = jnp.einsum(
        "td,tf->df", out_full, down_input, preferred_element_type=single
    )
    down_bias_grad = jnp.sum(out_float, axis=0)
    normed_grad = jnp.einsum("td,df->tf", out_full, down_t, preferred_element_type=single)
    scaled_grad = normed_grad * inner_gain.astype(single)
    first_total, second_total = hidden_totals(
        (jnp.sum(scaled_grad, axis=1), jnp.sum(scaled_grad * hidden_normed, axis=1))
    )
    hidden_grad = hidden_inv * (
        scaled_grad - first_total[:, None] / FF - hidden_normed * (second_total[:, None] / FF)
    )
    inner_gain_grad = jnp.sum(normed_grad * hidden_normed, axis=0)
    inner_bias_grad = jnp.sum(normed_grad, axis=0)
    gate_grad = (
        hidden_grad * up_value * sigmoid_gate * (1.0 + gate_value * (1.0 - sigmoid_gate))
    ).astype(narrow)
    up_grad = (hidden_grad * gate_value * sigmoid_gate).astype(narrow)
    gate_bias_grad = jnp.sum(gate_grad.astype(single), axis=0)
    up_bias_grad = jnp.sum(up_grad.astype(single), axis=0)
    gate_up_grad, _ = pack([gate_grad, up_grad, jnp.zeros((local_rows, 0), narrow)])
    gate_up_weight_grad = jnp.einsum(
        "td,tf->df", second_input, gate_up_grad, preferred_element_type=single
    )
    mid_small = jnp.concatenate([gate_bias_grad, up_bias_grad, inner_gain_grad, inner_bias_grad])
    mid_pack, mid_at = pack(
        [
            row_major(gate_up_weight_grad.astype(narrow)),
            row_major(down_weight_grad_t.astype(narrow)),
            jnp.concatenate(
                [down_bias_grad[:, None], spread(mid_small, rows_local, row_count)], axis=1
            ).astype(narrow),
            jnp.zeros((model_width, 256), narrow),
        ]
    )
    mid_pack, gate_up_grad, down_input_held = lax.optimization_barrier(
        (mid_pack, gate_up_grad, down_input)
    )
    mid_sums = lax.psum_scatter(mid_pack, "row", scatter_dimension=0, tiled=True).astype(single)
    second_back = join_columns(
        jnp.einsum("tf,df->td", gate_up_grad, gate_up_full, preferred_element_type=single)
    )
    second_delta, gain_two_grad, shift_two_grad = norm_backward(
        second_back, normed_two, inv_std_two, ffn_vectors[:, 0]
    )
    residual_grad = out_float + second_delta
    attn_grad = residual_grad.astype(narrow)
    proj_bias_grad = jnp.sum(attn_grad.astype(single), axis=0)
    proj_weight_grad_t = jnp.einsum(
        "td,te->de", attn_grad, attended, preferred_element_type=single
    )
    ffn_partial = jnp.einsum(
        "tf,df->td", down_input_held, down_t, preferred_element_type=single
    )
    layer_out = (
        residual_half
        + share_columns(ffn_partial)
        + own_half(ffn_vectors[:, 2], column, half_width)
    ).astype(narrow)
    attended_grad = jnp.einsum(
        "td,de->te", attn_grad, proj_t, preferred_element_type=single
    ).astype(narrow)

    def attend_back(operands):
        query_block, key_block, value_block, grad_block = operands
        scores = (
            jnp.einsum("qd,kd->qk", query_block, key_block, preferred_element_type=single) * scaling
        )
        weights = jax.nn.softmax(scores, axis=-1)
        value_grad = jnp.einsum(
            "qk,qd->kd", weights.astype(narrow), grad_block, preferred_element_type=single
        )
        weight_grad = jnp.einsum(
            "qd,kd->qk", grad_block, value_block, preferred_element_type=single
        )
        score_grad = (
            weights * (weight_grad - jnp.sum(weight_grad * weights, axis=-1, keepdims=True))
        ).astype(narrow)
        query_grad = (
            jnp.einsum("qk,kd->qd", score_grad, key_block, preferred_element_type=single) * scaling
        )
        key_grad = (
            jnp.einsum("qk,qd->kd", score_grad, query_block, preferred_element_type=single)
            * scaling
        )
        return (query_grad, key_grad, value_grad)

    query_grads, key_grads, value_grads = lax.map(
        attend_back,
        (by_head(queries), by_head(keys_all), by_head(values_all), by_head(attended_grad)),
    )
    query_pre = rotary_back(
        from_head(query_grads).reshape(local_rows, head_local, HD), cosine_table, sine_table
    )
    key_pre = rotary_back(
        from_head(key_grads).reshape(local_rows, head_local, HD), cosine_table, sine_table
    )
    qkv_grad = jnp.stack(
        [
            query_pre.reshape(local_rows, half_width),
            key_pre.reshape(local_rows, half_width),
            from_head(value_grads),
        ],
        axis=1,
    ).astype(narrow)
    qkv_grad_float = qkv_grad.astype(single)
    query_bias_grad = jnp.sum(qkv_grad_float[:, 0], axis=0)
    value_bias_grad = jnp.sum(qkv_grad_float[:, 2], axis=0)
    qkv_weight_grad = jnp.einsum(
        "td,tpe->dpe", first_input, qkv_grad, preferred_element_type=single
    )
    first_back = join_columns(
        jnp.einsum("tpe,dpe->td", qkv_grad, qkv_full, preferred_element_type=single)
    )
    first_delta, gain_one_grad, shift_one_grad = norm_backward(
        first_back, normed_one, inv_std_one, attn_vectors[:, 0]
    )
    input_grad = own_half(residual_grad + first_delta, column, half_width).astype(narrow)
    end_pack, end_at = pack(
        [
            qkv_weight_grad.reshape(model_width, 3 * half_width).astype(narrow),
            row_major(proj_weight_grad_t.astype(narrow)),
            jnp.concatenate(
                [
                    jnp.stack(
                        [gain_one_grad, shift_one_grad, proj_bias_grad, gain_two_grad, shift_two_grad],
                        axis=1,
                    ),
                    spread(
                        jnp.concatenate([query_bias_grad, value_bias_grad]), rows_local, row_count
                    ),
                ],
                axis=1,
            ).astype(narrow),
        ]
    )
    end_pack, mid_sums = lax.optimization_barrier((end_pack, mid_sums))
    end_sums = lax.psum_scatter(end_pack, "row", scatter_dimension=0, tiled=True).astype(single)

    def cut(sums, offset, width):
        return sums[:, offset : offset + width]

    mid_tail = cut(mid_sums, mid_at[2], 1 + -(-mid_small.shape[0] // rows_local))
    mid_small_sum = mid_tail[:, 1:].reshape(-1)
    end_tail = cut(end_sums, end_at[2], 5 + -(-2 * half_width // rows_local))
    end_small_sum = end_tail[:, 5:].reshape(-1)
    return (
        layer_out,
        input_grad,
        end_tail[:, 0],
        end_tail[:, 1],
        cut(end_sums, end_at[0], 3 * half_width).reshape(rows_local, 3, half_width),
        end_small_sum[:half_width],
        end_small_sum[half_width : 2 * half_width],
        cut(end_sums, end_at[1], half_width).T,
        end_tail[:, 2],
        end_tail[:, 3],
        end_tail[:, 4],
        cut(mid_sums, mid_at[0], ff_local),
        mid_small_sum[:ff_local],
        cut(mid_sums, mid_at[0] + ffn_at[1], ff_local),
        mid_small_sum[ff_local : 2 * ff_local],
        mid_small_sum[2 * ff_local : 3 * ff_local],
        mid_small_sum[3 * ff_local : 4 * ff_local],
        cut(mid_sums, mid_at[1], ff_local).T,
        mid_tail[:, 0],
    )


def solution(mesh):
    placed = (
        P("row", "col"),
        P("row"),
        P("row"),
        P("row", None, "col"),
        P("col"),
        P("col"),
        P("col", "row"),
        P("row"),
        P("row"),
        P("row"),
        P("row", "col"),
        P("col"),
        P("row", "col"),
        P("col"),
        P("col"),
        P("col"),
        P("col", "row"),
        P("row"),
        P("row", "col"),
    )
    return jax.shard_map(
        functools.partial(body, mesh.shape["row"]),
        mesh=mesh,
        in_specs=placed,
        out_specs=(
            P("row", "col"),
            P("row", "col"),
            P("row"),
            P("row"),
            P("row", None, "col"),
            P("col"),
            P("col"),
            P("col", "row"),
            P("row"),
            P("row"),
            P("row"),
            P("row", "col"),
            P("col"),
            P("row", "col"),
            P("col"),
            P("col"),
            P("col"),
            P("col", "row"),
            P("row"),
        ),
        check_vma=False,
    )
```

```python
import functools
import math

import jax
import jax.numpy as jnp
from jax import lax
from jax.experimental.layout import Layout, with_layout_constraint
from jax.sharding import PartitionSpec as P


HD = 64
FF = 2730
GRID = 32
SEQ = 1025


EPSILON = 1e-06


def norm_forward(values, norm_gain, norm_shift):
    row_mean = jnp.mean(values, axis=-1, keepdims=True)
    centred = values - row_mean
    variance = jnp.mean(centred * centred, axis=-1, keepdims=True)
    inv_std = lax.rsqrt(variance + EPSILON)
    normed = centred * inv_std
    return (normed * norm_gain + norm_shift, normed, inv_std)


def norm_backward(upstream, normed, inv_std, norm_gain):
    scaled = upstream * norm_gain
    first_mean = jnp.mean(scaled, axis=-1, keepdims=True)
    second_mean = jnp.mean(scaled * normed, axis=-1, keepdims=True)
    delta = inv_std * (scaled - first_mean - normed * second_mean)
    return (delta, jnp.sum(upstream * normed, axis=0), jnp.sum(upstream, axis=0))


def rotary_tables(length, seq_len, grid_side, head_size):
    quarter = head_size // 4
    position = jnp.arange(length, dtype=jnp.int32) % seq_len
    patch_index = jnp.maximum(position - 1, 0)
    inside = (position > 0).astype(jnp.float32)
    row_pos = (patch_index // grid_side).astype(jnp.float32) * inside
    col_pos = (patch_index % grid_side).astype(jnp.float32) * inside
    frequency = jnp.exp(-math.log(10000.0) * jnp.arange(quarter, dtype=jnp.float32) / quarter)
    row_angle = row_pos[:, None] * frequency[None, :]
    col_angle = col_pos[:, None] * frequency[None, :]
    angles = jnp.concatenate([row_angle, row_angle, col_angle, col_angle], axis=1)
    return (jnp.cos(angles), jnp.sin(angles))


def rotate(values):
    pieces = jnp.split(values, 4, axis=-1)
    return jnp.concatenate([-pieces[1], pieces[0], -pieces[3], pieces[2]], axis=-1)


def rotate_transposed(values):
    pieces = jnp.split(values, 4, axis=-1)
    return jnp.concatenate([pieces[1], -pieces[0], pieces[3], -pieces[2]], axis=-1)


def apply_rotary(values, cosine_table, sine_table):
    return values * cosine_table[:, None, :] + rotate(values) * sine_table[:, None, :]


def rotary_back(grads, cosine_table, sine_table):
    return grads * cosine_table[:, None, :] + rotate_transposed(grads * sine_table[:, None, :])


def own_half(vector, column, half_width):
    return lax.dynamic_slice_in_dim(vector, column * half_width, half_width, axis=vector.ndim - 1)


def swap_columns(values):
    return lax.ppermute(values, "col", [(0, 1), (1, 0)])


def share_columns(partial_sums):
    half = partial_sums.shape[1] // 2
    column = lax.axis_index("col")
    own = lax.dynamic_slice_in_dim(partial_sums, column * half, half, axis=1)
    other = lax.dynamic_slice_in_dim(partial_sums, (1 - column) * half, half, axis=1)
    return own + swap_columns(other.astype(jnp.bfloat16)).astype(jnp.float32)


def join_columns(partial_sums):
    narrow = partial_sums.astype(jnp.bfloat16)
    return narrow.astype(jnp.float32) + swap_columns(narrow).astype(jnp.float32)


def gather_columns(values):
    other = swap_columns(values)
    first = lax.axis_index("col") == 0
    return jnp.concatenate(
        [jnp.where(first, values, other), jnp.where(first, other, values)], axis=1
    )


def hidden_totals(row_sums):
    return tuple(part + swap_columns(part) for part in row_sums)


def row_major(values):
    return with_layout_constraint(values, Layout((0, 1)))


def lane_round(width):
    return -(-width // 128) * 128


def pack(pieces):
    offsets = []
    padded = []
    position = 0
    for piece in pieces:
        width = lane_round(piece.shape[1])
        offsets.append(position)
        padded.append(jnp.pad(piece, ((0, 0), (0, width - piece.shape[1]))))
        position += width
    return jnp.concatenate(padded, axis=1), offsets


def spread(vector, rows_local, row_count):
    cols = -(-vector.shape[0] // rows_local)
    block = jnp.pad(vector, (0, rows_local * cols - vector.shape[0])).reshape(rows_local, cols)
    return jnp.tile(block, (row_count, 1))


def body(
    row_count,
    tokens,
    norm1_gain,
    norm1_bias,
    qkv_weight,
    query_bias,
    value_bias,
    proj_weight,
    proj_bias,
    norm2_gain,
    norm2_bias,
    gate_weight,
    gate_bias,
    up_weight,
    up_bias,
    inner_gain,
    inner_bias,
    down_weight,
    down_bias,
    cotangent,
):
    single = jnp.float32
    narrow = jnp.bfloat16
    local_rows = tokens.shape[0]
    half_width = tokens.shape[1]
    rows_local = norm1_gain.shape[0]
    model_width = rows_local * row_count
    ff_local = gate_weight.shape[1]
    head_local = half_width // HD
    images_local = local_rows // SEQ
    column = lax.axis_index("col")
    scaling = 1.0 / math.sqrt(HD)
    cosine_table, sine_table = rotary_tables(local_rows, SEQ, GRID, HD)

    def by_head(array):
        shaped = array.reshape(images_local, SEQ, head_local, HD).transpose(0, 2, 1, 3)
        return shaped.reshape(images_local * head_local, SEQ, HD)

    def from_head(array):
        shaped = array.reshape(images_local, head_local, SEQ, HD).transpose(0, 2, 1, 3)
        return shaped.reshape(local_rows, half_width)

    attn_pack, attn_at = pack(
        [
            qkv_weight.reshape(rows_local, 3 * half_width),
            proj_weight.T,
            jnp.stack(
                [norm1_gain, norm1_bias, proj_bias, norm2_gain, norm2_bias, down_bias], axis=1
            ),
        ]
    )
    attn_full = lax.all_gather(attn_pack, "row", axis=0, tiled=True)
    qkv_full = attn_full[:, attn_at[0] : attn_at[0] + 3 * half_width].reshape(
        model_width, 3, half_width
    )
    proj_t = attn_full[:, attn_at[1] : attn_at[1] + half_width]
    attn_vectors = attn_full[:, attn_at[2] : attn_at[2] + 6].astype(single)
    ffn_vectors = attn_vectors[:, 3:]

    whole_input = gather_columns(tokens).astype(single)
    normed_out, normed_one, inv_std_one = norm_forward(
        whole_input, attn_vectors[:, 0], attn_vectors[:, 1]
    )
    first_input = normed_out.astype(narrow)
    qkv_bias = jnp.stack(
        [query_bias.astype(single), jnp.zeros((half_width,), single), value_bias.astype(single)]
    )
    projected = (
        jnp.einsum("td,dpe->tpe", first_input, qkv_full, preferred_element_type=single) + qkv_bias
    )
    queries = apply_rotary(
        projected[:, 0].reshape(local_rows, head_local, HD), cosine_table, sine_table
    ).astype(narrow)
    keys_all = apply_rotary(
        projected[:, 1].reshape(local_rows, head_local, HD), cosine_table, sine_table
    ).astype(narrow)
    values_all = projected[:, 2].astype(narrow)

    def attend(operands):
        query_block, key_block, value_block = operands
        scores = (
            jnp.einsum("qd,kd->qk", query_block, key_block, preferred_element_type=single) * scaling
        )
        weights = jax.nn.softmax(scores, axis=-1)
        mixed = jnp.einsum(
            "qk,kd->qd", weights.astype(narrow), value_block, preferred_element_type=single
        )
        return mixed.astype(narrow)

    attended = from_head(
        lax.map(attend, (by_head(queries), by_head(keys_all), by_head(values_all)))
    )
    attn_partial = jnp.einsum("te,de->td", attended, proj_t, preferred_element_type=single)
    residual_half = (
        tokens.astype(single)
        + share_columns(attn_partial)
        + own_half(attn_vectors[:, 2], column, half_width)
    )
    residual_full = gather_columns(residual_half.astype(jnp.bfloat16)).astype(residual_half.dtype)

    ffn_pack, ffn_at = pack(
        [
            gate_weight,
            up_weight,
            down_weight.T,
        ]
    )
    ffn_full = lax.all_gather(ffn_pack, "row", axis=0, tiled=True)
    gate_up_full = ffn_full[:, : ffn_at[2]]
    down_t = ffn_full[:, ffn_at[2] : ffn_at[2] + ff_local]

    second_out, normed_two, inv_std_two = norm_forward(
        residual_full, ffn_vectors[:, 0], ffn_vectors[:, 1]
    )
    second_input = second_out.astype(narrow)
    gate_up_value = jnp.dot(second_input, gate_up_full, preferred_element_type=single)
    gate_value = gate_up_value[:, :ff_local] + gate_bias.astype(single)
    up_value = gate_up_value[:, ffn_at[1] : ffn_at[1] + ff_local] + up_bias.astype(single)
    sigmoid_gate = jax.nn.sigmoid(gate_value)
    hidden = gate_value * sigmoid_gate * up_value
    hidden_mean = hidden_totals((jnp.sum(hidden, axis=1),))[0][:, None] / FF
    hidden_centred = hidden - hidden_mean
    hidden_var = hidden_totals((jnp.sum(hidden_centred * hidden_centred, axis=1),))[0][:, None] / FF
    hidden_inv = lax.rsqrt(hidden_var + EPSILON)
    hidden_normed = hidden_centred * hidden_inv
    down_input = (hidden_normed * inner_gain.astype(single) + inner_bias.astype(single)).astype(
        narrow
    )
    out_full = gather_columns(cotangent)
    out_float = out_full.astype(single)
    down_weight_grad_t = jnp.einsum(
        "td,tf->df", out_full, down_input, preferred_element_type=single
    )
    down_bias_grad = jnp.sum(out_float, axis=0)
    normed_grad = jnp.einsum("td,df->tf", out_full, down_t, preferred_element_type=single)
    scaled_grad = normed_grad * inner_gain.astype(single)
    first_total, second_total = hidden_totals(
        (jnp.sum(scaled_grad, axis=1), jnp.sum(scaled_grad * hidden_normed, axis=1))
    )
    hidden_grad = hidden_inv * (
        scaled_grad - first_total[:, None] / FF - hidden_normed * (second_total[:, None] / FF)
    )
    inner_gain_grad = jnp.sum(normed_grad * hidden_normed, axis=0)
    inner_bias_grad = jnp.sum(normed_grad, axis=0)
    gate_grad = (
        hidden_grad * up_value * sigmoid_gate * (1.0 + gate_value * (1.0 - sigmoid_gate))
    ).astype(narrow)
    up_grad = (hidden_grad * gate_value * sigmoid_gate).astype(narrow)
    gate_bias_grad = jnp.sum(gate_grad.astype(single), axis=0)
    up_bias_grad = jnp.sum(up_grad.astype(single), axis=0)
    gate_up_grad, _ = pack([gate_grad, up_grad, jnp.zeros((local_rows, 0), narrow)])
    gate_up_weight_grad = jnp.einsum(
        "td,tf->df", second_input, gate_up_grad, preferred_element_type=single
    )
    second_back = join_columns(
        jnp.einsum("tf,df->td", gate_up_grad, gate_up_full, preferred_element_type=single)
    )
    second_delta, gain_two_grad, shift_two_grad = norm_backward(
        second_back, normed_two, inv_std_two, ffn_vectors[:, 0]
    )
    residual_grad = out_float + second_delta
    attn_grad = residual_grad.astype(narrow)
    proj_bias_grad = jnp.sum(attn_grad.astype(single), axis=0)
    proj_weight_grad_t = jnp.einsum(
        "td,te->de", attn_grad, attended, preferred_element_type=single
    )
    mid_small = jnp.concatenate([gate_bias_grad, up_bias_grad, inner_gain_grad, inner_bias_grad])
    mid_pack, mid_at = pack(
        [
            row_major(gate_up_weight_grad.astype(narrow)),
            row_major(down_weight_grad_t.astype(narrow)),
            row_major(proj_weight_grad_t.astype(narrow)),
            jnp.stack(
                [gain_two_grad, shift_two_grad, down_bias_grad, proj_bias_grad], axis=1
            ).astype(narrow),
            spread(mid_small, rows_local, row_count).astype(narrow),
        ]
    )
    mid_pack, attn_grad_held, down_input_held = lax.optimization_barrier(
        (mid_pack, attn_grad, down_input)
    )
    ffn_partial = jnp.einsum(
        "tf,df->td", down_input_held, down_t, preferred_element_type=single
    )
    layer_out = (
        residual_half
        + share_columns(ffn_partial)
        + own_half(ffn_vectors[:, 2], column, half_width)
    ).astype(narrow)
    mid_sums = lax.psum_scatter(mid_pack, "row", scatter_dimension=0, tiled=True).astype(single)
    attended_grad = jnp.einsum(
        "td,de->te", attn_grad_held, proj_t, preferred_element_type=single
    ).astype(narrow)

    def attend_back(operands):
        query_block, key_block, value_block, grad_block = operands
        scores = (
            jnp.einsum("qd,kd->qk", query_block, key_block, preferred_element_type=single) * scaling
        )
        weights = jax.nn.softmax(scores, axis=-1)
        value_grad = jnp.einsum(
            "qk,qd->kd", weights.astype(narrow), grad_block, preferred_element_type=single
        )
        weight_grad = jnp.einsum(
            "qd,kd->qk", grad_block, value_block, preferred_element_type=single
        )
        score_grad = (
            weights * (weight_grad - jnp.sum(weight_grad * weights, axis=-1, keepdims=True))
        ).astype(narrow)
        query_grad = (
            jnp.einsum("qk,kd->qd", score_grad, key_block, preferred_element_type=single) * scaling
        )
        key_grad = (
            jnp.einsum("qk,qd->kd", score_grad, query_block, preferred_element_type=single)
            * scaling
        )
        return (query_grad, key_grad, value_grad)

    query_grads, key_grads, value_grads = lax.map(
        attend_back,
        (by_head(queries), by_head(keys_all), by_head(values_all), by_head(attended_grad)),
    )
    back_cosine, back_sine, query_grads = lax.optimization_barrier(
        (cosine_table, sine_table, query_grads)
    )
    query_pre = rotary_back(
        from_head(query_grads).reshape(local_rows, head_local, HD), back_cosine, back_sine
    )
    key_pre = rotary_back(
        from_head(key_grads).reshape(local_rows, head_local, HD), back_cosine, back_sine
    )
    qkv_grad = jnp.stack(
        [
            query_pre.reshape(local_rows, half_width),
            key_pre.reshape(local_rows, half_width),
            from_head(value_grads),
        ],
        axis=1,
    ).astype(narrow)
    qkv_grad_float = qkv_grad.astype(single)
    query_bias_grad = jnp.sum(qkv_grad_float[:, 0], axis=0)
    value_bias_grad = jnp.sum(qkv_grad_float[:, 2], axis=0)
    qkv_weight_grad = jnp.einsum(
        "td,tpe->dpe", first_input, qkv_grad, preferred_element_type=single
    )
    first_back = join_columns(
        jnp.einsum("tpe,dpe->td", qkv_grad, qkv_full, preferred_element_type=single)
    )
    first_delta, gain_one_grad, shift_one_grad = norm_backward(
        first_back, normed_one, inv_std_one, attn_vectors[:, 0]
    )
    input_grad = own_half(residual_grad + first_delta, column, half_width).astype(narrow)
    end_pack, end_at = pack(
        [
            qkv_weight_grad.reshape(model_width, 3 * half_width).astype(narrow),
            jnp.stack([gain_one_grad, shift_one_grad], axis=1).astype(narrow),
            spread(
                jnp.concatenate([query_bias_grad, value_bias_grad]), rows_local, row_count
            ).astype(narrow),
        ]
    )
    end_pack, mid_sums = lax.optimization_barrier((end_pack, mid_sums))
    end_sums = lax.psum_scatter(end_pack, "row", scatter_dimension=0, tiled=True).astype(single)

    def cut(sums, offset, width):
        return sums[:, offset : offset + width]

    mid_vectors = cut(mid_sums, mid_at[3], 4)
    mid_small_sum = cut(mid_sums, mid_at[4], -(-mid_small.shape[0] // rows_local)).reshape(-1)
    end_vectors = cut(end_sums, end_at[1], 2)
    end_small_sum = cut(end_sums, end_at[2], -(-2 * half_width // rows_local)).reshape(-1)
    return (
        layer_out,
        input_grad,
        end_vectors[:, 0],
        end_vectors[:, 1],
        cut(end_sums, end_at[0], 3 * half_width).reshape(rows_local, 3, half_width),
        end_small_sum[:half_width],
        end_small_sum[half_width : 2 * half_width],
        cut(mid_sums, mid_at[2], half_width).T,
        mid_vectors[:, 3],
        mid_vectors[:, 0],
        mid_vectors[:, 1],
        cut(mid_sums, mid_at[0], ff_local),
        mid_small_sum[:ff_local],
        cut(mid_sums, mid_at[0] + ffn_at[1], ff_local),
        mid_small_sum[ff_local : 2 * ff_local],
        mid_small_sum[2 * ff_local : 3 * ff_local],
        mid_small_sum[3 * ff_local : 4 * ff_local],
        cut(mid_sums, mid_at[1], ff_local).T,
        mid_vectors[:, 2],
    )


def solution(mesh):
    placed = (
        P("row", "col"),
        P("row"),
        P("row"),
        P("row", None, "col"),
        P("col"),
        P("col"),
        P("col", "row"),
        P("row"),
        P("row"),
        P("row"),
        P("row", "col"),
        P("col"),
        P("row", "col"),
        P("col"),
        P("col"),
        P("col"),
        P("col", "row"),
        P("row"),
        P("row", "col"),
    )
    return jax.shard_map(
        functools.partial(body, mesh.shape["row"]),
        mesh=mesh,
        in_specs=placed,
        out_specs=(
            P("row", "col"),
            P("row", "col"),
            P("row"),
            P("row"),
            P("row", None, "col"),
            P("col"),
            P("col"),
            P("col", "row"),
            P("row"),
            P("row"),
            P("row"),
            P("row", "col"),
            P("col"),
            P("row", "col"),
            P("col"),
            P("col"),
            P("col"),
            P("col", "row"),
            P("row"),
        ),
        check_vma=False,
    )
```

```python
import functools
import math

import jax
import jax.numpy as jnp
from jax import lax
from jax.experimental.layout import Layout, with_layout_constraint
from jax.sharding import PartitionSpec as P


HD = 64
FF = 2730
GRID = 32
SEQ = 1025


EPSILON = 1e-06


def norm_forward(values, norm_gain, norm_shift):
    row_mean = jnp.mean(values, axis=-1, keepdims=True)
    centred = values - row_mean
    variance = jnp.mean(centred * centred, axis=-1, keepdims=True)
    inv_std = lax.rsqrt(variance + EPSILON)
    normed = centred * inv_std
    return (normed * norm_gain + norm_shift, normed, inv_std)


def norm_backward(upstream, normed, inv_std, norm_gain):
    scaled = upstream * norm_gain
    first_mean = jnp.mean(scaled, axis=-1, keepdims=True)
    second_mean = jnp.mean(scaled * normed, axis=-1, keepdims=True)
    delta = inv_std * (scaled - first_mean - normed * second_mean)
    return (delta, jnp.sum(upstream * normed, axis=0), jnp.sum(upstream, axis=0))


def rotary_tables(length, seq_len, grid_side, head_size):
    quarter = head_size // 4
    position = jnp.arange(length, dtype=jnp.int32) % seq_len
    patch_index = jnp.maximum(position - 1, 0)
    inside = (position > 0).astype(jnp.float32)
    row_pos = (patch_index // grid_side).astype(jnp.float32) * inside
    col_pos = (patch_index % grid_side).astype(jnp.float32) * inside
    frequency = jnp.exp(-math.log(10000.0) * jnp.arange(quarter, dtype=jnp.float32) / quarter)
    row_angle = row_pos[:, None] * frequency[None, :]
    col_angle = col_pos[:, None] * frequency[None, :]
    angles = jnp.concatenate([row_angle, row_angle, col_angle, col_angle], axis=1)
    return (jnp.cos(angles), jnp.sin(angles))


def rotate(values):
    pieces = jnp.split(values, 4, axis=-1)
    return jnp.concatenate([-pieces[1], pieces[0], -pieces[3], pieces[2]], axis=-1)


def rotate_transposed(values):
    pieces = jnp.split(values, 4, axis=-1)
    return jnp.concatenate([pieces[1], -pieces[0], pieces[3], -pieces[2]], axis=-1)


def apply_rotary(values, cosine_table, sine_table):
    return values * cosine_table[:, None, :] + rotate(values) * sine_table[:, None, :]


def rotary_back(grads, cosine_table, sine_table):
    return grads * cosine_table[:, None, :] + rotate_transposed(grads * sine_table[:, None, :])


def own_half(vector, column, half_width):
    return lax.dynamic_slice_in_dim(vector, column * half_width, half_width, axis=vector.ndim - 1)


def swap_columns(values):
    return lax.ppermute(values, "col", [(0, 1), (1, 0)])


def share_columns(partial_sums):
    half = partial_sums.shape[1] // 2
    column = lax.axis_index("col")
    own = lax.dynamic_slice_in_dim(partial_sums, column * half, half, axis=1)
    other = lax.dynamic_slice_in_dim(partial_sums, (1 - column) * half, half, axis=1)
    return own + swap_columns(other.astype(jnp.bfloat16)).astype(jnp.float32)


def join_columns(partial_sums):
    narrow = partial_sums.astype(jnp.bfloat16)
    return narrow.astype(jnp.float32) + swap_columns(narrow).astype(jnp.float32)


def gather_columns(values):
    other = swap_columns(values)
    half = values.shape[1]
    column = lax.axis_index("col")
    full = jnp.zeros((values.shape[0], 2 * half), values.dtype)
    full = lax.dynamic_update_slice_in_dim(full, values, column * half, axis=1)
    return lax.dynamic_update_slice_in_dim(full, other, (1 - column) * half, axis=1)


def hidden_totals(row_sums):
    return tuple(part + swap_columns(part) for part in row_sums)


def row_major(values):
    return with_layout_constraint(values, Layout((0, 1)))


def lane_round(width):
    return -(-width // 128) * 128


def pack(pieces):
    offsets = []
    padded = []
    position = 0
    for piece in pieces:
        width = lane_round(piece.shape[1])
        offsets.append(position)
        padded.append(jnp.pad(piece, ((0, 0), (0, width - piece.shape[1]))))
        position += width
    return jnp.concatenate(padded, axis=1), offsets


def spread(vector, rows_local, row_count):
    cols = -(-vector.shape[0] // rows_local)
    block = jnp.pad(vector, (0, rows_local * cols - vector.shape[0])).reshape(rows_local, cols)
    return jnp.tile(block, (row_count, 1))


def body(
    row_count,
    tokens,
    norm1_gain,
    norm1_bias,
    qkv_weight,
    query_bias,
    value_bias,
    proj_weight,
    proj_bias,
    norm2_gain,
    norm2_bias,
    gate_weight,
    gate_bias,
    up_weight,
    up_bias,
    inner_gain,
    inner_bias,
    down_weight,
    down_bias,
    cotangent,
):
    single = jnp.float32
    narrow = jnp.bfloat16
    local_rows = tokens.shape[0]
    half_width = tokens.shape[1]
    rows_local = norm1_gain.shape[0]
    model_width = rows_local * row_count
    ff_local = gate_weight.shape[1]
    head_local = half_width // HD
    images_local = local_rows // SEQ
    column = lax.axis_index("col")
    scaling = 1.0 / math.sqrt(HD)
    cosine_table, sine_table = rotary_tables(local_rows, SEQ, GRID, HD)

    def by_head(array):
        shaped = array.reshape(images_local, SEQ, head_local, HD).transpose(0, 2, 1, 3)
        return shaped.reshape(images_local * head_local, SEQ, HD)

    def from_head(array):
        shaped = array.reshape(images_local, head_local, SEQ, HD).transpose(0, 2, 1, 3)
        return shaped.reshape(local_rows, half_width)

    attn_pack, attn_at = pack(
        [
            qkv_weight.reshape(rows_local, 3 * half_width),
            proj_weight.T,
            jnp.stack(
                [norm1_gain, norm1_bias, proj_bias, norm2_gain, norm2_bias, down_bias], axis=1
            ),
        ]
    )
    attn_full = lax.all_gather(attn_pack, "row", axis=0, tiled=True)
    qkv_full = attn_full[:, attn_at[0] : attn_at[0] + 3 * half_width].reshape(
        model_width, 3, half_width
    )
    proj_t = attn_full[:, attn_at[1] : attn_at[1] + half_width]
    attn_vectors = attn_full[:, attn_at[2] : attn_at[2] + 6].astype(single)
    ffn_vectors = attn_vectors[:, 3:]

    whole_input = gather_columns(tokens).astype(single)
    normed_out, normed_one, inv_std_one = norm_forward(
        whole_input, attn_vectors[:, 0], attn_vectors[:, 1]
    )
    first_input = normed_out.astype(narrow)
    qkv_bias = jnp.stack(
        [query_bias.astype(single), jnp.zeros((half_width,), single), value_bias.astype(single)]
    )
    projected = (
        jnp.einsum("td,dpe->tpe", first_input, qkv_full, preferred_element_type=single) + qkv_bias
    )
    queries = apply_rotary(
        projected[:, 0].reshape(local_rows, head_local, HD), cosine_table, sine_table
    ).astype(narrow)
    keys_all = apply_rotary(
        projected[:, 1].reshape(local_rows, head_local, HD), cosine_table, sine_table
    ).astype(narrow)
    values_all = projected[:, 2].astype(narrow)

    def attend(operands):
        query_block, key_block, value_block = operands
        scores = (
            jnp.einsum("qd,kd->qk", query_block, key_block, preferred_element_type=single) * scaling
        )
        weights = jax.nn.softmax(scores, axis=-1)
        mixed = jnp.einsum(
            "qk,kd->qd", weights.astype(narrow), value_block, preferred_element_type=single
        )
        return mixed.astype(narrow)

    attended = from_head(
        lax.map(attend, (by_head(queries), by_head(keys_all), by_head(values_all)))
    )
    attn_partial = jnp.einsum("te,de->td", attended, proj_t, preferred_element_type=single)
    residual_half = (
        tokens.astype(single)
        + share_columns(attn_partial)
        + own_half(attn_vectors[:, 2], column, half_width)
    )
    residual_full = gather_columns(residual_half.astype(jnp.bfloat16)).astype(residual_half.dtype)

    ffn_pack, ffn_at = pack(
        [
            gate_weight,
            up_weight,
            down_weight.T,
        ]
    )
    ffn_full = lax.all_gather(ffn_pack, "row", axis=0, tiled=True)
    gate_up_full = ffn_full[:, : ffn_at[2]]
    down_t = ffn_full[:, ffn_at[2] : ffn_at[2] + ff_local]

    second_out, normed_two, inv_std_two = norm_forward(
        residual_full, ffn_vectors[:, 0], ffn_vectors[:, 1]
    )
    second_input = second_out.astype(narrow)
    gate_up_value = jnp.dot(second_input, gate_up_full, preferred_element_type=single)
    gate_value = gate_up_value[:, :ff_local] + gate_bias.astype(single)
    up_value = gate_up_value[:, ffn_at[1] : ffn_at[1] + ff_local] + up_bias.astype(single)
    sigmoid_gate = jax.nn.sigmoid(gate_value)
    hidden = gate_value * sigmoid_gate * up_value
    hidden_mean = hidden_totals((jnp.sum(hidden, axis=1),))[0][:, None] / FF
    hidden_centred = hidden - hidden_mean
    hidden_var = hidden_totals((jnp.sum(hidden_centred * hidden_centred, axis=1),))[0][:, None] / FF
    hidden_inv = lax.rsqrt(hidden_var + EPSILON)
    hidden_normed = hidden_centred * hidden_inv
    down_input = (hidden_normed * inner_gain.astype(single) + inner_bias.astype(single)).astype(
        narrow
    )
    out_full = gather_columns(cotangent)
    out_float = out_full.astype(single)
    down_weight_grad_t = jnp.einsum(
        "td,tf->df", out_full, down_input, preferred_element_type=single
    )
    down_bias_grad = jnp.sum(out_float, axis=0)
    normed_grad = jnp.einsum("td,df->tf", out_full, down_t, preferred_element_type=single)
    scaled_grad = normed_grad * inner_gain.astype(single)
    first_total, second_total = hidden_totals(
        (jnp.sum(scaled_grad, axis=1), jnp.sum(scaled_grad * hidden_normed, axis=1))
    )
    hidden_grad = hidden_inv * (
        scaled_grad - first_total[:, None] / FF - hidden_normed * (second_total[:, None] / FF)
    )
    inner_gain_grad = jnp.sum(normed_grad * hidden_normed, axis=0)
    inner_bias_grad = jnp.sum(normed_grad, axis=0)
    gate_grad = (
        hidden_grad * up_value * sigmoid_gate * (1.0 + gate_value * (1.0 - sigmoid_gate))
    ).astype(narrow)
    up_grad = (hidden_grad * gate_value * sigmoid_gate).astype(narrow)
    gate_bias_grad = jnp.sum(gate_grad.astype(single), axis=0)
    up_bias_grad = jnp.sum(up_grad.astype(single), axis=0)
    gate_up_grad, _ = pack([gate_grad, up_grad, jnp.zeros((local_rows, 0), narrow)])
    gate_up_weight_grad = jnp.einsum(
        "td,tf->df", second_input, gate_up_grad, preferred_element_type=single
    )
    second_back = join_columns(
        jnp.einsum("tf,df->td", gate_up_grad, gate_up_full, preferred_element_type=single)
    )
    second_delta, gain_two_grad, shift_two_grad = norm_backward(
        second_back, normed_two, inv_std_two, ffn_vectors[:, 0]
    )
    residual_grad = out_float + second_delta
    attn_grad = residual_grad.astype(narrow)
    proj_bias_grad = jnp.sum(attn_grad.astype(single), axis=0)
    proj_weight_grad_t = jnp.einsum(
        "td,te->de", attn_grad, attended, preferred_element_type=single
    )
    mid_small = jnp.concatenate([gate_bias_grad, up_bias_grad, inner_gain_grad, inner_bias_grad])
    mid_pack, mid_at = pack(
        [
            row_major(gate_up_weight_grad.astype(narrow)),
            row_major(down_weight_grad_t.astype(narrow)),
            row_major(proj_weight_grad_t.astype(narrow)),
            jnp.stack(
                [gain_two_grad, shift_two_grad, down_bias_grad, proj_bias_grad], axis=1
            ).astype(narrow),
            spread(mid_small, rows_local, row_count).astype(narrow),
        ]
    )
    mid_pack, attn_grad_held, down_input_held = lax.optimization_barrier(
        (mid_pack, attn_grad, down_input)
    )
    ffn_partial = jnp.einsum(
        "tf,df->td", down_input_held, down_t, preferred_element_type=single
    )
    layer_out = (
        residual_half
        + share_columns(ffn_partial)
        + own_half(ffn_vectors[:, 2], column, half_width)
    ).astype(narrow)
    mid_sums = lax.psum_scatter(mid_pack, "row", scatter_dimension=0, tiled=True).astype(single)
    attended_grad = jnp.einsum(
        "td,de->te", attn_grad_held, proj_t, preferred_element_type=single
    ).astype(narrow)

    def attend_back(operands):
        query_block, key_block, value_block, grad_block = operands
        scores = (
            jnp.einsum("qd,kd->qk", query_block, key_block, preferred_element_type=single) * scaling
        )
        weights = jax.nn.softmax(scores, axis=-1)
        value_grad = jnp.einsum(
            "qk,qd->kd", weights.astype(narrow), grad_block, preferred_element_type=single
        )
        weight_grad = jnp.einsum(
            "qd,kd->qk", grad_block, value_block, preferred_element_type=single
        )
        score_grad = (
            weights * (weight_grad - jnp.sum(weight_grad * weights, axis=-1, keepdims=True))
        ).astype(narrow)
        query_grad = (
            jnp.einsum("qk,kd->qd", score_grad, key_block, preferred_element_type=single) * scaling
        )
        key_grad = (
            jnp.einsum("qk,qd->kd", score_grad, query_block, preferred_element_type=single)
            * scaling
        )
        return (query_grad, key_grad, value_grad)

    query_grads, key_grads, value_grads = lax.map(
        attend_back,
        (by_head(queries), by_head(keys_all), by_head(values_all), by_head(attended_grad)),
    )
    query_pre = rotary_back(
        from_head(query_grads).reshape(local_rows, head_local, HD), cosine_table, sine_table
    )
    key_pre = rotary_back(
        from_head(key_grads).reshape(local_rows, head_local, HD), cosine_table, sine_table
    )
    qkv_grad = jnp.stack(
        [
            query_pre.reshape(local_rows, half_width),
            key_pre.reshape(local_rows, half_width),
            from_head(value_grads),
        ],
        axis=1,
    ).astype(narrow)
    qkv_grad_float = qkv_grad.astype(single)
    query_bias_grad = jnp.sum(qkv_grad_float[:, 0], axis=0)
    value_bias_grad = jnp.sum(qkv_grad_float[:, 2], axis=0)
    qkv_weight_grad = jnp.einsum(
        "td,tpe->dpe", first_input, qkv_grad, preferred_element_type=single
    )
    first_back = join_columns(
        jnp.einsum("tpe,dpe->td", qkv_grad, qkv_full, preferred_element_type=single)
    )
    first_delta, gain_one_grad, shift_one_grad = norm_backward(
        first_back, normed_one, inv_std_one, attn_vectors[:, 0]
    )
    input_grad = own_half(residual_grad + first_delta, column, half_width).astype(narrow)
    end_pack, end_at = pack(
        [
            qkv_weight_grad.reshape(model_width, 3 * half_width).astype(narrow),
            jnp.stack([gain_one_grad, shift_one_grad], axis=1).astype(narrow),
            spread(
                jnp.concatenate([query_bias_grad, value_bias_grad]), rows_local, row_count
            ).astype(narrow),
        ]
    )
    end_pack, mid_sums = lax.optimization_barrier((end_pack, mid_sums))
    end_sums = lax.psum_scatter(end_pack, "row", scatter_dimension=0, tiled=True).astype(single)

    def cut(sums, offset, width):
        return sums[:, offset : offset + width]

    mid_vectors = cut(mid_sums, mid_at[3], 4)
    mid_small_sum = cut(mid_sums, mid_at[4], -(-mid_small.shape[0] // rows_local)).reshape(-1)
    end_vectors = cut(end_sums, end_at[1], 2)
    end_small_sum = cut(end_sums, end_at[2], -(-2 * half_width // rows_local)).reshape(-1)
    return (
        layer_out,
        input_grad,
        end_vectors[:, 0],
        end_vectors[:, 1],
        cut(end_sums, end_at[0], 3 * half_width).reshape(rows_local, 3, half_width),
        end_small_sum[:half_width],
        end_small_sum[half_width : 2 * half_width],
        cut(mid_sums, mid_at[2], half_width).T,
        mid_vectors[:, 3],
        mid_vectors[:, 0],
        mid_vectors[:, 1],
        cut(mid_sums, mid_at[0], ff_local),
        mid_small_sum[:ff_local],
        cut(mid_sums, mid_at[0] + ffn_at[1], ff_local),
        mid_small_sum[ff_local : 2 * ff_local],
        mid_small_sum[2 * ff_local : 3 * ff_local],
        mid_small_sum[3 * ff_local : 4 * ff_local],
        cut(mid_sums, mid_at[1], ff_local).T,
        mid_vectors[:, 2],
    )


def solution(mesh):
    placed = (
        P("row", "col"),
        P("row"),
        P("row"),
        P("row", None, "col"),
        P("col"),
        P("col"),
        P("col", "row"),
        P("row"),
        P("row"),
        P("row"),
        P("row", "col"),
        P("col"),
        P("row", "col"),
        P("col"),
        P("col"),
        P("col"),
        P("col", "row"),
        P("row"),
        P("row", "col"),
    )
    return jax.shard_map(
        functools.partial(body, mesh.shape["row"]),
        mesh=mesh,
        in_specs=placed,
        out_specs=(
            P("row", "col"),
            P("row", "col"),
            P("row"),
            P("row"),
            P("row", None, "col"),
            P("col"),
            P("col"),
            P("col", "row"),
            P("row"),
            P("row"),
            P("row"),
            P("row", "col"),
            P("col"),
            P("row", "col"),
            P("col"),
            P("col"),
            P("col"),
            P("col", "row"),
            P("row"),
        ),
        check_vma=False,
    )
```

```python
import functools
import math

import jax
import jax.numpy as jnp
from jax import lax
from jax.experimental.layout import Layout, with_layout_constraint
from jax.sharding import PartitionSpec as P


HD = 64
FF = 2730
GRID = 32
SEQ = 1025


EPSILON = 1e-06


def norm_forward(values, norm_gain, norm_shift):
    row_mean = jnp.mean(values, axis=-1, keepdims=True)
    centred = values - row_mean
    variance = jnp.mean(centred * centred, axis=-1, keepdims=True)
    inv_std = lax.rsqrt(variance + EPSILON)
    normed = centred * inv_std
    return (normed * norm_gain + norm_shift, normed, inv_std)


def norm_backward(upstream, normed, inv_std, norm_gain):
    scaled = upstream * norm_gain
    first_mean = jnp.mean(scaled, axis=-1, keepdims=True)
    second_mean = jnp.mean(scaled * normed, axis=-1, keepdims=True)
    delta = inv_std * (scaled - first_mean - normed * second_mean)
    return (delta, jnp.sum(upstream * normed, axis=0), jnp.sum(upstream, axis=0))


def rotary_tables(length, seq_len, grid_side, head_size):
    quarter = head_size // 4
    position = jnp.arange(length, dtype=jnp.int32) % seq_len
    patch_index = jnp.maximum(position - 1, 0)
    inside = (position > 0).astype(jnp.float32)
    row_pos = (patch_index // grid_side).astype(jnp.float32) * inside
    col_pos = (patch_index % grid_side).astype(jnp.float32) * inside
    frequency = jnp.exp(-math.log(10000.0) * jnp.arange(quarter, dtype=jnp.float32) / quarter)
    row_angle = row_pos[:, None] * frequency[None, :]
    col_angle = col_pos[:, None] * frequency[None, :]
    angles = jnp.concatenate([row_angle, row_angle, col_angle, col_angle], axis=1)
    return (jnp.cos(angles), jnp.sin(angles))


def rotate(values):
    pieces = jnp.split(values, 4, axis=-1)
    return jnp.concatenate([-pieces[1], pieces[0], -pieces[3], pieces[2]], axis=-1)


def rotate_transposed(values):
    pieces = jnp.split(values, 4, axis=-1)
    return jnp.concatenate([pieces[1], -pieces[0], pieces[3], -pieces[2]], axis=-1)


def apply_rotary(values, cosine_table, sine_table):
    return values * cosine_table[:, None, :] + rotate(values) * sine_table[:, None, :]


def rotary_back(grads, cosine_table, sine_table):
    return grads * cosine_table[:, None, :] + rotate_transposed(grads * sine_table[:, None, :])


def own_half(vector, column, half_width):
    return lax.dynamic_slice_in_dim(vector, column * half_width, half_width, axis=vector.ndim - 1)


def swap_columns(values):
    return lax.ppermute(values, "col", [(0, 1), (1, 0)])


def share_columns(partial_sums):
    half = partial_sums.shape[1] // 2
    column = lax.axis_index("col")
    own = lax.dynamic_slice_in_dim(partial_sums, column * half, half, axis=1)
    other = lax.dynamic_slice_in_dim(partial_sums, (1 - column) * half, half, axis=1)
    return own + swap_columns(other.astype(jnp.bfloat16)).astype(jnp.float32)


def join_columns(partial_sums):
    narrow = partial_sums.astype(jnp.bfloat16)
    return narrow.astype(jnp.float32) + swap_columns(narrow).astype(jnp.float32)


def gather_columns(values):
    other = swap_columns(values)
    first = lax.axis_index("col") == 0
    return jnp.concatenate(
        [jnp.where(first, values, other), jnp.where(first, other, values)], axis=1
    )


def hidden_totals(row_sums):
    return tuple(part + swap_columns(part) for part in row_sums)


def row_major(values):
    return with_layout_constraint(values, Layout((0, 1)))


def lane_round(width):
    return -(-width // 128) * 128


def pack(pieces):
    offsets = []
    padded = []
    position = 0
    for piece in pieces:
        width = lane_round(piece.shape[1])
        offsets.append(position)
        padded.append(jnp.pad(piece, ((0, 0), (0, width - piece.shape[1]))))
        position += width
    return jnp.concatenate(padded, axis=1), offsets


def spread(vector, rows_local, row_count):
    cols = -(-vector.shape[0] // rows_local)
    block = jnp.pad(vector, (0, rows_local * cols - vector.shape[0])).reshape(rows_local, cols)
    return jnp.tile(block, (row_count, 1))


def body(
    row_count,
    tokens,
    norm1_gain,
    norm1_bias,
    qkv_weight,
    query_bias,
    value_bias,
    proj_weight,
    proj_bias,
    norm2_gain,
    norm2_bias,
    gate_weight,
    gate_bias,
    up_weight,
    up_bias,
    inner_gain,
    inner_bias,
    down_weight,
    down_bias,
    cotangent,
):
    single = jnp.float32
    narrow = jnp.bfloat16
    local_rows = tokens.shape[0]
    half_width = tokens.shape[1]
    rows_local = norm1_gain.shape[0]
    model_width = rows_local * row_count
    ff_local = gate_weight.shape[1]
    head_local = half_width // HD
    images_local = local_rows // SEQ
    column = lax.axis_index("col")
    scaling = 1.0 / math.sqrt(HD)
    cosine_table, sine_table = rotary_tables(local_rows, SEQ, GRID, HD)

    def by_head(array):
        shaped = array.reshape(images_local, SEQ, head_local, HD).transpose(0, 2, 1, 3)
        return shaped.reshape(images_local * head_local, SEQ, HD)

    def from_head(array):
        shaped = array.reshape(images_local, head_local, SEQ, HD).transpose(0, 2, 1, 3)
        return shaped.reshape(local_rows, half_width)

    attn_pack, attn_at = pack(
        [
            qkv_weight.reshape(rows_local, 3 * half_width),
            proj_weight.T,
            jnp.stack(
                [norm1_gain, norm1_bias, proj_bias, norm2_gain, norm2_bias, down_bias], axis=1
            ),
        ]
    )
    attn_full = lax.all_gather(attn_pack, "row", axis=0, tiled=True)
    qkv_full = attn_full[:, attn_at[0] : attn_at[0] + 3 * half_width].reshape(
        model_width, 3, half_width
    )
    proj_t = attn_full[:, attn_at[1] : attn_at[1] + half_width]
    attn_vectors = attn_full[:, attn_at[2] : attn_at[2] + 6].astype(single)
    ffn_vectors = attn_vectors[:, 3:]

    whole_input = gather_columns(tokens).astype(single)
    normed_out, normed_one, inv_std_one = norm_forward(
        whole_input, attn_vectors[:, 0], attn_vectors[:, 1]
    )
    first_input = normed_out.astype(narrow)
    qkv_bias = jnp.stack(
        [query_bias.astype(single), jnp.zeros((half_width,), single), value_bias.astype(single)]
    )
    projected = (
        jnp.einsum("td,dpe->tpe", first_input, qkv_full, preferred_element_type=single) + qkv_bias
    )
    queries = apply_rotary(
        projected[:, 0].reshape(local_rows, head_local, HD), cosine_table, sine_table
    ).astype(narrow)
    keys_all = apply_rotary(
        projected[:, 1].reshape(local_rows, head_local, HD), cosine_table, sine_table
    ).astype(narrow)
    values_all = projected[:, 2].astype(narrow)

    def attend(operands):
        query_block, key_block, value_block = operands
        scores = (
            jnp.einsum("qd,kd->qk", query_block, key_block, preferred_element_type=single) * scaling
        )
        weights = jax.nn.softmax(scores, axis=-1)
        mixed = jnp.einsum(
            "qk,kd->qd", weights.astype(narrow), value_block, preferred_element_type=single
        )
        return mixed.astype(narrow)

    attended = from_head(
        lax.map(attend, (by_head(queries), by_head(keys_all), by_head(values_all)))
    )
    attn_partial = jnp.einsum("te,de->td", attended, proj_t, preferred_element_type=single)
    residual_half = (
        tokens.astype(single)
        + share_columns(attn_partial)
        + own_half(attn_vectors[:, 2], column, half_width)
    )
    residual_full = gather_columns(residual_half.astype(jnp.bfloat16)).astype(residual_half.dtype)

    ffn_pack, ffn_at = pack(
        [
            gate_weight,
            up_weight,
            down_weight.T,
        ]
    )
    ffn_full = lax.all_gather(ffn_pack, "row", axis=0, tiled=True)
    gate_up_full = ffn_full[:, : ffn_at[2]]
    down_t = ffn_full[:, ffn_at[2] : ffn_at[2] + ff_local]
    down_t_padded = ffn_full[:, ffn_at[2] : ffn_at[2] + lane_round(ff_local)]

    second_out, normed_two, inv_std_two = norm_forward(
        residual_full, ffn_vectors[:, 0], ffn_vectors[:, 1]
    )
    second_input = second_out.astype(narrow)
    gate_up_value = jnp.dot(second_input, gate_up_full, preferred_element_type=single)
    gate_value = gate_up_value[:, :ff_local] + gate_bias.astype(single)
    up_value = gate_up_value[:, ffn_at[1] : ffn_at[1] + ff_local] + up_bias.astype(single)
    sigmoid_gate = jax.nn.sigmoid(gate_value)
    hidden = gate_value * sigmoid_gate * up_value
    hidden_mean = hidden_totals((jnp.sum(hidden, axis=1),))[0][:, None] / FF
    hidden_centred = hidden - hidden_mean
    hidden_var = hidden_totals((jnp.sum(hidden_centred * hidden_centred, axis=1),))[0][:, None] / FF
    hidden_inv = lax.rsqrt(hidden_var + EPSILON)
    hidden_normed = hidden_centred * hidden_inv
    down_input = (hidden_normed * inner_gain.astype(single) + inner_bias.astype(single)).astype(
        narrow
    )
    down_padded = jnp.pad(down_input, ((0, 0), (0, lane_round(ff_local) - ff_local)))
    out_full = gather_columns(cotangent)
    out_float = out_full.astype(single)
    down_weight_grad_t = jnp.einsum(
        "td,tf->df", out_full, down_padded, preferred_element_type=single
    )
    down_bias_grad = jnp.sum(out_float, axis=0)
    normed_grad = jnp.einsum("td,df->tf", out_full, down_t, preferred_element_type=single)
    scaled_grad = normed_grad * inner_gain.astype(single)
    first_total, second_total = hidden_totals(
        (jnp.sum(scaled_grad, axis=1), jnp.sum(scaled_grad * hidden_normed, axis=1))
    )
    hidden_grad = hidden_inv * (
        scaled_grad - first_total[:, None] / FF - hidden_normed * (second_total[:, None] / FF)
    )
    inner_gain_grad = jnp.sum(normed_grad * hidden_normed, axis=0)
    inner_bias_grad = jnp.sum(normed_grad, axis=0)
    gate_grad = (
        hidden_grad * up_value * sigmoid_gate * (1.0 + gate_value * (1.0 - sigmoid_gate))
    ).astype(narrow)
    up_grad = (hidden_grad * gate_value * sigmoid_gate).astype(narrow)
    gate_bias_grad = jnp.sum(gate_grad.astype(single), axis=0)
    up_bias_grad = jnp.sum(up_grad.astype(single), axis=0)
    gate_up_grad, _ = pack([gate_grad, up_grad, jnp.zeros((local_rows, 0), narrow)])
    gate_up_weight_grad = jnp.einsum(
        "td,tf->df", second_input, gate_up_grad, preferred_element_type=single
    )
    second_back = join_columns(
        jnp.einsum("tf,df->td", gate_up_grad, gate_up_full, preferred_element_type=single)
    )
    second_delta, gain_two_grad, shift_two_grad = norm_backward(
        second_back, normed_two, inv_std_two, ffn_vectors[:, 0]
    )
    residual_grad = out_float + second_delta
    attn_grad = residual_grad.astype(narrow)
    proj_bias_grad = jnp.sum(attn_grad.astype(single), axis=0)
    proj_weight_grad_t = jnp.einsum(
        "td,te->de", attn_grad, attended, preferred_element_type=single
    )
    mid_small = jnp.concatenate([gate_bias_grad, up_bias_grad, inner_gain_grad, inner_bias_grad])
    mid_pack, mid_at = pack(
        [
            row_major(gate_up_weight_grad.astype(narrow)),
            row_major(down_weight_grad_t.astype(narrow)),
            row_major(proj_weight_grad_t.astype(narrow)),
            jnp.stack(
                [gain_two_grad, shift_two_grad, down_bias_grad, proj_bias_grad], axis=1
            ).astype(narrow),
            spread(mid_small, rows_local, row_count).astype(narrow),
        ]
    )
    mid_pack, attn_grad_held, down_input_held = lax.optimization_barrier(
        (mid_pack, attn_grad, down_padded)
    )
    ffn_partial = jnp.einsum(
        "tf,df->td", down_input_held, down_t_padded, preferred_element_type=single
    )
    layer_out = (
        residual_half
        + share_columns(ffn_partial)
        + own_half(ffn_vectors[:, 2], column, half_width)
    ).astype(narrow)
    mid_sums = lax.psum_scatter(mid_pack, "row", scatter_dimension=0, tiled=True).astype(single)
    attended_grad = jnp.einsum(
        "td,de->te", attn_grad_held, proj_t, preferred_element_type=single
    ).astype(narrow)

    def attend_back(operands):
        query_block, key_block, value_block, grad_block = operands
        scores = (
            jnp.einsum("qd,kd->qk", query_block, key_block, preferred_element_type=single) * scaling
        )
        weights = jax.nn.softmax(scores, axis=-1)
        value_grad = jnp.einsum(
            "qk,qd->kd", weights.astype(narrow), grad_block, preferred_element_type=single
        )
        weight_grad = jnp.einsum(
            "qd,kd->qk", grad_block, value_block, preferred_element_type=single
        )
        score_grad = (
            weights * (weight_grad - jnp.sum(weight_grad * weights, axis=-1, keepdims=True))
        ).astype(narrow)
        query_grad = (
            jnp.einsum("qk,kd->qd", score_grad, key_block, preferred_element_type=single) * scaling
        )
        key_grad = (
            jnp.einsum("qk,qd->kd", score_grad, query_block, preferred_element_type=single)
            * scaling
        )
        return (query_grad, key_grad, value_grad)

    query_grads, key_grads, value_grads = lax.map(
        attend_back,
        (by_head(queries), by_head(keys_all), by_head(values_all), by_head(attended_grad)),
    )
    query_pre = rotary_back(
        from_head(query_grads).reshape(local_rows, head_local, HD), cosine_table, sine_table
    )
    key_pre = rotary_back(
        from_head(key_grads).reshape(local_rows, head_local, HD), cosine_table, sine_table
    )
    qkv_grad = jnp.stack(
        [
            query_pre.reshape(local_rows, half_width),
            key_pre.reshape(local_rows, half_width),
            from_head(value_grads),
        ],
        axis=1,
    ).astype(narrow)
    qkv_grad_float = qkv_grad.astype(single)
    query_bias_grad = jnp.sum(qkv_grad_float[:, 0], axis=0)
    value_bias_grad = jnp.sum(qkv_grad_float[:, 2], axis=0)
    qkv_weight_grad = jnp.einsum(
        "td,tpe->dpe", first_input, qkv_grad, preferred_element_type=single
    )
    first_back = join_columns(
        jnp.einsum("tpe,dpe->td", qkv_grad, qkv_full, preferred_element_type=single)
    )
    first_delta, gain_one_grad, shift_one_grad = norm_backward(
        first_back, normed_one, inv_std_one, attn_vectors[:, 0]
    )
    input_grad = own_half(residual_grad + first_delta, column, half_width).astype(narrow)
    end_pack, end_at = pack(
        [
            qkv_weight_grad.reshape(model_width, 3 * half_width).astype(narrow),
            jnp.stack([gain_one_grad, shift_one_grad], axis=1).astype(narrow),
            spread(
                jnp.concatenate([query_bias_grad, value_bias_grad]), rows_local, row_count
            ).astype(narrow),
        ]
    )
    end_pack, mid_sums = lax.optimization_barrier((end_pack, mid_sums))
    end_sums = lax.psum_scatter(end_pack, "row", scatter_dimension=0, tiled=True).astype(single)

    def cut(sums, offset, width):
        return sums[:, offset : offset + width]

    mid_vectors = cut(mid_sums, mid_at[3], 4)
    mid_small_sum = cut(mid_sums, mid_at[4], -(-mid_small.shape[0] // rows_local)).reshape(-1)
    end_vectors = cut(end_sums, end_at[1], 2)
    end_small_sum = cut(end_sums, end_at[2], -(-2 * half_width // rows_local)).reshape(-1)
    return (
        layer_out,
        input_grad,
        end_vectors[:, 0],
        end_vectors[:, 1],
        cut(end_sums, end_at[0], 3 * half_width).reshape(rows_local, 3, half_width),
        end_small_sum[:half_width],
        end_small_sum[half_width : 2 * half_width],
        cut(mid_sums, mid_at[2], half_width).T,
        mid_vectors[:, 3],
        mid_vectors[:, 0],
        mid_vectors[:, 1],
        cut(mid_sums, mid_at[0], ff_local),
        mid_small_sum[:ff_local],
        cut(mid_sums, mid_at[0] + ffn_at[1], ff_local),
        mid_small_sum[ff_local : 2 * ff_local],
        mid_small_sum[2 * ff_local : 3 * ff_local],
        mid_small_sum[3 * ff_local : 4 * ff_local],
        cut(mid_sums, mid_at[1], ff_local).T,
        mid_vectors[:, 2],
    )


def solution(mesh):
    placed = (
        P("row", "col"),
        P("row"),
        P("row"),
        P("row", None, "col"),
        P("col"),
        P("col"),
        P("col", "row"),
        P("row"),
        P("row"),
        P("row"),
        P("row", "col"),
        P("col"),
        P("row", "col"),
        P("col"),
        P("col"),
        P("col"),
        P("col", "row"),
        P("row"),
        P("row", "col"),
    )
    return jax.shard_map(
        functools.partial(body, mesh.shape["row"]),
        mesh=mesh,
        in_specs=placed,
        out_specs=(
            P("row", "col"),
            P("row", "col"),
            P("row"),
            P("row"),
            P("row", None, "col"),
            P("col"),
            P("col"),
            P("col", "row"),
            P("row"),
            P("row"),
            P("row"),
            P("row", "col"),
            P("col"),
            P("row", "col"),
            P("col"),
            P("col"),
            P("col"),
            P("col", "row"),
            P("row"),
        ),
        check_vma=False,
    )
```

```python
import functools
import math

import jax
import jax.numpy as jnp
from jax import lax
from jax.experimental.layout import Layout, with_layout_constraint
from jax.sharding import PartitionSpec as P


HD = 64
FF = 2730
GRID = 32
SEQ = 1025


EPSILON = 1e-06


def norm_forward(values, norm_gain, norm_shift):
    row_mean = jnp.mean(values, axis=-1, keepdims=True)
    centred = values - row_mean
    variance = jnp.mean(centred * centred, axis=-1, keepdims=True)
    inv_std = lax.rsqrt(variance + EPSILON)
    normed = centred * inv_std
    return (normed * norm_gain + norm_shift, normed, inv_std)


def norm_backward(upstream, normed, inv_std, norm_gain):
    scaled = upstream * norm_gain
    first_mean = jnp.mean(scaled, axis=-1, keepdims=True)
    second_mean = jnp.mean(scaled * normed, axis=-1, keepdims=True)
    delta = inv_std * (scaled - first_mean - normed * second_mean)
    return (delta, jnp.sum(upstream * normed, axis=0), jnp.sum(upstream, axis=0))


def rotary_tables(length, seq_len, grid_side, head_size):
    quarter = head_size // 4
    position = jnp.arange(length, dtype=jnp.int32) % seq_len
    patch_index = jnp.maximum(position - 1, 0)
    inside = (position > 0).astype(jnp.float32)
    row_pos = (patch_index // grid_side).astype(jnp.float32) * inside
    col_pos = (patch_index % grid_side).astype(jnp.float32) * inside
    frequency = jnp.exp(-math.log(10000.0) * jnp.arange(quarter, dtype=jnp.float32) / quarter)
    row_angle = row_pos[:, None] * frequency[None, :]
    col_angle = col_pos[:, None] * frequency[None, :]
    angles = jnp.concatenate([row_angle, row_angle, col_angle, col_angle], axis=1)
    return (jnp.cos(angles), jnp.sin(angles))


def rotate(values):
    pieces = jnp.split(values, 4, axis=-1)
    return jnp.concatenate([-pieces[1], pieces[0], -pieces[3], pieces[2]], axis=-1)


def rotate_transposed(values):
    pieces = jnp.split(values, 4, axis=-1)
    return jnp.concatenate([pieces[1], -pieces[0], pieces[3], -pieces[2]], axis=-1)


def apply_rotary(values, cosine_table, sine_table):
    return values * cosine_table[:, None, :] + rotate(values) * sine_table[:, None, :]


def rotary_back(grads, cosine_table, sine_table):
    return grads * cosine_table[:, None, :] + rotate_transposed(grads * sine_table[:, None, :])


def own_half(vector, column, half_width):
    return lax.dynamic_slice_in_dim(vector, column * half_width, half_width, axis=vector.ndim - 1)


def swap_columns(values):
    return lax.ppermute(values, "col", [(0, 1), (1, 0)])


def share_columns(partial_sums):
    half = partial_sums.shape[1] // 2
    column = lax.axis_index("col")
    own = lax.dynamic_slice_in_dim(partial_sums, column * half, half, axis=1)
    other = lax.dynamic_slice_in_dim(partial_sums, (1 - column) * half, half, axis=1)
    return own + swap_columns(other.astype(jnp.bfloat16)).astype(jnp.float32)


def join_columns(partial_sums):
    narrow = partial_sums.astype(jnp.bfloat16)
    return narrow.astype(jnp.float32) + swap_columns(narrow).astype(jnp.float32)


def gather_columns(values):
    other = swap_columns(values)
    first = lax.axis_index("col") == 0
    return jnp.concatenate(
        [jnp.where(first, values, other), jnp.where(first, other, values)], axis=1
    )


def hidden_totals(row_sums):
    return tuple(part + swap_columns(part) for part in row_sums)


def row_major(values):
    return with_layout_constraint(values, Layout((0, 1)))


def lane_round(width):
    return -(-width // 128) * 128


def pack(pieces):
    offsets = []
    padded = []
    position = 0
    for piece in pieces:
        width = lane_round(piece.shape[1])
        offsets.append(position)
        padded.append(jnp.pad(piece, ((0, 0), (0, width - piece.shape[1]))))
        position += width
    return jnp.concatenate(padded, axis=1), offsets


def spread(vector, rows_local, row_count):
    cols = -(-vector.shape[0] // rows_local)
    block = jnp.pad(vector, (0, rows_local * cols - vector.shape[0])).reshape(rows_local, cols)
    return jnp.tile(block, (row_count, 1))


def body(
    row_count,
    tokens,
    norm1_gain,
    norm1_bias,
    qkv_weight,
    query_bias,
    value_bias,
    proj_weight,
    proj_bias,
    norm2_gain,
    norm2_bias,
    gate_weight,
    gate_bias,
    up_weight,
    up_bias,
    inner_gain,
    inner_bias,
    down_weight,
    down_bias,
    cotangent,
):
    single = jnp.float32
    narrow = jnp.bfloat16
    local_rows = tokens.shape[0]
    half_width = tokens.shape[1]
    rows_local = norm1_gain.shape[0]
    model_width = rows_local * row_count
    ff_local = gate_weight.shape[1]
    head_local = half_width // HD
    images_local = local_rows // SEQ
    column = lax.axis_index("col")
    scaling = 1.0 / math.sqrt(HD)
    cosine_table, sine_table = rotary_tables(local_rows, SEQ, GRID, HD)

    def by_head(array):
        shaped = array.reshape(images_local, SEQ, head_local, HD).transpose(0, 2, 1, 3)
        return shaped.reshape(images_local * head_local, SEQ, HD)

    def from_head(array):
        shaped = array.reshape(images_local, head_local, SEQ, HD).transpose(0, 2, 1, 3)
        return shaped.reshape(local_rows, half_width)

    attn_pack, attn_at = pack(
        [
            qkv_weight.reshape(rows_local, 3 * half_width),
            proj_weight.T,
            jnp.stack(
                [norm1_gain, norm1_bias, proj_bias, norm2_gain, norm2_bias, down_bias], axis=1
            ),
        ]
    )
    attn_full = lax.all_gather(attn_pack, "row", axis=0, tiled=True)
    qkv_full = attn_full[:, attn_at[0] : attn_at[0] + 3 * half_width].reshape(
        model_width, 3, half_width
    )
    proj_t = attn_full[:, attn_at[1] : attn_at[1] + half_width]
    attn_vectors = attn_full[:, attn_at[2] : attn_at[2] + 6].astype(single)
    ffn_vectors = attn_vectors[:, 3:]

    whole_input = gather_columns(tokens).astype(single)
    normed_out, normed_one, inv_std_one = norm_forward(
        whole_input, attn_vectors[:, 0], attn_vectors[:, 1]
    )
    first_input = normed_out.astype(narrow)
    qkv_bias = jnp.stack(
        [query_bias.astype(single), jnp.zeros((half_width,), single), value_bias.astype(single)]
    )
    projected = (
        jnp.einsum("td,dpe->tpe", first_input, qkv_full, preferred_element_type=single) + qkv_bias
    )
    queries = apply_rotary(
        projected[:, 0].reshape(local_rows, head_local, HD), cosine_table, sine_table
    ).astype(narrow)
    keys_all = apply_rotary(
        projected[:, 1].reshape(local_rows, head_local, HD), cosine_table, sine_table
    ).astype(narrow)
    values_all = projected[:, 2].astype(narrow)

    def attend(operands):
        query_block, key_block, value_block = operands
        scores = (
            jnp.einsum("qd,kd->qk", query_block, key_block, preferred_element_type=single) * scaling
        )
        weights = jax.nn.softmax(scores, axis=-1)
        mixed = jnp.einsum(
            "qk,kd->qd", weights.astype(narrow), value_block, preferred_element_type=single
        )
        return mixed.astype(narrow)

    attended = from_head(
        lax.map(attend, (by_head(queries), by_head(keys_all), by_head(values_all)))
    )
    attn_partial = jnp.einsum("te,de->td", attended, proj_t, preferred_element_type=single)
    residual_half = (
        tokens.astype(single)
        + share_columns(attn_partial)
        + own_half(attn_vectors[:, 2], column, half_width)
    )
    residual_full = gather_columns(residual_half.astype(jnp.bfloat16)).astype(residual_half.dtype)

    ffn_pack, ffn_at = pack(
        [
            gate_weight,
            up_weight,
            down_weight.T,
        ]
    )
    ffn_full = lax.all_gather(ffn_pack, "row", axis=0, tiled=True)
    gate_up_full = ffn_full[:, : ffn_at[2]]
    down_t = ffn_full[:, ffn_at[2] : ffn_at[2] + ff_local]

    second_out, normed_two, inv_std_two = norm_forward(
        residual_full, ffn_vectors[:, 0], ffn_vectors[:, 1]
    )
    second_input = second_out.astype(narrow)
    gate_value = jnp.dot(
        second_input, gate_up_full[:, :ff_local], preferred_element_type=single
    ) + gate_bias.astype(single)
    up_value = jnp.dot(
        second_input, gate_up_full[:, ffn_at[1] : ffn_at[1] + ff_local], preferred_element_type=single
    ) + up_bias.astype(single)
    sigmoid_gate = jax.nn.sigmoid(gate_value)
    hidden = gate_value * sigmoid_gate * up_value
    hidden_mean = hidden_totals((jnp.sum(hidden, axis=1),))[0][:, None] / FF
    hidden_centred = hidden - hidden_mean
    hidden_var = hidden_totals((jnp.sum(hidden_centred * hidden_centred, axis=1),))[0][:, None] / FF
    hidden_inv = lax.rsqrt(hidden_var + EPSILON)
    hidden_normed = hidden_centred * hidden_inv
    down_input = (hidden_normed * inner_gain.astype(single) + inner_bias.astype(single)).astype(
        narrow
    )
    out_full = gather_columns(cotangent)
    out_float = out_full.astype(single)
    down_weight_grad_t = jnp.einsum(
        "td,tf->df", out_full, down_input, preferred_element_type=single
    )
    down_bias_grad = jnp.sum(out_float, axis=0)
    normed_grad = jnp.einsum("td,df->tf", out_full, down_t, preferred_element_type=single)
    scaled_grad = normed_grad * inner_gain.astype(single)
    first_total, second_total = hidden_totals(
        (jnp.sum(scaled_grad, axis=1), jnp.sum(scaled_grad * hidden_normed, axis=1))
    )
    hidden_grad = hidden_inv * (
        scaled_grad - first_total[:, None] / FF - hidden_normed * (second_total[:, None] / FF)
    )
    inner_gain_grad = jnp.sum(normed_grad * hidden_normed, axis=0)
    inner_bias_grad = jnp.sum(normed_grad, axis=0)
    gate_grad = (
        hidden_grad * up_value * sigmoid_gate * (1.0 + gate_value * (1.0 - sigmoid_gate))
    ).astype(narrow)
    up_grad = (hidden_grad * gate_value * sigmoid_gate).astype(narrow)
    gate_bias_grad = jnp.sum(gate_grad.astype(single), axis=0)
    up_bias_grad = jnp.sum(up_grad.astype(single), axis=0)
    gate_up_grad, _ = pack([gate_grad, up_grad, jnp.zeros((local_rows, 0), narrow)])
    gate_up_weight_grad = jnp.einsum(
        "td,tf->df", second_input, gate_up_grad, preferred_element_type=single
    )
    second_back = join_columns(
        jnp.einsum("tf,df->td", gate_up_grad, gate_up_full, preferred_element_type=single)
    )
    second_delta, gain_two_grad, shift_two_grad = norm_backward(
        second_back, normed_two, inv_std_two, ffn_vectors[:, 0]
    )
    residual_grad = out_float + second_delta
    attn_grad = residual_grad.astype(narrow)
    proj_bias_grad = jnp.sum(attn_grad.astype(single), axis=0)
    proj_weight_grad_t = jnp.einsum(
        "td,te->de", attn_grad, attended, preferred_element_type=single
    )
    mid_small = jnp.concatenate([gate_bias_grad, up_bias_grad, inner_gain_grad, inner_bias_grad])
    mid_pack, mid_at = pack(
        [
            row_major(gate_up_weight_grad.astype(narrow)),
            row_major(down_weight_grad_t.astype(narrow)),
            row_major(proj_weight_grad_t.astype(narrow)),
            jnp.stack(
                [gain_two_grad, shift_two_grad, down_bias_grad, proj_bias_grad], axis=1
            ).astype(narrow),
            spread(mid_small, rows_local, row_count).astype(narrow),
        ]
    )
    mid_pack, attn_grad_held, down_input_held = lax.optimization_barrier(
        (mid_pack, attn_grad, down_input)
    )
    ffn_partial = jnp.einsum(
        "tf,df->td", down_input_held, down_t, preferred_element_type=single
    )
    layer_out = (
        residual_half
        + share_columns(ffn_partial)
        + own_half(ffn_vectors[:, 2], column, half_width)
    ).astype(narrow)
    mid_sums = lax.psum_scatter(mid_pack, "row", scatter_dimension=0, tiled=True).astype(single)
    attended_grad = jnp.einsum(
        "td,de->te", attn_grad_held, proj_t, preferred_element_type=single
    ).astype(narrow)

    def attend_back(operands):
        query_block, key_block, value_block, grad_block = operands
        scores = (
            jnp.einsum("qd,kd->qk", query_block, key_block, preferred_element_type=single) * scaling
        )
        weights = jax.nn.softmax(scores, axis=-1)
        value_grad = jnp.einsum(
            "qk,qd->kd", weights.astype(narrow), grad_block, preferred_element_type=single
        )
        weight_grad = jnp.einsum(
            "qd,kd->qk", grad_block, value_block, preferred_element_type=single
        )
        score_grad = (
            weights * (weight_grad - jnp.sum(weight_grad * weights, axis=-1, keepdims=True))
        ).astype(narrow)
        query_grad = (
            jnp.einsum("qk,kd->qd", score_grad, key_block, preferred_element_type=single) * scaling
        )
        key_grad = (
            jnp.einsum("qk,qd->kd", score_grad, query_block, preferred_element_type=single)
            * scaling
        )
        return (query_grad, key_grad, value_grad)

    query_grads, key_grads, value_grads = lax.map(
        attend_back,
        (by_head(queries), by_head(keys_all), by_head(values_all), by_head(attended_grad)),
    )
    query_pre = rotary_back(
        from_head(query_grads).reshape(local_rows, head_local, HD), cosine_table, sine_table
    )
    key_pre = rotary_back(
        from_head(key_grads).reshape(local_rows, head_local, HD), cosine_table, sine_table
    )
    qkv_grad = jnp.stack(
        [
            query_pre.reshape(local_rows, half_width),
            key_pre.reshape(local_rows, half_width),
            from_head(value_grads),
        ],
        axis=1,
    ).astype(narrow)
    qkv_grad_float = qkv_grad.astype(single)
    query_bias_grad = jnp.sum(qkv_grad_float[:, 0], axis=0)
    value_bias_grad = jnp.sum(qkv_grad_float[:, 2], axis=0)
    qkv_weight_grad = jnp.einsum(
        "td,tpe->dpe", first_input, qkv_grad, preferred_element_type=single
    )
    first_back = join_columns(
        jnp.einsum("tpe,dpe->td", qkv_grad, qkv_full, preferred_element_type=single)
    )
    first_delta, gain_one_grad, shift_one_grad = norm_backward(
        first_back, normed_one, inv_std_one, attn_vectors[:, 0]
    )
    input_grad = own_half(residual_grad + first_delta, column, half_width).astype(narrow)
    end_pack, end_at = pack(
        [
            qkv_weight_grad.reshape(model_width, 3 * half_width).astype(narrow),
            jnp.stack([gain_one_grad, shift_one_grad], axis=1).astype(narrow),
            spread(
                jnp.concatenate([query_bias_grad, value_bias_grad]), rows_local, row_count
            ).astype(narrow),
        ]
    )
    end_pack, mid_sums = lax.optimization_barrier((end_pack, mid_sums))
    end_sums = lax.psum_scatter(end_pack, "row", scatter_dimension=0, tiled=True).astype(single)

    def cut(sums, offset, width):
        return sums[:, offset : offset + width]

    mid_vectors = cut(mid_sums, mid_at[3], 4)
    mid_small_sum = cut(mid_sums, mid_at[4], -(-mid_small.shape[0] // rows_local)).reshape(-1)
    end_vectors = cut(end_sums, end_at[1], 2)
    end_small_sum = cut(end_sums, end_at[2], -(-2 * half_width // rows_local)).reshape(-1)
    return (
        layer_out,
        input_grad,
        end_vectors[:, 0],
        end_vectors[:, 1],
        cut(end_sums, end_at[0], 3 * half_width).reshape(rows_local, 3, half_width),
        end_small_sum[:half_width],
        end_small_sum[half_width : 2 * half_width],
        cut(mid_sums, mid_at[2], half_width).T,
        mid_vectors[:, 3],
        mid_vectors[:, 0],
        mid_vectors[:, 1],
        cut(mid_sums, mid_at[0], ff_local),
        mid_small_sum[:ff_local],
        cut(mid_sums, mid_at[0] + ffn_at[1], ff_local),
        mid_small_sum[ff_local : 2 * ff_local],
        mid_small_sum[2 * ff_local : 3 * ff_local],
        mid_small_sum[3 * ff_local : 4 * ff_local],
        cut(mid_sums, mid_at[1], ff_local).T,
        mid_vectors[:, 2],
    )


def solution(mesh):
    placed = (
        P("row", "col"),
        P("row"),
        P("row"),
        P("row", None, "col"),
        P("col"),
        P("col"),
        P("col", "row"),
        P("row"),
        P("row"),
        P("row"),
        P("row", "col"),
        P("col"),
        P("row", "col"),
        P("col"),
        P("col"),
        P("col"),
        P("col", "row"),
        P("row"),
        P("row", "col"),
    )
    return jax.shard_map(
        functools.partial(body, mesh.shape["row"]),
        mesh=mesh,
        in_specs=placed,
        out_specs=(
            P("row", "col"),
            P("row", "col"),
            P("row"),
            P("row"),
            P("row", None, "col"),
            P("col"),
            P("col"),
            P("col", "row"),
            P("row"),
            P("row"),
            P("row"),
            P("row", "col"),
            P("col"),
            P("row", "col"),
            P("col"),
            P("col"),
            P("col"),
            P("col", "row"),
            P("row"),
        ),
        check_vma=False,
    )
```
